8 devices in a mesh: dp: 1 (over z), tp: 2 (over y), pp: 4 (over x, core).
Axes of the slice: x: 2, y: 2, z: 1, core: 2. Of those that a mesh axis runs over, the one named last changes fastest.
Arguments:
- hidden: bfloat16 [2, 128, 2048], P('dp')
- positions: int32 [2, 128], P('dp')
- key_cache: bfloat16 [4, 2, 128, 32, 32, 64], P('pp', 'dp', None, 'tp')
- value_cache: bfloat16 [4, 2, 128, 32, 32, 64], P('pp', 'dp', None, 'tp')
- attn_norm: bfloat16 [4, 2048], P('pp')
- w_query: bfloat16 [4, 2048, 2048], P('pp', None, 'tp')
- w_key: bfloat16 [4, 2048, 2048], P('pp', None, 'tp')
- w_value: bfloat16 [4, 2048, 2048], P('pp', None, 'tp')
- w_out: bfloat16 [4, 2048, 2048], P('pp', 'tp')
- mlp_norm: bfloat16 [4, 2048], P('pp')
- w_gate: bfloat16 [4, 2048, 8192], P('pp', None, 'tp')
- w_up: bfloat16 [4, 2048, 8192], P('pp', None, 'tp')
- w_down: bfloat16 [4, 8192, 2048], P('pp', 'tp')
Outputs:
- output 1: bfloat16 [2, 128, 2048], P('dp')
- output 2: bfloat16 [4, 2, 128, 32, 32, 64], P('pp', 'dp', None, 'tp')
- output 3: bfloat16 [4, 2, 128, 32, 32, 64], P('pp', 'dp', None, 'tp')
All inputs are finite; a program needn't handle non-finite values.
Results may differ from the reference program's by a relative error of at most 0.02.
Values are sent between devices in bfloat16 or wider.
A program may use at most 1 GiB of HBM per device.

```python
import math
import jax
import jax.numpy as jnp
from jax import lax

D = 2048
HEADS = 32
KV_HEADS = 32
HEAD = 64
FF = 8192
GROUPS = 2
BATCH = 128
SEQ = 32
LAYERS = 4

ROPE_THETA = 500000.0
SCALE_FACTOR = 8.0
LOW_FACTOR = 1.0
HIGH_FACTOR = 4.0
ORIG_CONTEXT = 8192.0
NORM_EPS = 1e-5
GQA_SIZE = HEADS // KV_HEADS


def rope_freqs():
    freq_index = jnp.arange(HEAD // 2, dtype=jnp.float32)
    base_freq = ROPE_THETA ** (-2.0 * freq_index / HEAD)
    wave_len = 2.0 * math.pi / base_freq
    smooth_t = (ORIG_CONTEXT / wave_len - LOW_FACTOR) / (HIGH_FACTOR - LOW_FACTOR)
    mixed_freq = (1.0 - smooth_t) * base_freq / SCALE_FACTOR + smooth_t * base_freq
    long_freq = jnp.where(wave_len > ORIG_CONTEXT / LOW_FACTOR, base_freq / SCALE_FACTOR, mixed_freq)
    return jnp.where(wave_len < ORIG_CONTEXT / HIGH_FACTOR, base_freq, long_freq)


def rms_norm(values, gain_vec):
    values_f = values.astype(jnp.float32)
    inv_rms = lax.rsqrt(jnp.mean(values_f * values_f, axis=-1, keepdims=True) + NORM_EPS)
    return (values_f * inv_rms * gain_vec.astype(jnp.float32)).astype(jnp.bfloat16)


def rotate(values_f, cosine, sine_t):
    half_dim = values_f.shape[-1] // 2
    first_half = values_f[..., :half_dim]
    second_half = values_f[..., half_dim:]
    return jnp.concatenate([first_half * cosine - second_half * sine_t, second_half * cosine + first_half * sine_t], axis=-1)


def setup_inputs(seed: int = 0, part: int = 0) -> dict:
    root_key = jax.random.key(seed)
    part_keys = jax.random.split(jax.random.fold_in(root_key, part), 5)
    weight_keys = jax.random.split(root_key, 9)
    hidden = jax.random.normal(part_keys[0], (GROUPS, BATCH, D), jnp.float32)
    group_len = jax.random.randint(part_keys[1], (GROUPS,), max(SEQ // 8, 1), SEQ + 1, dtype=jnp.int32)
    raw_pos = jax.random.randint(part_keys[2], (GROUPS, BATCH), 0, SEQ, dtype=jnp.int32)
    positions = ((raw_pos * group_len[:, None]) // SEQ).at[0, 0].set(SEQ - 1)
    cache_shape = (LAYERS, GROUPS, BATCH, KV_HEADS, SEQ, HEAD)
    key_cache = jax.random.normal(part_keys[3], cache_shape, jnp.float32)
    value_cache = jax.random.normal(part_keys[4], cache_shape, jnp.float32)
    attn_norm = 1.0 + 0.3 * jax.random.normal(weight_keys[0], (LAYERS, D), jnp.float32)
    w_query = jax.random.normal(weight_keys[1], (LAYERS, D, HEADS * HEAD), jnp.float32) * D ** -0.5
    w_key = jax.random.normal(weight_keys[2], (LAYERS, D, KV_HEADS * HEAD), jnp.float32) * D ** -0.5
    w_value = jax.random.normal(weight_keys[3], (LAYERS, D, KV_HEADS * HEAD), jnp.float32) * D ** -0.5
    w_out = jax.random.normal(weight_keys[4], (LAYERS, HEADS * HEAD, D), jnp.float32) * 2.0 * (HEADS * HEAD) ** -0.5
    mlp_norm = jax.random.normal(weight_keys[5], (LAYERS, D), jnp.float32)
    w_gate = jax.random.normal(weight_keys[6], (LAYERS, D, FF), jnp.float32) * D ** -0.5
    w_up = jax.random.normal(weight_keys[7], (LAYERS, D, FF), jnp.float32) * D ** -0.5
    w_down = jax.random.normal(weight_keys[8], (LAYERS, FF, D), jnp.float32) * FF ** -0.5
    return {
        "hidden": hidden.astype(jnp.bfloat16),
        "positions": positions,
        "key_cache": key_cache.astype(jnp.bfloat16),
        "value_cache": value_cache.astype(jnp.bfloat16),
        "attn_norm": attn_norm.astype(jnp.bfloat16),
        "w_query": w_query.astype(jnp.bfloat16),
        "w_key": w_key.astype(jnp.bfloat16),
        "w_value": w_value.astype(jnp.bfloat16),
        "w_out": w_out.astype(jnp.bfloat16),
        "mlp_norm": mlp_norm.astype(jnp.bfloat16),
        "w_gate": w_gate.astype(jnp.bfloat16),
        "w_up": w_up.astype(jnp.bfloat16),
        "w_down": w_down.astype(jnp.bfloat16),
    }


def reference(hidden, positions, key_cache, value_cache, attn_norm, w_query, w_key, w_value, w_out, mlp_norm, w_gate, w_up, w_down):
    inv_freq = rope_freqs()
    seq_rows = jnp.arange(SEQ)

    def one_layer(state_h, layer_in):
        key_l, value_l, gain_attn, wq_l, wk_l, wv_l, wo_l, gain_mlp, wg_l, wu_l, wd_l = layer_in

        def one_group(group_in):
            tokens, key_g, value_g, pos_g = group_in
            angles = pos_g.astype(jnp.float32)[:, None] * inv_freq
            cosine = jnp.cos(angles)
            sine_t = jnp.sin(angles)
            normed = rms_norm(tokens, gain_attn)
            query_f = jnp.dot(normed, wq_l, preferred_element_type=jnp.float32).reshape(BATCH, KV_HEADS, GQA_SIZE, HEAD)
            query_h = rotate(query_f, cosine[:, None, None, :], sine_t[:, None, None, :]).astype(jnp.bfloat16)
            key_f = jnp.dot(normed, wk_l, preferred_element_type=jnp.float32).reshape(BATCH, KV_HEADS, HEAD)
            key_new = rotate(key_f, cosine[:, None, :], sine_t[:, None, :]).astype(jnp.bfloat16)
            value_new = jnp.dot(normed, wv_l, preferred_element_type=jnp.float32).astype(jnp.bfloat16).reshape(BATCH, KV_HEADS, HEAD)
            row_hit = (seq_rows[None, :] == pos_g[:, None])[:, None, :, None]
            key_g = jnp.where(row_hit, key_new[:, :, None, :], key_g)
            value_g = jnp.where(row_hit, value_new[:, :, None, :], value_g)
            scores = jnp.einsum("bkgd,bksd->bkgs", query_h.astype(jnp.float32), key_g.astype(jnp.float32)) * HEAD ** -0.5
            visible = (seq_rows[None, :] <= pos_g[:, None])[:, None, None, :]
            attn_probs = jax.nn.softmax(jnp.where(visible, scores, -jnp.inf), axis=-1).astype(jnp.bfloat16)
            attn_vals = jnp.einsum("bkgs,bksd->bkgd", attn_probs.astype(jnp.float32), value_g.astype(jnp.float32)).astype(jnp.bfloat16).reshape(BATCH, HEADS * HEAD)
            attn_out = jnp.dot(attn_vals, wo_l, preferred_element_type=jnp.float32).astype(jnp.bfloat16)
            mid_state = (tokens.astype(jnp.float32) + attn_out.astype(jnp.float32)).astype(jnp.bfloat16)
            normed_mlp = rms_norm(mid_state, gain_mlp)
            gate_f = jnp.dot(normed_mlp, wg_l, preferred_element_type=jnp.float32)
            up_f = jnp.dot(normed_mlp, wu_l, preferred_element_type=jnp.float32)
            act_bf = (jax.nn.silu(gate_f) * up_f).astype(jnp.bfloat16)
            mlp_out = jnp.dot(act_bf, wd_l, preferred_element_type=jnp.float32).astype(jnp.bfloat16)
            new_state = (mid_state.astype(jnp.float32) + mlp_out.astype(jnp.float32)).astype(jnp.bfloat16)
            return new_state, key_g, value_g

        new_state, key_l, value_l = lax.map(one_group, (state_h, key_l, value_l, positions))
        return new_state, (key_l, value_l)

    final_state, caches = lax.scan(one_layer, hidden, (key_cache, value_cache, attn_norm, w_query, w_key, w_value, w_out, mlp_norm, w_gate, w_up, w_down))
    return final_state, caches[0], caches[1]
```

```python
import functools
import math
import jax
import jax.numpy as jnp
from jax import lax
from jax.experimental import pallas as pl
from jax.experimental.pallas import tpu as pltpu
from jax.sharding import PartitionSpec as P

ROPE_THETA = 500000.0
SCALE_FACTOR = 8.0
LOW_FACTOR = 1.0
HIGH_FACTOR = 4.0
ORIG_CONTEXT = 8192.0
NORM_EPS = 1e-5
MESH = pl.DeviceIdType.MESH
F32 = jnp.float32
BF16 = jnp.bfloat16

COLS = 512
ROWS = 1024
KV_SLOTS = 4
NORM_ROWS = 16


def rope_freqs(head_dim):
    freq_index = jnp.arange(head_dim // 2, dtype=jnp.float32)
    base_freq = ROPE_THETA ** (-2.0 * freq_index / head_dim)
    wave_len = 2.0 * math.pi / base_freq
    smooth_t = (ORIG_CONTEXT / wave_len - LOW_FACTOR) / (HIGH_FACTOR - LOW_FACTOR)
    mixed_freq = (1.0 - smooth_t) * base_freq / SCALE_FACTOR + smooth_t * base_freq
    long_freq = jnp.where(wave_len > ORIG_CONTEXT / LOW_FACTOR, base_freq / SCALE_FACTOR, mixed_freq)
    return jnp.where(wave_len < ORIG_CONTEXT / HIGH_FACTOR, base_freq, long_freq)


def layer_kernel(dims, cos_ref, sin_ref, pos_ref, ga_ref, gm_ref, hid, kc, vc, wq, wk, wv, wo, wg, wu, wd,
                 hout, knew, vnew,
                 wqkv_v, wo_v, wg_v, wu_v, wd_v, k_v, v_v, hbuf, recvp, recvd, nbuf, qt, ubuf, sc,
                 hid_sem, wqkv_sem, wo_sem, gu_sem, wd_sem, k_sem, v_sem,
                 p_send, p_recv, d_send, d_recv, h_send, h_recv):
    n_groups, n_batch, d_model, heads, seq, hd, ff, n_pp, n_tp = dims
    hw = heads * hd
    n_chunk = d_model // COLS
    n_gu = ff // COLS
    n_kb = ff // ROWS
    pp = lax.axis_index("pp")
    tp = lax.axis_index("tp")
    peer = {"tp": lax.rem(tp + 1, n_tp)}
    nxt = {"pp": lax.rem(pp + 1, n_pp)}
    prv = {"pp": lax.rem(pp + n_pp - 1, n_pp)}

    def kv_copies(item, slot):
        g = item // heads
        h = lax.rem(item, heads)
        return (pltpu.make_async_copy(kc.at[g, h], k_v.at[slot], k_sem.at[slot]),
                pltpu.make_async_copy(vc.at[g, h], v_v.at[slot], v_sem.at[slot]))

    def gu_copies(j):
        cols = pl.ds(j * COLS, COLS)
        return (pltpu.make_async_copy(wg.at[:, cols], wg_v.at[j], gu_sem.at[0, j]),
                pltpu.make_async_copy(wu.at[:, cols], wu_v.at[j], gu_sem.at[1, j]))

    def wd_copy(nb, kb):
        return pltpu.make_async_copy(wd.at[pl.ds(kb * ROWS, ROWS), pl.ds(nb * COLS, COLS)], wd_v.at[kb], wd_sem.at[kb])

    def qkv_copies():
        return [pltpu.make_async_copy(src, wqkv_v.at[i], wqkv_sem.at[i]) for i, src in enumerate((wq, wk, wv))]

    def wo_copy():
        return pltpu.make_async_copy(wo, wo_v, wo_sem)

    def hid_copy(g):
        return pltpu.make_async_copy(hid.at[g], hbuf.at[g], hid_sem.at[g])

    def piece(ref, g, c):
        return ref.at[g, :, pl.ds(pl.multiple_of(c * COLS, COLS), COLS)]

    def p_copy(g, c):
        return pltpu.make_async_remote_copy(piece(hout, g, c), piece(recvp, g, c), p_send.at[g, c], p_recv.at[g, c], device_id=peer, device_id_type=MESH)

    def d_copy(g, c):
        return pltpu.make_async_remote_copy(piece(recvp, g, c), piece(recvd, g, c), d_send.at[g, c], d_recv.at[g, c], device_id=peer, device_id_type=MESH)

    def h_copy(g, c):
        return pltpu.make_async_remote_copy(piece(hout, g, c), piece(hbuf, g, c), h_send.at[g, c], h_recv.at[g, c], device_id=nxt, device_id_type=MESH)

    first = pp == 0
    last = pp == n_pp - 1

    @pl.when(first)
    def _():
        for g in range(n_groups):
            hid_copy(g).start()
    for copy in qkv_copies():
        copy.start()
    for slot in range(KV_SLOTS):
        for copy in kv_copies(slot, slot):
            copy.start()
    wo_copy().start()

    barrier = pltpu.get_barrier_semaphore()
    for other in (peer, nxt, prv):
        pl.semaphore_signal(barrier, inc=1, device_id=other, device_id_type=MESH)
    pl.semaphore_wait(barrier, 3)

    for copy in qkv_copies():
        copy.wait()
    for j in range(n_gu):
        for copy in gu_copies(j):
            copy.start()
    for kb in range(n_kb):
        wd_copy(0, kb).start()

    def norm_rows(g, gain_ref, with_partial):
        def body(r, carry):
            rows = pl.ds(pl.multiple_of(r * NORM_ROWS, NORM_ROWS), NORM_ROWS)
            x = hbuf[g, rows, :].astype(F32)
            if with_partial:
                part = (hout[g, rows, :].astype(F32) + recvp[g, rows, :].astype(F32)).astype(BF16)
                x = (x + part.astype(F32)).astype(BF16)
                hbuf[g, rows, :] = x
                x = x.astype(F32)
            inv = lax.rsqrt(jnp.mean(x * x, axis=-1, keepdims=True) + NORM_EPS)
            nbuf[rows, :] = (x * inv * gain_ref[...].astype(F32)).astype(BF16)
            return carry
        lax.fori_loop(0, n_batch // NORM_ROWS, body, 0)

    def attention_phase(g, carry):
        @pl.when(first)
        def _():
            hid_copy(g).wait()

        @pl.when(pp > 0)
        def _():
            for c in range(n_chunk):
                h_copy(g, c).wait_recv()

        norm_rows(g, ga_ref, False)
        cosine = cos_ref[g]
        sine = sin_ref[g]
        half = hd // 2
        for which in range(3):
            for c in range(hw // COLS):
                cols = slice(c * COLS, (c + 1) * COLS)
                prod = jnp.dot(nbuf[...], wqkv_v[which, :, cols], preferred_element_type=F32)
                prod_t = prod.T
                for h in range(COLS // hd):
                    head = c * (COLS // hd) + h
                    a = prod_t[h * hd:h * hd + half]
                    b = prod_t[h * hd + half:(h + 1) * hd]
                    if which < 2:
                        a, b = a * cosine - b * sine, b * cosine + a * sine
                    a, b = a.astype(BF16), b.astype(BF16)
                    if which == 0:
                        qt[head * hd:head * hd + half, :] = a
                        qt[head * hd + half:(head + 1) * hd, :] = b
                    else:
                        dst = knew if which == 1 else vnew
                        dst[g, head, 0:half, :] = a
                        dst[g, head, half:hd, :] = b

        pos = pos_ref[g]
        row_id = lax.broadcasted_iota(jnp.int32, (seq, n_batch), 0)
        hit = row_id == pos
        seen = row_id <= pos

        def head_body(h, inner):
            item = g * heads + h
            slot = lax.rem(item, KV_SLOTS)
            for copy in kv_copies(item, slot):
                copy.wait()
            rows = pl.ds(pl.multiple_of(h * hd, hd), hd)
            q = qt[rows, :].astype(F32)
            fresh = jnp.sum(q * knew[g, h].astype(F32), axis=0, keepdims=True)
            for s in range(seq):
                sc[s:s + 1, :] = jnp.sum(k_v[slot, s].astype(F32) * q, axis=0, keepdims=True)
            scores = jnp.where(hit, fresh, sc[...]) * hd ** -0.5
            scores = jnp.where(seen, scores, -jnp.inf)
            top = jnp.max(scores, axis=0, keepdims=True)
            expd = jnp.exp(scores - top)
            probs = (expd / jnp.sum(expd, axis=0, keepdims=True)).astype(BF16).astype(F32)
            sc[...] = jnp.where(hit, 0.0, probs)
            acc = jnp.sum(jnp.where(hit, probs, 0.0), axis=0, keepdims=True) * vnew[g, h].astype(F32)
            for s in range(seq):
                acc = acc + sc[s:s + 1, :] * v_v[slot, s].astype(F32)
            qt[rows, :] = acc.astype(BF16)

            @pl.when(item + KV_SLOTS < n_groups * heads)
            def _():
                for copy in kv_copies(item + KV_SLOTS, slot):
                    copy.start()
            return inner
        lax.fori_loop(0, heads, head_body, 0)

        @pl.when(g == 0)
        def _():
            wo_copy().wait()
        for c in range(hw // COLS):
            cols = slice(c * COLS, (c + 1) * COLS)
            nbuf[:, cols] = qt[cols, :].astype(F32).T.astype(BF16)

        for c in range(n_chunk):
            part = jnp.dot(nbuf[:, 0:hw], wo_v[:, c * COLS:(c + 1) * COLS], preferred_element_type=F32)
            hout[g, :, c * COLS:(c + 1) * COLS] = part.astype(BF16)
            p_copy(g, c).start()
        return carry

    def mlp_phase(g, carry):
        for c in range(n_chunk):
            p_copy(g, c).wait()
        norm_rows(g, gm_ref, True)

        def gu_body(j, inner):
            @pl.when(g == 0)
            def _():
                for copy in gu_copies(j):
                    copy.wait()
            gate = jnp.dot(nbuf[...], wg_v[j], preferred_element_type=F32)
            up = jnp.dot(nbuf[...], wu_v[j], preferred_element_type=F32)
            ubuf[:, pl.ds(pl.multiple_of(j * COLS, COLS), COLS)] = (jax.nn.silu(gate) * up).astype(BF16)
            return inner
        lax.fori_loop(0, n_gu, gu_body, 0)

        def wd_body(nb, inner):
            acc = None
            for kb in range(n_kb):
                wd_copy(nb, kb).wait()
                prod = jnp.dot(ubuf[:, kb * ROWS:(kb + 1) * ROWS], wd_v[kb], preferred_element_type=F32)
                acc = prod if acc is None else acc + prod

                @pl.when(g * n_chunk + nb + 1 < n_groups * n_chunk)
                def _():
                    wd_copy(lax.rem(nb + 1, n_chunk), kb).start()
            recvp[g, :, pl.ds(pl.multiple_of(nb * COLS, COLS), COLS)] = acc.astype(BF16)
            d_copy(g, nb).start()
            return inner
        lax.fori_loop(0, n_chunk, wd_body, 0)
        return carry

    def finish_phase(g, carry):
        for c in range(n_chunk):
            d_copy(g, c).wait()
            cols = slice(c * COLS, (c + 1) * COLS)
            part = (recvd[g, :, cols].astype(F32) + recvp[g, :, cols].astype(F32)).astype(BF16)
            hout[g, :, cols] = (hbuf[g, :, cols].astype(F32) + part.astype(F32)).astype(BF16)

            @pl.when(jnp.logical_not(last))
            def _():
                h_copy(g, c).start()
        return carry

    lax.fori_loop(0, n_groups, attention_phase, 0)
    lax.fori_loop(0, n_groups, mlp_phase, 0)
    lax.fori_loop(0, n_groups, finish_phase, 0)

    @pl.when(jnp.logical_not(last))
    def _():
        for g in range(n_groups):
            for c in range(n_chunk):
                h_copy(g, c).wait_send()


def run_layer(dims, *args):
    n_groups, n_batch, d_model, heads, seq, hd, ff, n_pp, n_tp = dims
    hw = heads * hd
    n_chunk = d_model // COLS
    n_gu = ff // COLS
    n_kb = ff // ROWS
    vmem = pl.BlockSpec(memory_space=pltpu.VMEM)
    hbm = pl.BlockSpec(memory_space=pl.ANY)
    dma = pltpu.SemaphoreType.DMA
    return pl.pallas_call(
        functools.partial(layer_kernel, dims),
        out_shape=(jax.ShapeDtypeStruct((n_groups, n_batch, d_model), BF16),
                   jax.ShapeDtypeStruct((n_groups, heads, hd, n_batch), BF16),
                   jax.ShapeDtypeStruct((n_groups, heads, hd, n_batch), BF16)),
        in_specs=[vmem] * 5 + [hbm] * 10,
        out_specs=(vmem, vmem, vmem),
        scratch_shapes=[
            pltpu.VMEM((3, d_model, hw), BF16),
            pltpu.VMEM((hw, d_model), BF16),
            pltpu.VMEM((n_gu, d_model, COLS), BF16),
            pltpu.VMEM((n_gu, d_model, COLS), BF16),
            pltpu.VMEM((n_kb, ROWS, COLS), BF16),
            pltpu.VMEM((KV_SLOTS, seq, hd, n_batch), BF16),
            pltpu.VMEM((KV_SLOTS, seq, hd, n_batch), BF16),
            pltpu.VMEM((n_groups, n_batch, d_model), BF16),
            pltpu.VMEM((n_groups, n_batch, d_model), BF16),
            pltpu.VMEM((n_groups, n_batch, d_model), BF16),
            pltpu.VMEM((n_batch, d_model), BF16),
            pltpu.VMEM((hw, n_batch), BF16),
            pltpu.VMEM((n_batch, ff), BF16),
            pltpu.VMEM((seq, n_batch), F32),
            dma((n_groups,)), dma((3,)), dma, dma((2, n_gu)), dma((n_kb,)), dma((KV_SLOTS,)), dma((KV_SLOTS,)),
            dma((n_groups, n_chunk)), dma((n_groups, n_chunk)), dma((n_groups, n_chunk)),
            dma((n_groups, n_chunk)), dma((n_groups, n_chunk)), dma((n_groups, n_chunk)),
        ],
        compiler_params=pltpu.CompilerParams(collective_id=0, has_side_effects=True, vmem_limit_bytes=67043328),
        name="layer",
    )(*args)


def solution(mesh):
    n_pp = mesh.shape["pp"]
    n_tp = mesh.shape["tp"]
    cache_spec = P("pp", "dp", None, "tp", None, None)
    col_spec = P("pp", None, "tp")
    row_spec = P("pp", "tp", None)
    gain_spec = P("pp", None)
    in_specs = (P("dp", None, None), P("dp", None), cache_spec, cache_spec, gain_spec, col_spec, col_spec, col_spec, row_spec, gain_spec, col_spec, col_spec, row_spec)
    out_specs = (P("dp", None, None), cache_spec, cache_spec)

    def per_device(hidden, positions, key_cache, value_cache, attn_norm, w_query, w_key, w_value, w_out, mlp_norm, w_gate, w_up, w_down):
        _, n_groups, n_batch, heads, seq, hd = key_cache.shape
        d_model = hidden.shape[-1]
        ff = w_gate.shape[-1]
        dims = (n_groups, n_batch, d_model, heads, seq, hd, ff, n_pp, n_tp)
        angles = positions.astype(F32)[:, None, :] * rope_freqs(hd)[None, :, None]
        key_t = jnp.transpose(key_cache[0], (0, 2, 3, 4, 1))
        value_t = jnp.transpose(value_cache[0], (0, 2, 3, 4, 1))
        state, key_new, value_new = run_layer(
            dims, jnp.cos(angles), jnp.sin(angles), positions[:, None, :], attn_norm, mlp_norm, hidden, key_t, value_t,
            w_query[0], w_key[0], w_value[0], w_out[0], w_gate[0], w_up[0], w_down[0])

        stage = lax.axis_index("pp")
        from_last = [lax.ppermute(state, "pp", [(n_pp - 1, dst)]) for dst in range(1, n_pp - 1)]
        from_last.append(lax.ppermute(from_last[0], "pp", [(1, 0)]))
        final = jnp.where(stage == n_pp - 1, state, sum(from_last[1:], from_last[0]))

        row_hit = jnp.arange(seq, dtype=jnp.int32)[None, None, :, None, None] == positions[:, None, None, None, :]
        key_t = jnp.where(row_hit, key_new[:, :, None], key_t)
        value_t = jnp.where(row_hit, value_new[:, :, None], value_t)
        return final, jnp.transpose(key_t, (0, 4, 1, 2, 3))[None], jnp.transpose(value_t, (0, 4, 1, 2, 3))[None]

    return jax.shard_map(per_device, mesh=mesh, in_specs=in_specs, out_specs=out_specs, check_vma=False)
```

```python
import functools
import math
import jax
import jax.numpy as jnp
from jax import lax
from jax.experimental import pallas as pl
from jax.experimental.pallas import tpu as pltpu
from jax.sharding import PartitionSpec as P

ROPE_THETA = 500000.0
SCALE_FACTOR = 8.0
LOW_FACTOR = 1.0
HIGH_FACTOR = 4.0
ORIG_CONTEXT = 8192.0
NORM_EPS = 1e-5
MESH = pl.DeviceIdType.MESH
F32 = jnp.float32
BF16 = jnp.bfloat16

COLS = 512
ROWS = 1024
SLOTS = 8
NORM_ROWS = 32


def rope_freqs(head_dim):
    freq_index = jnp.arange(head_dim // 2, dtype=jnp.float32)
    base_freq = ROPE_THETA ** (-2.0 * freq_index / head_dim)
    wave_len = 2.0 * math.pi / base_freq
    smooth_t = (ORIG_CONTEXT / wave_len - LOW_FACTOR) / (HIGH_FACTOR - LOW_FACTOR)
    mixed_freq = (1.0 - smooth_t) * base_freq / SCALE_FACTOR + smooth_t * base_freq
    long_freq = jnp.where(wave_len > ORIG_CONTEXT / LOW_FACTOR, base_freq / SCALE_FACTOR, mixed_freq)
    return jnp.where(wave_len < ORIG_CONTEXT / HIGH_FACTOR, base_freq, long_freq)


def layer_kernel(dims, cos_ref, sin_ref, pos_ref, ga_ref, gm_ref, hid, kc, vc, wq, wk, wv, wo, wg, wu, wd,
                 hout, knew, vnew,
                 wqkv_v, wo_v, wg_v, wu_v, ring, hbuf, recvp, recvd, nbuf, qt, ubuf, sc,
                 hid_sem, wqkv_sem, wo_sem, gu_sem, ring_sem,
                 p_send, p_recv, d_send, d_recv, h_send, h_recv):
    n_groups, n_batch, d_model, heads, seq, hd, ff, n_pp, n_tp = dims
    hw = heads * hd
    n_chunk = d_model // COLS
    n_gu = ff // COLS
    n_kb = ff // ROWS
    pp = lax.axis_index("pp")
    tp = lax.axis_index("tp")
    peer = {"tp": lax.rem(tp + 1, n_tp)}
    nxt = {"pp": lax.rem(pp + 1, n_pp)}
    prv = {"pp": lax.rem(pp + n_pp - 1, n_pp)}

    n_kv = n_groups * heads
    n_wd = n_chunk * n_kb
    n_items = n_kv + n_groups * n_wd
    slabs = COLS // n_batch
    deep = ROWS // hd

    def kv_copies(item, slot):
        g = item // heads
        h = lax.rem(item, heads)
        return (pltpu.make_async_copy(kc.at[g, h], ring.at[slot, pl.ds(0, seq)], ring_sem.at[slot, 0]),
                pltpu.make_async_copy(vc.at[g, h], ring.at[slot, pl.ds(seq, seq)], ring_sem.at[slot, 1]))

    def wd_copies(item, slot):
        tile = lax.rem(item - n_kv, n_wd)
        nb = tile // n_kb
        kb = lax.rem(tile, n_kb)
        return [pltpu.make_async_copy(
            wd.at[pl.ds(kb * deep, deep), :, pl.ds(pl.multiple_of(nb * COLS + i * n_batch, n_batch), n_batch)],
            ring.at[slot, pl.ds(i * deep, deep)], ring_sem.at[slot, i]) for i in range(slabs)]

    def gu_copies(j):
        cols = pl.ds(j * COLS, COLS)
        return (pltpu.make_async_copy(wg.at[:, cols], wg_v.at[j], gu_sem.at[0, j]),
                pltpu.make_async_copy(wu.at[:, cols], wu_v.at[j], gu_sem.at[1, j]))

    def qkv_copies():
        return [pltpu.make_async_copy(src, wqkv_v.at[i], wqkv_sem.at[i]) for i, src in enumerate((wq, wk, wv))]

    def wo_copy():
        return pltpu.make_async_copy(wo, wo_v, wo_sem)

    def hid_copy(g):
        return pltpu.make_async_copy(hid.at[g], hbuf.at[g], hid_sem.at[g])

    def piece(ref, g, c):
        return ref.at[g, :, pl.ds(pl.multiple_of(c * COLS, COLS), COLS)]

    def p_copy(g, c):
        return pltpu.make_async_remote_copy(piece(hout, g, c), piece(recvp, g, c), p_send.at[g, c], p_recv.at[g, c], device_id=peer, device_id_type=MESH)

    def d_copy(g, c):
        return pltpu.make_async_remote_copy(piece(recvp, g, c), piece(recvd, g, c), d_send.at[g, c], d_recv.at[g, c], device_id=peer, device_id_type=MESH)

    def h_copy(g, c):
        return pltpu.make_async_remote_copy(piece(hout, g, c), piece(hbuf, g, c), h_send.at[g, c], h_recv.at[g, c], device_id=nxt, device_id_type=MESH)

    first = pp == 0
    last = pp == n_pp - 1

    @pl.when(first)
    def _():
        for g in range(n_groups):
            hid_copy(g).start()
    for copy in qkv_copies():
        copy.start()
    for slot in range(SLOTS):
        for copy in kv_copies(slot, slot):
            copy.start()
    wo_copy().start()

    barrier = pltpu.get_barrier_semaphore()
    for other in (peer, nxt, prv):
        pl.semaphore_signal(barrier, inc=1, device_id=other, device_id_type=MESH)
    pl.semaphore_wait(barrier, 3)

    for copy in qkv_copies():
        copy.wait()
    for j in range(n_gu):
        for copy in gu_copies(j):
            copy.start()
    def norm_rows(g, gain_ref, with_partial):
        def body(r, carry):
            rows = pl.ds(pl.multiple_of(r * NORM_ROWS, NORM_ROWS), NORM_ROWS)
            x = hbuf[g, rows, :].astype(F32)
            if with_partial:
                part = (hout[g, rows, :].astype(F32) + recvp[g, rows, :].astype(F32)).astype(BF16)
                x = (x + part.astype(F32)).astype(BF16)
                hbuf[g, rows, :] = x
                x = x.astype(F32)
            inv = lax.rsqrt(jnp.mean(x * x, axis=-1, keepdims=True) + NORM_EPS)
            nbuf[rows, :] = (x * inv * gain_ref[...].astype(F32)).astype(BF16)
            return carry
        lax.fori_loop(0, n_batch // NORM_ROWS, body, 0)

    def attention_phase(g, carry):
        @pl.when(first)
        def _():
            hid_copy(g).wait()

        @pl.when(pp > 0)
        def _():
            for c in range(n_chunk):
                h_copy(g, c).wait_recv()

        norm_rows(g, ga_ref, False)
        cosine = cos_ref[g]
        sine = sin_ref[g]
        half = hd // 2
        for which in range(3):
            for c in range(hw // COLS):
                cols = slice(c * COLS, (c + 1) * COLS)
                prod = jnp.dot(nbuf[...], wqkv_v[which, :, cols], preferred_element_type=F32)
                prod_t = prod.T
                for h in range(COLS // hd):
                    head = c * (COLS // hd) + h
                    a = prod_t[h * hd:h * hd + half]
                    b = prod_t[h * hd + half:(h + 1) * hd]
                    if which < 2:
                        a, b = a * cosine - b * sine, b * cosine + a * sine
                    a, b = a.astype(BF16), b.astype(BF16)
                    if which == 0:
                        qt[head * hd:head * hd + half, :] = a
                        qt[head * hd + half:(head + 1) * hd, :] = b
                    else:
                        dst = knew if which == 1 else vnew
                        dst[g, head, 0:half, :] = a
                        dst[g, head, half:hd, :] = b

        pos = pos_ref[g]
        row_id = lax.broadcasted_iota(jnp.int32, (seq, n_batch), 0)
        hit = row_id == pos
        seen = row_id <= pos

        def head_body(h, inner):
            item = g * heads + h
            slot = lax.rem(item, SLOTS)
            for copy in kv_copies(item, slot):
                copy.wait()
            rows = pl.ds(pl.multiple_of(h * hd, hd), hd)
            q = qt[rows, :].astype(F32)
            fresh = jnp.sum(q * knew[g, h].astype(F32), axis=0, keepdims=True)
            for s in range(seq):
                sc[s:s + 1, :] = jnp.sum(ring[slot, s].astype(F32) * q, axis=0, keepdims=True)
            scores = jnp.where(hit, fresh, sc[...]) * hd ** -0.5
            scores = jnp.where(seen, scores, -jnp.inf)
            top = jnp.max(scores, axis=0, keepdims=True)
            expd = jnp.exp(scores - top)
            probs = (expd / jnp.sum(expd, axis=0, keepdims=True)).astype(BF16).astype(F32)
            sc[...] = jnp.where(hit, 0.0, probs)
            acc = jnp.sum(jnp.where(hit, probs, 0.0), axis=0, keepdims=True) * vnew[g, h].astype(F32)
            for s in range(seq):
                acc = acc + sc[s:s + 1, :] * ring[slot, seq + s].astype(F32)
            qt[rows, :] = acc.astype(BF16)

            @pl.when(item + SLOTS < n_kv)
            def _():
                for copy in kv_copies(item + SLOTS, slot):
                    copy.start()

            @pl.when(item + SLOTS >= n_kv)
            def _():
                for copy in wd_copies(item + SLOTS, slot):
                    copy.start()
            return inner
        lax.fori_loop(0, heads, head_body, 0)

        @pl.when(g == 0)
        def _():
            wo_copy().wait()
        for c in range(hw // COLS):
            cols = slice(c * COLS, (c + 1) * COLS)
            nbuf[:, cols] = qt[cols, :].astype(F32).T.astype(BF16)

        for c in range(n_chunk):
            part = jnp.dot(nbuf[:, 0:hw], wo_v[:, c * COLS:(c + 1) * COLS], preferred_element_type=F32)
            hout[g, :, c * COLS:(c + 1) * COLS] = part.astype(BF16)
        for c in range(n_chunk):
            p_copy(g, c).start()
        return carry

    def mlp_phase(g, carry):
        for c in range(n_chunk):
            p_copy(g, c).wait()
        norm_rows(g, gm_ref, True)

        pair = n_gu // n_chunk

        def gu_body(c, inner):
            tiles = [c * pair + i for i in range(pair)]

            @pl.when(g == 0)
            def _():
                for j in tiles:
                    for copy in gu_copies(j):
                        copy.wait()

            @pl.when(g > 0)
            def _():
                finish_piece(g - 1, c)
            for j in tiles:
                gate = jnp.dot(nbuf[...], wg_v[j], preferred_element_type=F32)
                up = jnp.dot(nbuf[...], wu_v[j], preferred_element_type=F32)
                ubuf[:, pl.ds(pl.multiple_of(j * COLS, COLS), COLS)] = (jax.nn.silu(gate) * up).astype(BF16)
            return inner
        lax.fori_loop(0, n_chunk, gu_body, 0)

        def wd_body(nb, inner):
            item = n_kv + g * n_wd + nb * n_kb
            slot = lax.rem(item, SLOTS)
            for kb in range(n_kb):
                for copy in wd_copies(item + kb, slot + kb):
                    copy.wait()
            acc = None
            for kb in range(n_kb):
                tile = jnp.concatenate([ring[slot + kb, i * deep:(i + 1) * deep].reshape(ROWS, n_batch) for i in range(slabs)], axis=1)
                prod = jnp.dot(ubuf[:, kb * ROWS:(kb + 1) * ROWS], tile, preferred_element_type=F32)
                acc = prod if acc is None else acc + prod
            recvp[g, :, pl.ds(pl.multiple_of(nb * COLS, COLS), COLS)] = acc.astype(BF16)
            d_copy(g, nb).start()

            @pl.when(item + SLOTS < n_items)
            def _():
                for kb in range(n_kb):
                    for copy in wd_copies(item + SLOTS + kb, slot + kb):
                        copy.start()
            return inner
        lax.fori_loop(0, n_chunk, wd_body, 0)
        return carry

    def finish_piece(g, c):
        d_copy(g, c).wait()
        cols = pl.ds(pl.multiple_of(c * COLS, COLS), COLS)
        part = (recvd[g, :, cols].astype(F32) + recvp[g, :, cols].astype(F32)).astype(BF16)
        hout[g, :, cols] = (hbuf[g, :, cols].astype(F32) + part.astype(F32)).astype(BF16)

        @pl.when(jnp.logical_not(last))
        def _():
            h_copy(g, c).start()

    lax.fori_loop(0, n_groups, attention_phase, 0)
    lax.fori_loop(0, n_groups, mlp_phase, 0)
    for c in range(n_chunk):
        finish_piece(n_groups - 1, c)

    @pl.when(jnp.logical_not(last))
    def _():
        for g in range(n_groups):
            for c in range(n_chunk):
                h_copy(g, c).wait_send()


def run_layer(dims, *args):
    n_groups, n_batch, d_model, heads, seq, hd, ff, n_pp, n_tp = dims
    hw = heads * hd
    n_chunk = d_model // COLS
    n_gu = ff // COLS
    assert ROWS * COLS == 2 * seq * hd * n_batch and SLOTS % (ff // ROWS) == 0
    vmem = pl.BlockSpec(memory_space=pltpu.VMEM)
    hbm = pl.BlockSpec(memory_space=pl.ANY)
    dma = pltpu.SemaphoreType.DMA
    return pl.pallas_call(
        functools.partial(layer_kernel, dims),
        out_shape=(jax.ShapeDtypeStruct((n_groups, n_batch, d_model), BF16),
                   jax.ShapeDtypeStruct((n_groups, heads, hd, n_batch), BF16),
                   jax.ShapeDtypeStruct((n_groups, heads, hd, n_batch), BF16)),
        in_specs=[vmem] * 5 + [hbm] * 10,
        out_specs=(vmem, vmem, vmem),
        scratch_shapes=[
            pltpu.VMEM((3, d_model, hw), BF16),
            pltpu.VMEM((hw, d_model), BF16),
            pltpu.VMEM((n_gu, d_model, COLS), BF16),
            pltpu.VMEM((n_gu, d_model, COLS), BF16),
            pltpu.VMEM((SLOTS, 2 * seq, hd, n_batch), BF16),
            pltpu.VMEM((n_groups, n_batch, d_model), BF16),
            pltpu.VMEM((n_groups, n_batch, d_model), BF16),
            pltpu.VMEM((n_groups, n_batch, d_model), BF16),
            pltpu.VMEM((n_batch, d_model), BF16),
            pltpu.VMEM((hw, n_batch), BF16),
            pltpu.VMEM((n_batch, ff), BF16),
            pltpu.VMEM((seq, n_batch), F32),
            dma((n_groups,)), dma((3,)), dma, dma((2, n_gu)), dma((SLOTS, COLS // n_batch)),
            dma((n_groups, n_chunk)), dma((n_groups, n_chunk)), dma((n_groups, n_chunk)),
            dma((n_groups, n_chunk)), dma((n_groups, n_chunk)), dma((n_groups, n_chunk)),
        ],
        compiler_params=pltpu.CompilerParams(collective_id=0, has_side_effects=True, vmem_limit_bytes=67043328),
        name="layer",
    )(*args)


def solution(mesh):
    n_pp = mesh.shape["pp"]
    n_tp = mesh.shape["tp"]
    cache_spec = P("pp", "dp", None, "tp", None, None)
    col_spec = P("pp", None, "tp")
    row_spec = P("pp", "tp", None)
    gain_spec = P("pp", None)
    in_specs = (P("dp", None, None), P("dp", None), cache_spec, cache_spec, gain_spec, col_spec, col_spec, col_spec, row_spec, gain_spec, col_spec, col_spec, row_spec)
    out_specs = (P("dp", None, None), cache_spec, cache_spec)

    def per_device(hidden, positions, key_cache, value_cache, attn_norm, w_query, w_key, w_value, w_out, mlp_norm, w_gate, w_up, w_down):
        _, n_groups, n_batch, heads, seq, hd = key_cache.shape
        d_model = hidden.shape[-1]
        ff = w_gate.shape[-1]
        dims = (n_groups, n_batch, d_model, heads, seq, hd, ff, n_pp, n_tp)
        angles = positions.astype(F32)[:, None, :] * rope_freqs(hd)[None, :, None]
        key_t = jnp.transpose(key_cache[0], (0, 2, 3, 4, 1))
        value_t = jnp.transpose(value_cache[0], (0, 2, 3, 4, 1))
        state, key_new, value_new = run_layer(
            dims, jnp.cos(angles), jnp.sin(angles), positions[:, None, :], attn_norm, mlp_norm, hidden, key_t, value_t,
            w_query[0], w_key[0], w_value[0], w_out[0], w_gate[0], w_up[0], w_down[0].reshape(ff // hd, hd, d_model))

        stage = lax.axis_index("pp")
        from_last = [lax.ppermute(state, "pp", [(n_pp - 1, dst)]) for dst in range(n_pp - 1)]
        final = jnp.where(stage == n_pp - 1, state, sum(from_last[1:], from_last[0]))

        row_hit = jnp.arange(seq, dtype=jnp.int32)[None, None, :, None, None] == positions[:, None, None, None, :]
        key_t = jnp.where(row_hit, key_new[:, :, None], key_t)
        value_t = jnp.where(row_hit, value_new[:, :, None], value_t)
        return final, jnp.transpose(key_t, (0, 4, 1, 2, 3))[None], jnp.transpose(value_t, (0, 4, 1, 2, 3))[None]

    return jax.shard_map(per_device, mesh=mesh, in_specs=in_specs, out_specs=out_specs, check_vma=False)
```

```python
import functools
import math
import jax
import jax.numpy as jnp
from jax import lax
from jax.experimental import pallas as pl
from jax.experimental.pallas import tpu as pltpu
from jax.sharding import PartitionSpec as P

ROPE_THETA = 500000.0
SCALE_FACTOR = 8.0
LOW_FACTOR = 1.0
HIGH_FACTOR = 4.0
ORIG_CONTEXT = 8192.0
NORM_EPS = 1e-5
MESH = pl.DeviceIdType.MESH
F32 = jnp.float32
BF16 = jnp.bfloat16

COLS = 512
ROWS = 1024
SLOTS = 8
NORM_ROWS = 32
KEEP_SLOTS = 16
WRITE_SLOTS = 24


def rope_freqs(head_dim):
    freq_index = jnp.arange(head_dim // 2, dtype=jnp.float32)
    base_freq = ROPE_THETA ** (-2.0 * freq_index / head_dim)
    wave_len = 2.0 * math.pi / base_freq
    smooth_t = (ORIG_CONTEXT / wave_len - LOW_FACTOR) / (HIGH_FACTOR - LOW_FACTOR)
    mixed_freq = (1.0 - smooth_t) * base_freq / SCALE_FACTOR + smooth_t * base_freq
    long_freq = jnp.where(wave_len > ORIG_CONTEXT / LOW_FACTOR, base_freq / SCALE_FACTOR, mixed_freq)
    return jnp.where(wave_len < ORIG_CONTEXT / HIGH_FACTOR, base_freq, long_freq)


def layer_kernel(dims, after, cos_ref, sin_ref, pos_ref, ga_ref, gm_ref, hid, kc, vc, wq, wk, wv, wo, wg, wu, wd,
                 hout, knew, vnew,
                 wqkv_v, wo_v, wg_v, wu_v, ring, hbuf, recvp, recvd, nbuf, qt, ubuf, sc,
                 hid_sem, wqkv_sem, wo_sem, gu_sem, ring_sem,
                 p_send, p_recv, d_send, d_recv, h_send, h_recv):
    n_groups, n_batch, d_model, heads, seq, hd, ff, n_pp, n_tp = dims
    hw = heads * hd
    n_chunk = d_model // COLS
    n_gu = ff // COLS
    n_kb = ff // ROWS
    pp = lax.axis_index("pp")
    tp = lax.axis_index("tp")
    peer = {"tp": lax.rem(tp + 1, n_tp)}
    nxt = {"pp": lax.rem(pp + 1, n_pp)}
    prv = {"pp": lax.rem(pp + n_pp - 1, n_pp)}

    n_kv = n_groups * heads
    n_wd = n_chunk * n_kb
    n_items = n_kv + n_groups * n_wd
    slabs = COLS // n_batch
    deep = ROWS // hd

    def kv_copies(item, slot):
        g = item // heads
        h = lax.rem(item, heads)
        return (pltpu.make_async_copy(kc.at[g, h], ring.at[slot, pl.ds(0, seq)], ring_sem.at[slot, 0]),
                pltpu.make_async_copy(vc.at[g, h], ring.at[slot, pl.ds(seq, seq)], ring_sem.at[slot, 1]))

    def wd_copies(item, slot):
        tile = lax.rem(item - n_kv, n_wd)
        nb = tile // n_kb
        kb = lax.rem(tile, n_kb)
        return [pltpu.make_async_copy(
            wd.at[pl.ds(kb * deep, deep), :, pl.ds(pl.multiple_of(nb * COLS + i * n_batch, n_batch), n_batch)],
            ring.at[slot, pl.ds(i * deep, deep)], ring_sem.at[slot, i]) for i in range(slabs)]

    def gu_copies(j):
        cols = pl.ds(pl.multiple_of(j * COLS, COLS), COLS)
        return (pltpu.make_async_copy(wg.at[:, cols], wg_v.at[j], gu_sem.at[0, j]),
                pltpu.make_async_copy(wu.at[:, cols], wu_v.at[j], gu_sem.at[1, j]))

    def qkv_copies():
        return [pltpu.make_async_copy(src, wqkv_v.at[i], wqkv_sem.at[i]) for i, src in enumerate((wq, wk, wv))]

    def wo_copy():
        return pltpu.make_async_copy(wo, wo_v, wo_sem)

    def hid_copy(g):
        return pltpu.make_async_copy(hid.at[g], hbuf.at[g], hid_sem.at[g])

    def piece(ref, g, c):
        return ref.at[g, :, pl.ds(pl.multiple_of(c * COLS, COLS), COLS)]

    def p_copy(g, c):
        return pltpu.make_async_remote_copy(piece(hout, g, c), piece(recvp, g, c), p_send.at[g, c], p_recv.at[g, c], device_id=peer, device_id_type=MESH)

    def d_copy(g, c):
        return pltpu.make_async_remote_copy(piece(recvp, g, c), piece(recvd, g, c), d_send.at[g, c], d_recv.at[g, c], device_id=peer, device_id_type=MESH)

    def h_copy(g, c):
        return pltpu.make_async_remote_copy(piece(hout, g, c), piece(hbuf, g, c), h_send.at[g, c], h_recv.at[g, c], device_id=nxt, device_id_type=MESH)

    first = pp == 0
    last = pp == n_pp - 1

    @pl.when(first)
    def _():
        for g in range(n_groups):
            hid_copy(g).start()
    for copy in qkv_copies():
        copy.start()

    def start_kv_wo():
        for slot in range(SLOTS):
            for copy in kv_copies(slot, slot):
                copy.start()
        wo_copy().start()

    @pl.when(pp > 0)
    def _():
        start_kv_wo()
        for j in range(n_gu):
            for copy in gu_copies(j):
                copy.start()

    barrier = pltpu.get_barrier_semaphore()
    pl.semaphore_signal(barrier, inc=1, device_id=peer, device_id_type=MESH)

    @pl.when(jnp.logical_not(last))
    def _():
        pl.semaphore_signal(barrier, inc=1, device_id=nxt, device_id_type=MESH)

    @pl.when(pp > 0)
    def _():
        pl.semaphore_signal(barrier, inc=1, device_id=prv, device_id_type=MESH)
    ends = jnp.logical_or(first, last)

    @pl.when(ends)
    def _():
        pl.semaphore_wait(barrier, 2)

    @pl.when(jnp.logical_not(ends))
    def _():
        pl.semaphore_wait(barrier, 3)

    def norm_rows(g, gain_ref, with_partial):
        def body(r, carry):
            rows = pl.ds(pl.multiple_of(r * NORM_ROWS, NORM_ROWS), NORM_ROWS)
            x = hbuf[g, rows, :].astype(F32)
            if with_partial:
                part = (hout[g, rows, :].astype(F32) + recvp[g, rows, :].astype(F32)).astype(BF16)
                x = (x + part.astype(F32)).astype(BF16)
                hbuf[g, rows, :] = x
                x = x.astype(F32)
            inv = lax.rsqrt(jnp.mean(x * x, axis=-1, keepdims=True) + NORM_EPS)
            nbuf[rows, :] = (x * inv * gain_ref[...].astype(F32)).astype(BF16)
            return carry
        lax.fori_loop(0, n_batch // NORM_ROWS, body, 0)

    def attention_phase(g, carry):
        @pl.when(first)
        def _():
            hid_copy(g).wait()

        @pl.when(pp > 0)
        def _():
            for c in range(n_chunk):
                h_copy(g, c).wait_recv()

        norm_rows(g, ga_ref, False)
        cosine = cos_ref[g]
        sine = sin_ref[g]
        half = hd // 2
        for which in range(3):
            @pl.when(g == 0)
            def _():
                qkv_copies()[which].wait()
            if which == 0:
                @pl.when(jnp.logical_and(first, g == 0))
                def _():
                    start_kv_wo()
            for c in range(hw // COLS):
                cols = slice(c * COLS, (c + 1) * COLS)
                prod = jnp.dot(nbuf[...], wqkv_v[which, :, cols], preferred_element_type=F32)
                prod_t = prod.T
                for h in range(COLS // hd):
                    head = c * (COLS // hd) + h
                    a = prod_t[h * hd:h * hd + half]
                    b = prod_t[h * hd + half:(h + 1) * hd]
                    if which < 2:
                        a, b = a * cosine - b * sine, b * cosine + a * sine
                    a, b = a.astype(BF16), b.astype(BF16)
                    if which == 0:
                        qt[head * hd:head * hd + half, :] = a
                        qt[head * hd + half:(head + 1) * hd, :] = b
                    else:
                        dst = knew if which == 1 else vnew
                        dst[g, head, 0:half, :] = a
                        dst[g, head, half:hd, :] = b

        pos = pos_ref[g]
        row_id = lax.broadcasted_iota(jnp.int32, (seq, n_batch), 0)
        hit = row_id == pos
        seen = row_id <= pos

        def head_body(h, inner):
            item = g * heads + h
            slot = lax.rem(item, SLOTS)
            for copy in kv_copies(item, slot):
                copy.wait()
            rows = pl.ds(pl.multiple_of(h * hd, hd), hd)
            q = qt[rows, :].astype(F32)
            fresh = jnp.sum(q * knew[g, h].astype(F32), axis=0, keepdims=True)
            for s in range(seq):
                sc[s:s + 1, :] = jnp.sum(ring[slot, s].astype(F32) * q, axis=0, keepdims=True)
            scores = jnp.where(hit, fresh, sc[...]) * hd ** -0.5
            scores = jnp.where(seen, scores, -jnp.inf)
            top = jnp.max(scores, axis=0, keepdims=True)
            expd = jnp.exp(scores - top)
            probs = (expd / jnp.sum(expd, axis=0, keepdims=True)).astype(BF16).astype(F32)
            sc[...] = jnp.where(hit, 0.0, probs)
            acc = jnp.sum(jnp.where(hit, probs, 0.0), axis=0, keepdims=True) * vnew[g, h].astype(F32)
            for s in range(seq):
                acc = acc + sc[s:s + 1, :] * ring[slot, seq + s].astype(F32)
            qt[rows, :] = acc.astype(BF16)

            @pl.when(item + SLOTS < n_kv)
            def _():
                for copy in kv_copies(item + SLOTS, slot):
                    copy.start()

            @pl.when(jnp.logical_and(first, lax.rem(item, SLOTS) == SLOTS - 1))
            def _():
                for copy in gu_copies(item // SLOTS):
                    copy.start()

            @pl.when(item + SLOTS >= n_kv)
            def _():
                for copy in wd_copies(item + SLOTS, slot):
                    copy.start()
            return inner
        lax.fori_loop(0, heads, head_body, 0)

        @pl.when(g == 0)
        def _():
            wo_copy().wait()
        for c in range(hw // COLS):
            cols = slice(c * COLS, (c + 1) * COLS)
            nbuf[:, cols] = qt[cols, :].astype(F32).T.astype(BF16)

        for c in range(n_chunk):
            part = jnp.dot(nbuf[:, 0:hw], wo_v[:, c * COLS:(c + 1) * COLS], preferred_element_type=F32)
            hout[g, :, c * COLS:(c + 1) * COLS] = part.astype(BF16)
        for c in range(n_chunk):
            p_copy(g, c).start()
        return carry

    def mlp_phase(g, carry):
        @pl.when(jnp.logical_and(first, g == 0))
        def _():
            for j in range(n_kv // SLOTS, n_gu):
                for copy in gu_copies(j):
                    copy.start()

        for c in range(n_chunk):
            p_copy(g, c).wait()
        norm_rows(g, gm_ref, True)

        pair = n_gu // n_chunk

        def gu_body(c, inner):
            tiles = [c * pair + i for i in range(pair)]

            @pl.when(g == 0)
            def _():
                for j in tiles:
                    for copy in gu_copies(j):
                        copy.wait()

            @pl.when(g > 0)
            def _():
                finish_piece(g - 1, c)
            for j in tiles:
                gate = jnp.dot(nbuf[...], wg_v[j], preferred_element_type=F32)
                up = jnp.dot(nbuf[...], wu_v[j], preferred_element_type=F32)
                ubuf[:, pl.ds(pl.multiple_of(j * COLS, COLS), COLS)] = (jax.nn.silu(gate) * up).astype(BF16)
            return inner
        lax.fori_loop(0, n_chunk, gu_body, 0)

        def wd_body(nb, inner):
            item = n_kv + g * n_wd + nb * n_kb
            slot = lax.rem(item, SLOTS)
            for kb in range(n_kb):
                for copy in wd_copies(item + kb, slot + kb):
                    copy.wait()
            acc = None
            for kb in range(n_kb):
                tile = jnp.concatenate([ring[slot + kb, i * deep:(i + 1) * deep].reshape(ROWS, n_batch) for i in range(slabs)], axis=1)
                prod = jnp.dot(ubuf[:, kb * ROWS:(kb + 1) * ROWS], tile, preferred_element_type=F32)
                acc = prod if acc is None else acc + prod
            recvp[g, :, pl.ds(pl.multiple_of(nb * COLS, COLS), COLS)] = acc.astype(BF16)
            d_copy(g, nb).start()

            @pl.when(item + SLOTS < n_items)
            def _():
                for kb in range(n_kb):
                    for copy in wd_copies(item + SLOTS + kb, slot + kb):
                        copy.start()
            return inner
        lax.fori_loop(0, n_chunk, wd_body, 0)
        return carry

    def finish_piece(g, c):
        d_copy(g, c).wait()
        cols = pl.ds(pl.multiple_of(c * COLS, COLS), COLS)
        part = (recvd[g, :, cols].astype(F32) + recvp[g, :, cols].astype(F32)).astype(BF16)
        hout[g, :, cols] = (hbuf[g, :, cols].astype(F32) + part.astype(F32)).astype(BF16)

        @pl.when(jnp.logical_not(last))
        def _():
            h_copy(g, c).start()

    lax.fori_loop(0, n_groups, attention_phase, 0)
    lax.fori_loop(0, n_groups, mlp_phase, 0)
    for c in range(n_chunk):
        finish_piece(n_groups - 1, c)

    @pl.when(jnp.logical_not(last))
    def _():
        for g in range(n_groups):
            for c in range(n_chunk):
                h_copy(g, c).wait_send()


def run_layer(dims, *args):
    n_groups, n_batch, d_model, heads, seq, hd, ff, n_pp, n_tp = dims
    hw = heads * hd
    n_chunk = d_model // COLS
    n_gu = ff // COLS
    assert ROWS * COLS == 2 * seq * hd * n_batch and SLOTS % (ff // ROWS) == 0
    vmem = pl.BlockSpec(memory_space=pltpu.VMEM)
    hbm = pl.BlockSpec(memory_space=pl.ANY)
    dma = pltpu.SemaphoreType.DMA
    return pl.pallas_call(
        functools.partial(layer_kernel, dims),
        out_shape=(jax.ShapeDtypeStruct((n_groups, n_batch, d_model), BF16),
                   jax.ShapeDtypeStruct((n_groups, heads, hd, n_batch), BF16),
                   jax.ShapeDtypeStruct((n_groups, heads, hd, n_batch), BF16)),
        in_specs=[hbm] + [vmem] * 5 + [hbm] * 10,
        out_specs=(vmem, vmem, vmem),
        scratch_shapes=[
            pltpu.VMEM((3, d_model, hw), BF16),
            pltpu.VMEM((hw, d_model), BF16),
            pltpu.VMEM((n_gu, d_model, COLS), BF16),
            pltpu.VMEM((n_gu, d_model, COLS), BF16),
            pltpu.VMEM((SLOTS, 2 * seq, hd, n_batch), BF16),
            pltpu.VMEM((n_groups, n_batch, d_model), BF16),
            pltpu.VMEM((n_groups, n_batch, d_model), BF16),
            pltpu.VMEM((n_groups, n_batch, d_model), BF16),
            pltpu.VMEM((n_batch, d_model), BF16),
            pltpu.VMEM((hw, n_batch), BF16),
            pltpu.VMEM((n_batch, ff), BF16),
            pltpu.VMEM((seq, n_batch), F32),
            dma((n_groups,)), dma((3,)), dma, dma((2, n_gu)), dma((SLOTS, COLS // n_batch)),
            dma((n_groups, n_chunk)), dma((n_groups, n_chunk)), dma((n_groups, n_chunk)),
            dma((n_groups, n_chunk)), dma((n_groups, n_chunk)), dma((n_groups, n_chunk)),
        ],
        compiler_params=pltpu.CompilerParams(collective_id=0, has_side_effects=True, vmem_limit_bytes=67043328),
        name="layer",
    )(*args)


def keep_kernel(dims, pos, kc, vc, kout, vout, todo, kb, vb, flags, in_sem, out_sem):
    n_groups, n_batch, _, heads, seq, _, _, n_pp, _ = dims
    n_slab = n_groups * seq
    n_items = n_groups * heads
    ahead = KEEP_SLOTS // 2
    last = lax.axis_index("pp") == n_pp - 1

    def loads(i):
        slot = lax.rem(i, KEEP_SLOTS)
        g, h = i // heads, lax.rem(i, heads)
        return (pltpu.make_async_copy(kc.at[g, h], kb.at[slot], in_sem.at[0, slot]),
                pltpu.make_async_copy(vc.at[g, h], vb.at[slot], in_sem.at[1, slot]))

    def stores(i):
        slot = lax.rem(i, KEEP_SLOTS)
        g, h = i // heads, lax.rem(i, heads)
        return (pltpu.make_async_copy(kb.at[slot], kout.at[g, h], out_sem.at[0, slot]),
                pltpu.make_async_copy(vb.at[slot], vout.at[g, h], out_sem.at[1, slot]))

    @pl.when(jnp.logical_not(last))
    def _():
        todo[0] = n_slab

        def number(i, carry):
            todo[i + 1] = i
            return carry
        lax.fori_loop(0, n_slab, number, 0)

    @pl.when(last)
    def _():
        for i in range(ahead):
            for copy in loads(i):
                copy.start()

        def clear(i, carry):
            flags[i] = 0
            todo[i + 1] = 0
            return carry
        lax.fori_loop(0, n_slab, clear, 0)
        for g in range(n_groups):
            def mark(b, carry):
                flags[g * seq + pos[g, b]] = 1
                return carry
            lax.fori_loop(0, n_batch, mark, 0)

        def pick(i, count):
            hit = flags[i]

            @pl.when(hit == 1)
            def _():
                todo[count + 1] = i
            return count + hit
        todo[0] = lax.fori_loop(0, n_slab, pick, jnp.int32(0))

        def body(i, carry):
            for copy in loads(i):
                copy.wait()
            for copy in stores(i):
                copy.start()

            @pl.when(i + ahead < n_items)
            def _():
                @pl.when(i >= ahead)
                def _():
                    for copy in stores(i - ahead):
                        copy.wait()
                for copy in loads(i + ahead):
                    copy.start()
            return carry
        lax.fori_loop(0, n_items, body, 0)
        for i in range(n_items - 2 * ahead, n_items):
            for copy in stores(i):
                copy.wait()


def keep_old(dims, positions, key_t, value_t):
    n_groups, n_batch, _, heads, seq, hd, _, _, _ = dims
    hbm = pl.BlockSpec(memory_space=pl.ANY)
    smem = pl.BlockSpec(memory_space=pltpu.SMEM)
    dma = pltpu.SemaphoreType.DMA
    return pl.pallas_call(
        functools.partial(keep_kernel, dims),
        out_shape=(jax.ShapeDtypeStruct(key_t.shape, BF16), jax.ShapeDtypeStruct(value_t.shape, BF16),
                   jax.ShapeDtypeStruct((n_groups * seq + 1,), jnp.int32)),
        in_specs=[smem, hbm, hbm],
        out_specs=(hbm, hbm, smem),
        scratch_shapes=[
            pltpu.VMEM((KEEP_SLOTS, seq, hd, n_batch), BF16),
            pltpu.VMEM((KEEP_SLOTS, seq, hd, n_batch), BF16),
            pltpu.SMEM((n_groups * seq,), jnp.int32),
            dma((2, KEEP_SLOTS)), dma((2, KEEP_SLOTS)),
        ],
        compiler_params=pltpu.CompilerParams(vmem_limit_bytes=40 * 2**20),
        name="cache_keep",
    )(positions, key_t, value_t)


def write_kernel(dims, todo, pos_ref, knew, vnew, kc, vc, kold, vold, kout, vout, kb, vb, in_sem, out_sem):
    _, _, _, _, seq, _, _, _, _ = dims
    ahead = WRITE_SLOTS // 2
    count = todo[0]

    def place(i):
        entry = todo[i + 1]
        return entry // seq, lax.rem(entry, seq), lax.rem(i, WRITE_SLOTS)

    def loads(i):
        g, s, slot = place(i)
        return (pltpu.make_async_copy(kc.at[g, :, s], kb.at[slot], in_sem.at[0, slot]),
                pltpu.make_async_copy(vc.at[g, :, s], vb.at[slot], in_sem.at[1, slot]))

    def stores(i):
        g, s, slot = place(i)
        return (pltpu.make_async_copy(kb.at[slot], kout.at[g, :, s], out_sem.at[0, slot]),
                pltpu.make_async_copy(vb.at[slot], vout.at[g, :, s], out_sem.at[1, slot]))

    for i in range(ahead):
        @pl.when(i < count)
        def _():
            for copy in loads(i):
                copy.start()

    def body(i, carry):
        g, s, slot = place(i)
        for copy in loads(i):
            copy.wait()
        hit = (pos_ref[g] == s)[None]
        for new, buf in ((knew, kb), (vnew, vb)):
            buf[slot] = jnp.where(hit, new[g].astype(F32), buf[slot].astype(F32)).astype(BF16)
        for copy in stores(i):
            copy.start()

        @pl.when(i + ahead < count)
        def _():
            @pl.when(i >= ahead)
            def _():
                for copy in stores(i - ahead):
                    copy.wait()
            for copy in loads(i + ahead):
                copy.start()
        return carry
    lax.fori_loop(0, count, body, 0)

    def drain(i, carry):
        for copy in stores(i):
            copy.wait()
        return carry
    lax.fori_loop(jnp.maximum(count - 2 * ahead, 0), count, drain, 0)


def write_new(dims, todo, pos, key_new, value_new, key_t, value_t, key_old, value_old):
    n_groups, n_batch, _, heads, seq, hd, _, _, _ = dims
    hbm = pl.BlockSpec(memory_space=pl.ANY)
    vmem = pl.BlockSpec(memory_space=pltpu.VMEM)
    smem = pl.BlockSpec(memory_space=pltpu.SMEM)
    dma = pltpu.SemaphoreType.DMA
    return pl.pallas_call(
        functools.partial(write_kernel, dims),
        out_shape=(jax.ShapeDtypeStruct(key_t.shape, BF16), jax.ShapeDtypeStruct(value_t.shape, BF16)),
        in_specs=[smem, vmem, vmem, vmem, hbm, hbm, hbm, hbm],
        out_specs=(hbm, hbm),
        scratch_shapes=[
            pltpu.VMEM((WRITE_SLOTS, heads, hd, n_batch), BF16),
            pltpu.VMEM((WRITE_SLOTS, heads, hd, n_batch), BF16),
            dma((2, WRITE_SLOTS)), dma((2, WRITE_SLOTS)),
        ],
        input_output_aliases={6: 0, 7: 1},
        compiler_params=pltpu.CompilerParams(vmem_limit_bytes=40 * 2**20),
        cost_estimate=pl.CostEstimate(flops=n_groups * n_batch * heads * seq * hd * 40, bytes_accessed=8 * key_t.size, transcendentals=0),
        name="cache_write",
    )(todo, pos, key_new, value_new, key_t, value_t, key_old, value_old)


def solution(mesh):
    n_pp = mesh.shape["pp"]
    n_tp = mesh.shape["tp"]
    cache_spec = P("pp", "dp", None, "tp", None, None)
    col_spec = P("pp", None, "tp")
    row_spec = P("pp", "tp", None)
    gain_spec = P("pp", None)
    in_specs = (P("dp", None, None), P("dp", None), cache_spec, cache_spec, gain_spec, col_spec, col_spec, col_spec, row_spec, gain_spec, col_spec, col_spec, row_spec)
    out_specs = (P("dp", None, None), cache_spec, cache_spec)

    def per_device(hidden, positions, key_cache, value_cache, attn_norm, w_query, w_key, w_value, w_out, mlp_norm, w_gate, w_up, w_down):
        _, n_groups, n_batch, heads, seq, hd = key_cache.shape
        d_model = hidden.shape[-1]
        ff = w_gate.shape[-1]
        dims = (n_groups, n_batch, d_model, heads, seq, hd, ff, n_pp, n_tp)
        angles = positions.astype(F32)[:, None, :] * rope_freqs(hd)[None, :, None]
        key_t = jnp.transpose(key_cache[0], (0, 2, 3, 4, 1))
        value_t = jnp.transpose(value_cache[0], (0, 2, 3, 4, 1))
        pos = positions[:, None, :]
        key_old, value_old, todo = keep_old(dims, positions, key_t, value_t)
        state, key_new, value_new = run_layer(
            dims, todo, jnp.cos(angles), jnp.sin(angles), pos, attn_norm, mlp_norm, hidden, key_t, value_t,
            w_query[0], w_key[0], w_value[0], w_out[0], w_gate[0], w_up[0], w_down[0].reshape(ff // hd, hd, d_model))

        stage = lax.axis_index("pp")
        from_last = [lax.ppermute(state, "pp", [(n_pp - 1, dst)]) for dst in range(1, n_pp - 1)]
        key_t, value_t = write_new(dims, todo, pos, key_new, value_new, key_t, value_t, key_old, value_old)
        from_last[0], key_t = lax.optimization_barrier((from_last[0], key_t))
        from_last.append(lax.ppermute(from_last[0], "pp", [(1, 0)]))
        final = jnp.where(stage == n_pp - 1, state, sum(from_last[1:], from_last[0]))
        return final, jnp.transpose(key_t, (0, 4, 1, 2, 3))[None], jnp.transpose(value_t, (0, 4, 1, 2, 3))[None]

    return jax.shard_map(per_device, mesh=mesh, in_specs=in_specs, out_specs=out_specs, check_vma=False)
```

```python
import functools
import math
import jax
import jax.numpy as jnp
from jax import lax
from jax.experimental import pallas as pl
from jax.experimental.pallas import tpu as pltpu
from jax.sharding import PartitionSpec as P

ROPE_THETA = 500000.0
SCALE_FACTOR = 8.0
LOW_FACTOR = 1.0
HIGH_FACTOR = 4.0
ORIG_CONTEXT = 8192.0
NORM_EPS = 1e-5
MESH = pl.DeviceIdType.MESH
F32 = jnp.float32
BF16 = jnp.bfloat16

COLS = 512
SLOTS = 8
NORM_ROWS = 32
KEEP_SLOTS = 16
WRITE_SLOTS = 24


def rope_freqs(head_dim):
    freq_index = jnp.arange(head_dim // 2, dtype=jnp.float32)
    base_freq = ROPE_THETA ** (-2.0 * freq_index / head_dim)
    wave_len = 2.0 * math.pi / base_freq
    smooth_t = (ORIG_CONTEXT / wave_len - LOW_FACTOR) / (HIGH_FACTOR - LOW_FACTOR)
    mixed_freq = (1.0 - smooth_t) * base_freq / SCALE_FACTOR + smooth_t * base_freq
    long_freq = jnp.where(wave_len > ORIG_CONTEXT / LOW_FACTOR, base_freq / SCALE_FACTOR, mixed_freq)
    return jnp.where(wave_len < ORIG_CONTEXT / HIGH_FACTOR, base_freq, long_freq)


def layer_kernel(dims, after, cos_ref, sin_ref, pos_ref, ga_ref, gm_ref, hid, kc, vc, wq, wk, wv, wo, wg, wu, wd,
                 hout, knew, vnew,
                 wmix, wg_v, wu_v, ring, hbuf, recvp, recvd, nbuf, qt, ubuf, sc,
                 hid_sem, wqkv_sem, wo_sem, wd_sem, gu_sem, ring_sem,
                 p_send, p_recv, d_send, d_recv, h_send, h_recv):
    n_groups, n_batch, d_model, heads, seq, hd, ff, n_pp, n_tp = dims
    hw = heads * hd
    n_chunk = d_model // COLS
    n_gu = ff // COLS
    n_half = d_model // hw
    n_deep = ff // d_model
    pp = lax.axis_index("pp")
    tp = lax.axis_index("tp")
    peer = {"tp": lax.rem(tp + 1, n_tp)}
    nxt = {"pp": lax.rem(pp + 1, n_pp)}
    prv = {"pp": lax.rem(pp + n_pp - 1, n_pp)}

    n_kv = n_groups * heads

    def kv_copies(item, slot):
        g = item // heads
        h = lax.rem(item, heads)
        return (pltpu.make_async_copy(kc.at[g, h], ring.at[slot, pl.ds(0, seq)], ring_sem.at[slot, 0]),
                pltpu.make_async_copy(vc.at[g, h], ring.at[slot, pl.ds(seq, seq)], ring_sem.at[slot, 1]))

    def wd_copy(i):
        return pltpu.make_async_copy(wd.at[pl.ds(i % n_deep * d_model, d_model), pl.ds(i // n_deep * hw, hw)], wmix.at[i], wd_sem.at[i])

    def gu_copies(j):
        cols = pl.ds(pl.multiple_of(j * COLS, COLS), COLS)
        return (pltpu.make_async_copy(wg.at[:, cols], wg_v.at[j], gu_sem.at[0, j]),
                pltpu.make_async_copy(wu.at[:, cols], wu_v.at[j], gu_sem.at[1, j]))

    def qkv_copies():
        return [pltpu.make_async_copy(src, wmix.at[i], wqkv_sem.at[i]) for i, src in enumerate((wq, wk, wv))]

    def wo_copies():
        return [pltpu.make_async_copy(wo.at[:, pl.ds(i * hw, hw)], wmix.at[3, pl.ds(i * hw, hw)], wo_sem.at[i]) for i in range(n_half)]

    def hid_copy(g):
        return pltpu.make_async_copy(hid.at[g], hbuf.at[g], hid_sem.at[g])

    def piece(ref, g, c):
        return ref.at[g, :, pl.ds(pl.multiple_of(c * COLS, COLS), COLS)]

    def p_copy(g, c):
        return pltpu.make_async_remote_copy(piece(hout, g, c), piece(recvp, g, c), p_send.at[g, c], p_recv.at[g, c], device_id=peer, device_id_type=MESH)

    def d_copy(g, c):
        return pltpu.make_async_remote_copy(piece(recvp, g, c), piece(recvd, g, c), d_send.at[g, c], d_recv.at[g, c], device_id=peer, device_id_type=MESH)

    def h_copy(g, c):
        return pltpu.make_async_remote_copy(piece(hout, g, c), piece(hbuf, g, c), h_send.at[g, c], h_recv.at[g, c], device_id=nxt, device_id_type=MESH)

    first = pp == 0
    last = pp == n_pp - 1

    @pl.when(first)
    def _():
        for g in range(n_groups):
            hid_copy(g).start()
    for copy in qkv_copies():
        copy.start()

    def start_kv_wo():
        for slot in range(SLOTS):
            for copy in kv_copies(slot, slot):
                copy.start()
        for copy in wo_copies():
            copy.start()

    @pl.when(pp > 0)
    def _():
        start_kv_wo()
        for j in range(n_gu):
            for copy in gu_copies(j):
                copy.start()

    barrier = pltpu.get_barrier_semaphore()
    pl.semaphore_signal(barrier, inc=1, device_id=peer, device_id_type=MESH)

    @pl.when(jnp.logical_not(last))
    def _():
        pl.semaphore_signal(barrier, inc=1, device_id=nxt, device_id_type=MESH)

    @pl.when(pp > 0)
    def _():
        pl.semaphore_signal(barrier, inc=1, device_id=prv, device_id_type=MESH)
    ends = jnp.logical_or(first, last)

    @pl.when(ends)
    def _():
        pl.semaphore_wait(barrier, 2)

    @pl.when(jnp.logical_not(ends))
    def _():
        pl.semaphore_wait(barrier, 3)

    def norm_rows(g, gain_ref, with_partial):
        def body(r, carry):
            rows = pl.ds(pl.multiple_of(r * NORM_ROWS, NORM_ROWS), NORM_ROWS)
            x = hbuf[g, rows, :].astype(F32)
            if with_partial:
                part = (hout[g, rows, :].astype(F32) + recvp[g, rows, :].astype(F32)).astype(BF16)
                x = (x + part.astype(F32)).astype(BF16)
                hbuf[g, rows, :] = x
                x = x.astype(F32)
            inv = lax.rsqrt(jnp.mean(x * x, axis=-1, keepdims=True) + NORM_EPS)
            nbuf[rows, :] = (x * inv * gain_ref[...].astype(F32)).astype(BF16)
            return carry
        lax.fori_loop(0, n_batch // NORM_ROWS, body, 0)

    def attention_phase(g, carry):
        @pl.when(first)
        def _():
            hid_copy(g).wait()

        @pl.when(pp > 0)
        def _():
            for c in range(n_chunk):
                h_copy(g, c).wait_recv()

        norm_rows(g, ga_ref, False)
        cosine = cos_ref[g]
        sine = sin_ref[g]
        half = hd // 2

        @pl.when(g == 0)
        def _():
            for i, copy in enumerate(qkv_copies()):
                copy.wait()
                if i == 0:
                    pl.when(first)(start_kv_wo)

        for which in range(3):
            for c in range(hw // COLS):
                cols = slice(c * COLS, (c + 1) * COLS)
                prod_t = jnp.dot(nbuf[...], wmix[which, :, cols], preferred_element_type=F32).T
                for i in range(COLS // hd):
                    head = c * (COLS // hd) + i
                    a = prod_t[i * hd:i * hd + half]
                    b = prod_t[i * hd + half:(i + 1) * hd]
                    if which < 2:
                        a, b = a * cosine - b * sine, b * cosine + a * sine
                    both = jnp.concatenate([a, b], axis=0).astype(BF16)
                    if which == 0:
                        qt[head * hd:(head + 1) * hd, :] = both
                    else:
                        dst = knew if which == 1 else vnew
                        dst[g, head] = both

        @pl.when(g == n_groups - 1)
        def _():
            for i in range(3):
                wd_copy(i).start()

        pos = pos_ref[g]
        row_id = lax.broadcasted_iota(jnp.int32, (seq, n_batch), 0)
        hit = row_id == pos
        seen = row_id <= pos

        def head_body(h, inner):
            item = g * heads + h
            slot = lax.rem(item, SLOTS)
            for copy in kv_copies(item, slot):
                copy.wait()
            rows = pl.ds(pl.multiple_of(h * hd, hd), hd)
            q = qt[rows, :].astype(F32)
            fresh = jnp.sum(q * knew[g, h].astype(F32), axis=0, keepdims=True)
            for s in range(seq):
                sc[s:s + 1, :] = jnp.sum(ring[slot, s].astype(F32) * q, axis=0, keepdims=True)
            scores = jnp.where(hit, fresh, sc[...]) * hd ** -0.5
            scores = jnp.where(seen, scores, -jnp.inf)
            top = jnp.max(scores, axis=0, keepdims=True)
            expd = jnp.exp(scores - top)
            probs = (expd / jnp.sum(expd, axis=0, keepdims=True)).astype(BF16).astype(F32)
            sc[...] = jnp.where(hit, 0.0, probs)
            acc = jnp.sum(jnp.where(hit, probs, 0.0), axis=0, keepdims=True) * vnew[g, h].astype(F32)
            for s in range(seq):
                acc = acc + sc[s:s + 1, :] * ring[slot, seq + s].astype(F32)
            qt[rows, :] = acc.astype(BF16)

            @pl.when(item + SLOTS < n_kv)
            def _():
                for copy in kv_copies(item + SLOTS, slot):
                    copy.start()

            @pl.when(jnp.logical_and(first, lax.rem(item, SLOTS) == SLOTS - 1))
            def _():
                for copy in gu_copies(item // SLOTS):
                    copy.start()
            return inner
        lax.fori_loop(0, heads, head_body, 0)

        @pl.when(g == 0)
        def _():
            for copy in wo_copies():
                copy.wait()
        for c in range(hw // COLS):
            cols = slice(c * COLS, (c + 1) * COLS)
            nbuf[:, cols] = qt[cols, :].astype(F32).T.astype(BF16)

        for c in range(n_chunk):
            at, col = divmod(c * COLS, hw)
            part = jnp.dot(nbuf[:, 0:hw], wmix[3, at * hw:(at + 1) * hw, col:col + COLS], preferred_element_type=F32)
            hout[g, :, c * COLS:(c + 1) * COLS] = part.astype(BF16)
        for c in range(n_chunk):
            p_copy(g, c).start()

        @pl.when(g == n_groups - 1)
        def _():
            wd_copy(3).start()
        return carry

    def mlp_phase(g, carry):
        @pl.when(jnp.logical_and(first, g == 0))
        def _():
            for j in range(n_kv // SLOTS, n_gu):
                for copy in gu_copies(j):
                    copy.start()

        for c in range(n_chunk):
            p_copy(g, c).wait()
        norm_rows(g, gm_ref, True)

        pair = n_gu // n_chunk

        def gu_body(c, inner):
            tiles = [c * pair + i for i in range(pair)]

            @pl.when(g == 0)
            def _():
                for j in tiles:
                    for copy in gu_copies(j):
                        copy.wait()

            @pl.when(g > 0)
            def _():
                finish_piece(g - 1, c)
            for j in tiles:
                gate = jnp.dot(nbuf[...], wg_v[j], preferred_element_type=F32)
                up = jnp.dot(nbuf[...], wu_v[j], preferred_element_type=F32)
                ubuf[:, pl.ds(pl.multiple_of(j * COLS, COLS), COLS)] = (jax.nn.silu(gate) * up).astype(BF16)
            return inner
        lax.fori_loop(0, n_chunk, gu_body, 0)

        for c in range(n_chunk):
            at, col = divmod(c * COLS, hw)
            if col == 0:
                @pl.when(g == 0)
                def _():
                    for i in range(n_deep):
                        wd_copy(at * n_deep + i).wait()
            acc = None
            for i in range(n_deep):
                prod = jnp.dot(ubuf[:, i * d_model:(i + 1) * d_model], wmix[at * n_deep + i, :, col:col + COLS], preferred_element_type=F32)
                acc = prod if acc is None else acc + prod
            recvp[g, :, c * COLS:(c + 1) * COLS] = acc.astype(BF16)
            d_copy(g, c).start()
        return carry

    def finish_piece(g, c):
        d_copy(g, c).wait()
        cols = pl.ds(pl.multiple_of(c * COLS, COLS), COLS)
        part = (recvd[g, :, cols].astype(F32) + recvp[g, :, cols].astype(F32)).astype(BF16)
        hout[g, :, cols] = (hbuf[g, :, cols].astype(F32) + part.astype(F32)).astype(BF16)

        @pl.when(jnp.logical_not(last))
        def _():
            h_copy(g, c).start()

    lax.fori_loop(0, n_groups, attention_phase, 0)
    lax.fori_loop(0, n_groups, mlp_phase, 0)
    for c in range(n_chunk):
        finish_piece(n_groups - 1, c)

    @pl.when(jnp.logical_not(last))
    def _():
        for g in range(n_groups):
            for c in range(n_chunk):
                h_copy(g, c).wait_send()


def run_layer(dims, *args):
    n_groups, n_batch, d_model, heads, seq, hd, ff, n_pp, n_tp = dims
    hw = heads * hd
    n_chunk = d_model // COLS
    n_gu = ff // COLS
    assert ff * d_model == 4 * d_model * hw
    vmem = pl.BlockSpec(memory_space=pltpu.VMEM)
    hbm = pl.BlockSpec(memory_space=pl.ANY)
    dma = pltpu.SemaphoreType.DMA
    return pl.pallas_call(
        functools.partial(layer_kernel, dims),
        out_shape=(jax.ShapeDtypeStruct((n_groups, n_batch, d_model), BF16),
                   jax.ShapeDtypeStruct((n_groups, heads, hd, n_batch), BF16),
                   jax.ShapeDtypeStruct((n_groups, heads, hd, n_batch), BF16)),
        in_specs=[hbm] + [vmem] * 5 + [hbm] * 10,
        out_specs=(vmem, vmem, vmem),
        scratch_shapes=[
            pltpu.VMEM((4, d_model, hw), BF16),
            pltpu.VMEM((n_gu, d_model, COLS), BF16),
            pltpu.VMEM((n_gu, d_model, COLS), BF16),
            pltpu.VMEM((SLOTS, 2 * seq, hd, n_batch), BF16),
            pltpu.VMEM((n_groups, n_batch, d_model), BF16),
            pltpu.VMEM((n_groups, n_batch, d_model), BF16),
            pltpu.VMEM((n_groups, n_batch, d_model), BF16),
            pltpu.VMEM((n_batch, d_model), BF16),
            pltpu.VMEM((hw, n_batch), BF16),
            pltpu.VMEM((n_batch, ff), BF16),
            pltpu.VMEM((seq, n_batch), F32),
            dma((n_groups,)), dma((3,)), dma((d_model // hw,)), dma((4,)), dma((2, n_gu)), dma((SLOTS, 2)),
            dma((n_groups, n_chunk)), dma((n_groups, n_chunk)), dma((n_groups, n_chunk)),
            dma((n_groups, n_chunk)), dma((n_groups, n_chunk)), dma((n_groups, n_chunk)),
        ],
        compiler_params=pltpu.CompilerParams(collective_id=0, has_side_effects=True, vmem_limit_bytes=67043328),
        name="layer",
    )(*args)


def keep_kernel(dims, pos_hbm, kc, vc, kout, vout, todo_hbm, kb, vb, pos, todo, flags, in_sem, out_sem, pos_sem, todo_sem):
    n_groups, n_batch, _, heads, seq, _, _, n_pp, _ = dims
    n_slab = n_groups * seq
    n_items = n_groups * heads
    ahead = KEEP_SLOTS // 2
    last = lax.axis_index("pp") == n_pp - 1

    def loads(i):
        slot = lax.rem(i, KEEP_SLOTS)
        g, h = i // heads, lax.rem(i, heads)
        return (pltpu.make_async_copy(kc.at[g, h], kb.at[slot], in_sem.at[0, slot]),
                pltpu.make_async_copy(vc.at[g, h], vb.at[slot], in_sem.at[1, slot]))

    def stores(i):
        slot = lax.rem(i, KEEP_SLOTS)
        g, h = i // heads, lax.rem(i, heads)
        return (pltpu.make_async_copy(kb.at[slot], kout.at[g, h], out_sem.at[0, slot]),
                pltpu.make_async_copy(vb.at[slot], vout.at[g, h], out_sem.at[1, slot]))

    @pl.when(last)
    def _():
        for i in range(ahead):
            for copy in loads(i):
                copy.start()

        pos_copy = pltpu.make_async_copy(pos_hbm, pos, pos_sem)
        pos_copy.start()
        pos_copy.wait()

        def clear(i, carry):
            flags[i] = 0
            todo[i + 1] = 0
            return carry
        lax.fori_loop(0, n_slab, clear, 0)
        for g in range(n_groups):
            def mark(b, carry):
                flags[g * seq + pos[g, b]] = 1
                return carry
            lax.fori_loop(0, n_batch, mark, 0)

        def pick(i, count):
            hit = flags[i]

            @pl.when(hit == 1)
            def _():
                todo[count + 1] = i
            return count + hit
        todo[0] = lax.fori_loop(0, n_slab, pick, jnp.int32(0))
        todo_copy = pltpu.make_async_copy(todo, todo_hbm, todo_sem)
        todo_copy.start()

        def body(i, carry):
            for copy in loads(i):
                copy.wait()
            for copy in stores(i):
                copy.start()

            @pl.when(i + ahead < n_items)
            def _():
                @pl.when(i >= ahead)
                def _():
                    for copy in stores(i - ahead):
                        copy.wait()
                for copy in loads(i + ahead):
                    copy.start()
            return carry
        lax.fori_loop(0, n_items, body, 0)
        for i in range(n_items - 2 * ahead, n_items):
            for copy in stores(i):
                copy.wait()
        todo_copy.wait()


def keep_old(dims, positions, key_t, value_t):
    n_groups, n_batch, _, heads, seq, hd, _, _, _ = dims
    hbm = pl.BlockSpec(memory_space=pl.ANY)
    dma = pltpu.SemaphoreType.DMA
    return pl.pallas_call(
        functools.partial(keep_kernel, dims),
        out_shape=(jax.ShapeDtypeStruct(key_t.shape, BF16), jax.ShapeDtypeStruct(value_t.shape, BF16),
                   jax.ShapeDtypeStruct((n_groups * seq + 1,), jnp.int32)),
        in_specs=[hbm] * 3,
        out_specs=(hbm, hbm, hbm),
        scratch_shapes=[
            pltpu.VMEM((KEEP_SLOTS, seq, hd, n_batch), BF16),
            pltpu.VMEM((KEEP_SLOTS, seq, hd, n_batch), BF16),
            pltpu.SMEM((n_groups, n_batch), jnp.int32),
            pltpu.SMEM((n_groups * seq + 1,), jnp.int32),
            pltpu.SMEM((n_groups * seq,), jnp.int32),
            dma((2, KEEP_SLOTS)), dma((2, KEEP_SLOTS)), dma, dma,
        ],
        compiler_params=pltpu.CompilerParams(vmem_limit_bytes=40 * 2**20),
        name="cache_keep",
    )(positions, key_t, value_t)


def write_kernel(dims, todo_hbm, pos_hbm, knew_hbm, vnew_hbm, kc, vc, kold, vold, kout, vout,
                 todo, pos_ref, knew, vnew, kb, vb, in_sem, out_sem, small_sem):
    n_groups, _, _, _, seq, _, _, n_pp, _ = dims
    ahead = WRITE_SLOTS // 2
    last = lax.axis_index("pp") == n_pp - 1
    small = [pltpu.make_async_copy(src, dst, small_sem.at[i]) for i, (src, dst) in enumerate(
        ((todo_hbm, todo), (pos_hbm, pos_ref), (knew_hbm, knew), (vnew_hbm, vnew)))]
    for copy in small:
        copy.start()
    small[0].wait()
    count = jnp.where(last, todo[0], n_groups * seq)

    def place(i):
        entry = jnp.where(last, todo[i + 1], i)
        return entry // seq, lax.rem(entry, seq), lax.rem(i, WRITE_SLOTS)

    def loads(i):
        g, s, slot = place(i)
        return (pltpu.make_async_copy(kc.at[g, :, s], kb.at[slot], in_sem.at[0, slot]),
                pltpu.make_async_copy(vc.at[g, :, s], vb.at[slot], in_sem.at[1, slot]))

    def stores(i):
        g, s, slot = place(i)
        return (pltpu.make_async_copy(kb.at[slot], kout.at[g, :, s], out_sem.at[0, slot]),
                pltpu.make_async_copy(vb.at[slot], vout.at[g, :, s], out_sem.at[1, slot]))

    for i in range(ahead):
        @pl.when(i < count)
        def _():
            for copy in loads(i):
                copy.start()

    for copy in small[1:]:
        copy.wait()

    def body(i, carry):
        g, s, slot = place(i)
        for copy in loads(i):
            copy.wait()
        hit = (pos_ref[g] == s)[None]
        for new, buf in ((knew, kb), (vnew, vb)):
            buf[slot] = jnp.where(hit, new[g].astype(F32), buf[slot].astype(F32)).astype(BF16)
        for copy in stores(i):
            copy.start()

        @pl.when(i + ahead < count)
        def _():
            @pl.when(i >= ahead)
            def _():
                for copy in stores(i - ahead):
                    copy.wait()
            for copy in loads(i + ahead):
                copy.start()
        return carry
    lax.fori_loop(0, count, body, 0)

    def drain(i, carry):
        for copy in stores(i):
            copy.wait()
        return carry
    lax.fori_loop(jnp.maximum(count - 2 * ahead, 0), count, drain, 0)


def write_new(dims, todo, pos, key_new, value_new, key_t, value_t, key_old, value_old):
    n_groups, n_batch, _, heads, seq, hd, _, _, _ = dims
    hbm = pl.BlockSpec(memory_space=pl.ANY)
    dma = pltpu.SemaphoreType.DMA
    return pl.pallas_call(
        functools.partial(write_kernel, dims),
        out_shape=(jax.ShapeDtypeStruct(key_t.shape, BF16), jax.ShapeDtypeStruct(value_t.shape, BF16)),
        in_specs=[hbm] * 8,
        out_specs=(hbm, hbm),
        scratch_shapes=[
            pltpu.SMEM((n_groups * seq + 1,), jnp.int32),
            pltpu.VMEM((n_groups, 1, n_batch), jnp.int32),
            pltpu.VMEM((n_groups, heads, hd, n_batch), BF16),
            pltpu.VMEM((n_groups, heads, hd, n_batch), BF16),
            pltpu.VMEM((WRITE_SLOTS, heads, hd, n_batch), BF16),
            pltpu.VMEM((WRITE_SLOTS, heads, hd, n_batch), BF16),
            dma((2, WRITE_SLOTS)), dma((2, WRITE_SLOTS)), dma((4,)),
        ],
        input_output_aliases={6: 0, 7: 1},
        compiler_params=pltpu.CompilerParams(vmem_limit_bytes=40 * 2**20),
        cost_estimate=pl.CostEstimate(flops=n_groups * n_batch * heads * seq * hd * 40, bytes_accessed=8 * key_t.size, transcendentals=0),
        name="cache_write",
    )(todo, pos, key_new, value_new, key_t, value_t, key_old, value_old)


def solution(mesh):
    n_pp = mesh.shape["pp"]
    n_tp = mesh.shape["tp"]
    cache_spec = P("pp", "dp", None, "tp", None, None)
    col_spec = P("pp", None, "tp")
    row_spec = P("pp", "tp", None)
    gain_spec = P("pp", None)
    in_specs = (P("dp", None, None), P("dp", None), cache_spec, cache_spec, gain_spec, col_spec, col_spec, col_spec, row_spec, gain_spec, col_spec, col_spec, row_spec)
    out_specs = (P("dp", None, None), cache_spec, cache_spec)

    def per_device(hidden, positions, key_cache, value_cache, attn_norm, w_query, w_key, w_value, w_out, mlp_norm, w_gate, w_up, w_down):
        _, n_groups, n_batch, heads, seq, hd = key_cache.shape
        d_model = hidden.shape[-1]
        ff = w_gate.shape[-1]
        dims = (n_groups, n_batch, d_model, heads, seq, hd, ff, n_pp, n_tp)
        angles = positions.astype(F32)[:, None, :] * rope_freqs(hd)[None, :, None]
        key_t = jnp.transpose(key_cache[0], (0, 2, 3, 4, 1))
        value_t = jnp.transpose(value_cache[0], (0, 2, 3, 4, 1))
        pos = positions[:, None, :]
        key_old, value_old, todo = keep_old(dims, positions, key_t, value_t)
        state, key_new, value_new = run_layer(
            dims, todo, jnp.cos(angles), jnp.sin(angles), pos, attn_norm, mlp_norm, hidden, key_t, value_t,
            w_query[0], w_key[0], w_value[0], w_out[0], w_gate[0], w_up[0], w_down[0])

        stage = lax.axis_index("pp")
        from_last = [lax.ppermute(state, "pp", [(n_pp - 1, dst)]) for dst in range(1, n_pp - 1)]
        key_t, value_t = write_new(dims, todo, pos, key_new, value_new, key_t, value_t, key_old, value_old)
        from_last[0], key_t = lax.optimization_barrier((from_last[0], key_t))
        from_last.append(lax.ppermute(from_last[0], "pp", [(1, 0)]))
        final = jnp.where(stage == n_pp - 1, state, sum(from_last[1:], from_last[0]))
        return final, jnp.transpose(key_t, (0, 4, 1, 2, 3))[None], jnp.transpose(value_t, (0, 4, 1, 2, 3))[None]

    return jax.shard_map(per_device, mesh=mesh, in_specs=in_specs, out_specs=out_specs, check_vma=False)
```

```python
import functools
import math
import jax
import jax.numpy as jnp
from jax import lax
from jax.experimental import pallas as pl
from jax.experimental.pallas import tpu as pltpu
from jax.sharding import PartitionSpec as P

ROPE_THETA = 500000.0
SCALE_FACTOR = 8.0
LOW_FACTOR = 1.0
HIGH_FACTOR = 4.0
ORIG_CONTEXT = 8192.0
NORM_EPS = 1e-5
MESH = pl.DeviceIdType.MESH
F32 = jnp.float32
BF16 = jnp.bfloat16

COLS = 512
SLOTS = 8
NORM_ROWS = 64
KEEP_SLOTS = 16
WRITE_SLOTS = 24


def rope_freqs(head_dim):
    freq_index = jnp.arange(head_dim // 2, dtype=jnp.float32)
    base_freq = ROPE_THETA ** (-2.0 * freq_index / head_dim)
    wave_len = 2.0 * math.pi / base_freq
    smooth_t = (ORIG_CONTEXT / wave_len - LOW_FACTOR) / (HIGH_FACTOR - LOW_FACTOR)
    mixed_freq = (1.0 - smooth_t) * base_freq / SCALE_FACTOR + smooth_t * base_freq
    long_freq = jnp.where(wave_len > ORIG_CONTEXT / LOW_FACTOR, base_freq / SCALE_FACTOR, mixed_freq)
    return jnp.where(wave_len < ORIG_CONTEXT / HIGH_FACTOR, base_freq, long_freq)


def layer_kernel(dims, after, cos_ref, sin_ref, pos_ref, ga_ref, gm_ref, hid, kc, vc, wq, wk, wv, wo, wg, wu, wd,
                 hout, knew, vnew,
                 wmix, wg_v, wu_v, ring, hbuf, recvp, recvd, nbuf, qt, ubuf, sc,
                 hid_sem, wqkv_sem, wo_sem, wd_sem, gu_sem, ring_sem,
                 p_send, p_recv, d_send, d_recv, h_send, h_recv):
    n_groups, n_batch, d_model, heads, seq, hd, ff, n_pp, n_tp = dims
    hw = heads * hd
    n_chunk = d_model // COLS
    n_gu = ff // COLS
    n_half = d_model // hw
    n_deep = ff // d_model
    pp = lax.axis_index("pp")
    tp = lax.axis_index("tp")
    peer = {"tp": lax.rem(tp + 1, n_tp)}
    nxt = {"pp": lax.rem(pp + 1, n_pp)}
    prv = {"pp": lax.rem(pp + n_pp - 1, n_pp)}

    n_kv = n_groups * heads

    def kv_copies(item, slot):
        g = item // heads
        h = lax.rem(item, heads)
        return (pltpu.make_async_copy(kc.at[g, h], ring.at[slot, pl.ds(0, seq)], ring_sem.at[slot, 0]),
                pltpu.make_async_copy(vc.at[g, h], ring.at[slot, pl.ds(seq, seq)], ring_sem.at[slot, 1]))

    def wd_copy(i):
        return pltpu.make_async_copy(wd.at[pl.ds(i % n_deep * d_model, d_model), pl.ds(i // n_deep * hw, hw)], wmix.at[i], wd_sem.at[i])

    def gu_copies(j):
        cols = pl.ds(pl.multiple_of(j * COLS, COLS), COLS)
        return (pltpu.make_async_copy(wg.at[:, cols], wg_v.at[j], gu_sem.at[0, j]),
                pltpu.make_async_copy(wu.at[:, cols], wu_v.at[j], gu_sem.at[1, j]))

    def qkv_copies():
        return [pltpu.make_async_copy(src, wmix.at[i], wqkv_sem.at[i]) for i, src in enumerate((wq, wk, wv))]

    def wo_copies():
        return [pltpu.make_async_copy(wo.at[:, pl.ds(i * hw, hw)], wmix.at[3, pl.ds(i * hw, hw)], wo_sem.at[i]) for i in range(n_half)]

    def hid_copy(g):
        return pltpu.make_async_copy(hid.at[g], hbuf.at[g], hid_sem.at[g])

    def piece(ref, g, c):
        return ref.at[g, :, pl.ds(pl.multiple_of(c * COLS, COLS), COLS)]

    def p_copy(g, c):
        return pltpu.make_async_remote_copy(piece(hout, g, c), piece(recvp, g, c), p_send.at[g, c], p_recv.at[g, c], device_id=peer, device_id_type=MESH)

    def d_copy(g, c):
        return pltpu.make_async_remote_copy(piece(recvp, g, c), piece(recvd, g, c), d_send.at[g, c], d_recv.at[g, c], device_id=peer, device_id_type=MESH)

    def h_copy(g, c):
        return pltpu.make_async_remote_copy(piece(hout, g, c), piece(hbuf, g, c), h_send.at[g, c], h_recv.at[g, c], device_id=nxt, device_id_type=MESH)

    first = pp == 0
    last = pp == n_pp - 1

    @pl.when(first)
    def _():
        for g in range(n_groups):
            hid_copy(g).start()
    for copy in qkv_copies():
        copy.start()

    def start_kv_wo():
        for slot in range(SLOTS):
            for copy in kv_copies(slot, slot):
                copy.start()
        for copy in wo_copies():
            copy.start()

    @pl.when(pp > 0)
    def _():
        start_kv_wo()
        for j in range(n_gu):
            for copy in gu_copies(j):
                copy.start()

    barrier = pltpu.get_barrier_semaphore()
    pl.semaphore_signal(barrier, inc=1, device_id=peer, device_id_type=MESH)

    @pl.when(jnp.logical_not(last))
    def _():
        pl.semaphore_signal(barrier, inc=1, device_id=nxt, device_id_type=MESH)

    @pl.when(pp > 0)
    def _():
        pl.semaphore_signal(barrier, inc=1, device_id=prv, device_id_type=MESH)
    ends = jnp.logical_or(first, last)

    @pl.when(ends)
    def _():
        pl.semaphore_wait(barrier, 2)

    @pl.when(jnp.logical_not(ends))
    def _():
        pl.semaphore_wait(barrier, 3)

    def norm_rows(g, gain_ref, with_partial):
        def body(r, carry):
            rows = pl.ds(pl.multiple_of(r * NORM_ROWS, NORM_ROWS), NORM_ROWS)
            x = hbuf[g, rows, :].astype(F32)
            if with_partial:
                part = (hout[g, rows, :].astype(F32) + recvp[g, rows, :].astype(F32)).astype(BF16)
                x = (x + part.astype(F32)).astype(BF16)
                hbuf[g, rows, :] = x
                x = x.astype(F32)
            inv = lax.rsqrt(jnp.mean(x * x, axis=-1, keepdims=True) + NORM_EPS)
            nbuf[rows, :] = (x * inv * gain_ref[...].astype(F32)).astype(BF16)
            return carry
        lax.fori_loop(0, n_batch // NORM_ROWS, body, 0)

    def attention_phase(g, carry):
        @pl.when(first)
        def _():
            hid_copy(g).wait()

        @pl.when(pp > 0)
        def _():
            for c in range(n_chunk):
                h_copy(g, c).wait_recv()

        norm_rows(g, ga_ref, False)
        cosine = cos_ref[g]
        sine = sin_ref[g]
        half = hd // 2

        @pl.when(g == 0)
        def _():
            for i, copy in enumerate(qkv_copies()):
                copy.wait()
                if i == 0:
                    pl.when(first)(start_kv_wo)

        for which in range(3):
            for c in range(hw // COLS):
                cols = slice(c * COLS, (c + 1) * COLS)
                prod_t = jnp.dot(nbuf[...], wmix[which, :, cols], preferred_element_type=F32).T
                for i in range(COLS // hd):
                    head = c * (COLS // hd) + i
                    a = prod_t[i * hd:i * hd + half]
                    b = prod_t[i * hd + half:(i + 1) * hd]
                    if which < 2:
                        a, b = a * cosine - b * sine, b * cosine + a * sine
                    both = jnp.concatenate([a, b], axis=0).astype(BF16)
                    if which == 0:
                        qt[head * hd:(head + 1) * hd, :] = both
                    else:
                        dst = knew if which == 1 else vnew
                        dst[g, head] = both

        pos = pos_ref[g]
        row_id = lax.broadcasted_iota(jnp.int32, (seq, n_batch), 0)
        hit = row_id == pos
        seen = row_id <= pos

        def head_body(h, inner):
            item = g * heads + h
            slot = lax.rem(item, SLOTS)
            for copy in kv_copies(item, slot):
                copy.wait()
            rows = pl.ds(pl.multiple_of(h * hd, hd), hd)
            q = qt[rows, :].astype(F32)
            fresh = jnp.sum(q * knew[g, h].astype(F32), axis=0, keepdims=True)
            for s in range(seq):
                sc[s:s + 1, :] = jnp.sum(ring[slot, s].astype(F32) * q, axis=0, keepdims=True)
            scores = jnp.where(hit, fresh, sc[...]) * hd ** -0.5
            scores = jnp.where(seen, scores, -jnp.inf)
            top = jnp.max(scores, axis=0, keepdims=True)
            expd = jnp.exp(scores - top)
            probs = (expd / jnp.sum(expd, axis=0, keepdims=True)).astype(BF16).astype(F32)
            sc[...] = jnp.where(hit, 0.0, probs)
            acc = jnp.sum(jnp.where(hit, probs, 0.0), axis=0, keepdims=True) * vnew[g, h].astype(F32)
            for s in range(seq):
                acc = acc + sc[s:s + 1, :] * ring[slot, seq + s].astype(F32)
            qt[rows, :] = acc.astype(BF16)

            @pl.when(item + SLOTS < n_kv)
            def _():
                for copy in kv_copies(item + SLOTS, slot):
                    copy.start()

            @pl.when(jnp.logical_and(first, lax.rem(item, n_kv // n_gu) == 0))
            def _():
                for copy in gu_copies(item // (n_kv // n_gu)):
                    copy.start()

            @pl.when(item + SLOTS == n_kv)
            def _():
                for i in range(3):
                    wd_copy(i).start()
            return inner
        lax.fori_loop(0, heads, head_body, 0)

        @pl.when(g == 0)
        def _():
            for copy in wo_copies():
                copy.wait()
        for c in range(hw // COLS):
            cols = slice(c * COLS, (c + 1) * COLS)
            nbuf[:, cols] = qt[cols, :].astype(F32).T.astype(BF16)

        for c in range(n_chunk):
            at, col = divmod(c * COLS, hw)
            part = jnp.dot(nbuf[:, 0:hw], wmix[3, at * hw:(at + 1) * hw, col:col + COLS], preferred_element_type=F32)
            hout[g, :, c * COLS:(c + 1) * COLS] = part.astype(BF16)
        for c in range(n_chunk):
            p_copy(g, c).start()

        @pl.when(g == n_groups - 1)
        def _():
            wd_copy(3).start()
        return carry

    def mlp_phase(g, carry):
        for c in range(n_chunk):
            p_copy(g, c).wait()
        norm_rows(g, gm_ref, True)

        some = n_gu // 2

        def finish_some(part):
            @pl.when(g > 0)
            def _():
                for c in range(n_chunk // 2):
                    finish_piece(g - 1, part * (n_chunk // 2) + c)

        def gu_body(part, inner):
            tiles = [part * some + i for i in range(some)]

            @pl.when(g == 0)
            def _():
                for j in tiles:
                    for copy in gu_copies(j):
                        copy.wait()
            pl.when(part > 0)(lambda: finish_some(part - 1))
            for j in tiles:
                gate = jnp.dot(nbuf[...], wg_v[j], preferred_element_type=F32)
                up = jnp.dot(nbuf[...], wu_v[j], preferred_element_type=F32)
                ubuf[:, pl.ds(pl.multiple_of(j * COLS, COLS), COLS)] = (jax.nn.silu(gate) * up).astype(BF16)
            return inner
        lax.fori_loop(0, 2, gu_body, 0)
        finish_some(1)

        for c in range(n_chunk):
            at, col = divmod(c * COLS, hw)
            if col == 0:
                @pl.when(g == 0)
                def _():
                    for i in range(n_deep):
                        wd_copy(at * n_deep + i).wait()
            acc = None
            for i in range(n_deep):
                prod = jnp.dot(ubuf[:, i * d_model:(i + 1) * d_model], wmix[at * n_deep + i, :, col:col + COLS], preferred_element_type=F32)
                acc = prod if acc is None else acc + prod
            recvp[g, :, c * COLS:(c + 1) * COLS] = acc.astype(BF16)
            d_copy(g, c).start()
        return carry

    def finish_piece(g, c):
        d_copy(g, c).wait()
        cols = pl.ds(pl.multiple_of(c * COLS, COLS), COLS)
        part = (recvd[g, :, cols].astype(F32) + recvp[g, :, cols].astype(F32)).astype(BF16)
        hout[g, :, cols] = (hbuf[g, :, cols].astype(F32) + part.astype(F32)).astype(BF16)

        @pl.when(jnp.logical_not(last))
        def _():
            h_copy(g, c).start()

    lax.fori_loop(0, n_groups, attention_phase, 0)
    lax.fori_loop(0, n_groups, mlp_phase, 0)
    for c in range(n_chunk):
        finish_piece(n_groups - 1, c)

    @pl.when(jnp.logical_not(last))
    def _():
        for g in range(n_groups):
            for c in range(n_chunk):
                h_copy(g, c).wait_send()


def run_layer(dims, *args):
    n_groups, n_batch, d_model, heads, seq, hd, ff, n_pp, n_tp = dims
    hw = heads * hd
    n_chunk = d_model // COLS
    n_gu = ff // COLS
    assert ff * d_model == 4 * d_model * hw
    vmem = pl.BlockSpec(memory_space=pltpu.VMEM)
    hbm = pl.BlockSpec(memory_space=pltpu.HBM)
    dma = pltpu.SemaphoreType.DMA
    return pl.pallas_call(
        functools.partial(layer_kernel, dims),
        out_shape=(jax.ShapeDtypeStruct((n_groups, n_batch, d_model), BF16),
                   jax.ShapeDtypeStruct((n_groups, heads, hd, n_batch), BF16),
                   jax.ShapeDtypeStruct((n_groups, heads, hd, n_batch), BF16)),
        in_specs=[hbm] + [vmem] * 5 + [hbm] * 10,
        out_specs=(vmem, vmem, vmem),
        scratch_shapes=[
            pltpu.VMEM((4, d_model, hw), BF16),
            pltpu.VMEM((n_gu, d_model, COLS), BF16),
            pltpu.VMEM((n_gu, d_model, COLS), BF16),
            pltpu.VMEM((SLOTS, 2 * seq, hd, n_batch), BF16),
            pltpu.VMEM((n_groups, n_batch, d_model), BF16),
            pltpu.VMEM((n_groups, n_batch, d_model), BF16),
            pltpu.VMEM((n_groups, n_batch, d_model), BF16),
            pltpu.VMEM((n_batch, d_model), BF16),
            pltpu.VMEM((hw, n_batch), BF16),
            pltpu.VMEM((n_batch, ff), BF16),
            pltpu.VMEM((seq, n_batch), F32),
            dma((n_groups,)), dma((3,)), dma((d_model // hw,)), dma((4,)), dma((2, n_gu)), dma((SLOTS, 2)),
            dma((n_groups, n_chunk)), dma((n_groups, n_chunk)), dma((n_groups, n_chunk)),
            dma((n_groups, n_chunk)), dma((n_groups, n_chunk)), dma((n_groups, n_chunk)),
        ],
        compiler_params=pltpu.CompilerParams(collective_id=0, has_side_effects=True, vmem_limit_bytes=67043328),
        name="layer",
    )(*args)


def keep_kernel(dims, pos_hbm, kc, vc, kout, vout, todo_hbm, kb, vb, pos, todo, flags, in_sem, out_sem, pos_sem, todo_sem):
    n_groups, n_batch, _, heads, seq, _, _, n_pp, _ = dims
    n_slab = n_groups * seq
    n_items = n_groups * heads
    ahead = KEEP_SLOTS // 2
    last = lax.axis_index("pp") == n_pp - 1

    def loads(i):
        slot = lax.rem(i, KEEP_SLOTS)
        g, h = i // heads, lax.rem(i, heads)
        return (pltpu.make_async_copy(kc.at[g, h], kb.at[slot], in_sem.at[0, slot]),
                pltpu.make_async_copy(vc.at[g, h], vb.at[slot], in_sem.at[1, slot]))

    def stores(i):
        slot = lax.rem(i, KEEP_SLOTS)
        g, h = i // heads, lax.rem(i, heads)
        return (pltpu.make_async_copy(kb.at[slot], kout.at[g, h], out_sem.at[0, slot]),
                pltpu.make_async_copy(vb.at[slot], vout.at[g, h], out_sem.at[1, slot]))

    @pl.when(last)
    def _():
        for i in range(ahead):
            for copy in loads(i):
                copy.start()

        pos_copy = pltpu.make_async_copy(pos_hbm, pos, pos_sem)
        pos_copy.start()
        pos_copy.wait()

        def clear(i, carry):
            flags[i] = 0
            todo[i + 1] = 0
            return carry
        lax.fori_loop(0, n_slab, clear, 0)
        for g in range(n_groups):
            def mark(b, carry):
                flags[g * seq + pos[g, b]] = 1
                return carry
            lax.fori_loop(0, n_batch, mark, 0)

        def pick(i, count):
            hit = flags[i]

            @pl.when(hit == 1)
            def _():
                todo[count + 1] = i
            return count + hit
        todo[0] = lax.fori_loop(0, n_slab, pick, jnp.int32(0))
        todo_copy = pltpu.make_async_copy(todo, todo_hbm, todo_sem)
        todo_copy.start()

        def body(i, carry):
            for copy in loads(i):
                copy.wait()
            for copy in stores(i):
                copy.start()

            @pl.when(i + ahead < n_items)
            def _():
                @pl.when(i >= ahead)
                def _():
                    for copy in stores(i - ahead):
                        copy.wait()
                for copy in loads(i + ahead):
                    copy.start()
            return carry
        lax.fori_loop(0, n_items, body, 0)
        for i in range(n_items - 2 * ahead, n_items):
            for copy in stores(i):
                copy.wait()
        todo_copy.wait()


def keep_old(dims, positions, key_t, value_t):
    n_groups, n_batch, _, heads, seq, hd, _, _, _ = dims
    hbm = pl.BlockSpec(memory_space=pltpu.HBM)
    dma = pltpu.SemaphoreType.DMA
    return pl.pallas_call(
        functools.partial(keep_kernel, dims),
        out_shape=(jax.ShapeDtypeStruct(key_t.shape, BF16), jax.ShapeDtypeStruct(value_t.shape, BF16),
                   jax.ShapeDtypeStruct((n_groups * seq + 1,), jnp.int32)),
        in_specs=[hbm] * 3,
        out_specs=(hbm, hbm, hbm),
        scratch_shapes=[
            pltpu.VMEM((KEEP_SLOTS, seq, hd, n_batch), BF16),
            pltpu.VMEM((KEEP_SLOTS, seq, hd, n_batch), BF16),
            pltpu.SMEM((n_groups, n_batch), jnp.int32),
            pltpu.SMEM((n_groups * seq + 1,), jnp.int32),
            pltpu.SMEM((n_groups * seq,), jnp.int32),
            dma((2, KEEP_SLOTS)), dma((2, KEEP_SLOTS)), dma, dma,
        ],
        compiler_params=pltpu.CompilerParams(vmem_limit_bytes=67043328),
        name="cache_keep",
    )(positions, key_t, value_t)


def write_kernel(dims, todo_hbm, pos_hbm, knew_hbm, vnew_hbm, kc, vc, kold, vold, kout, vout,
                 todo, pos_ref, knew, vnew, kb, vb, in_sem, out_sem, small_sem):
    n_groups, _, _, _, seq, _, _, n_pp, _ = dims
    ahead = WRITE_SLOTS // 2
    last = lax.axis_index("pp") == n_pp - 1
    small = [pltpu.make_async_copy(src, dst, small_sem.at[i]) for i, (src, dst) in enumerate(
        ((todo_hbm, todo), (pos_hbm, pos_ref), (knew_hbm, knew), (vnew_hbm, vnew)))]
    for copy in small:
        copy.start()
    small[0].wait()
    count = jnp.where(last, todo[0], n_groups * seq)

    def place(i):
        entry = jnp.where(last, todo[i + 1], i)
        return entry // seq, lax.rem(entry, seq), lax.rem(i, WRITE_SLOTS)

    def loads(i):
        g, s, slot = place(i)
        return (pltpu.make_async_copy(kc.at[g, :, s], kb.at[slot], in_sem.at[0, slot]),
                pltpu.make_async_copy(vc.at[g, :, s], vb.at[slot], in_sem.at[1, slot]))

    def stores(i):
        g, s, slot = place(i)
        return (pltpu.make_async_copy(kb.at[slot], kout.at[g, :, s], out_sem.at[0, slot]),
                pltpu.make_async_copy(vb.at[slot], vout.at[g, :, s], out_sem.at[1, slot]))

    for i in range(ahead):
        @pl.when(i < count)
        def _():
            for copy in loads(i):
                copy.start()

    for copy in small[1:]:
        copy.wait()

    def body(i, carry):
        g, s, slot = place(i)
        for copy in loads(i):
            copy.wait()
        hit = (pos_ref[g] == s)[None]
        for new, buf in ((knew, kb), (vnew, vb)):
            buf[slot] = jnp.where(hit, new[g].astype(F32), buf[slot].astype(F32)).astype(BF16)
        for copy in stores(i):
            copy.start()

        @pl.when(i + ahead < count)
        def _():
            @pl.when(i >= ahead)
            def _():
                for copy in stores(i - ahead):
                    copy.wait()
            for copy in loads(i + ahead):
                copy.start()
        return carry
    lax.fori_loop(0, count, body, 0)

    def drain(i, carry):
        for copy in stores(i):
            copy.wait()
        return carry
    lax.fori_loop(jnp.maximum(count - 2 * ahead, 0), count, drain, 0)


def write_new(dims, todo, pos, key_new, value_new, key_t, value_t, key_old, value_old):
    n_groups, n_batch, _, heads, seq, hd, _, _, _ = dims
    hbm = pl.BlockSpec(memory_space=pltpu.HBM)
    dma = pltpu.SemaphoreType.DMA
    return pl.pallas_call(
        functools.partial(write_kernel, dims),
        out_shape=(jax.ShapeDtypeStruct(key_t.shape, BF16), jax.ShapeDtypeStruct(value_t.shape, BF16)),
        in_specs=[hbm] * 8,
        out_specs=(hbm, hbm),
        scratch_shapes=[
            pltpu.SMEM((n_groups * seq + 1,), jnp.int32),
            pltpu.VMEM((n_groups, 1, n_batch), jnp.int32),
            pltpu.VMEM((n_groups, heads, hd, n_batch), BF16),
            pltpu.VMEM((n_groups, heads, hd, n_batch), BF16),
            pltpu.VMEM((WRITE_SLOTS, heads, hd, n_batch), BF16),
            pltpu.VMEM((WRITE_SLOTS, heads, hd, n_batch), BF16),
            dma((2, WRITE_SLOTS)), dma((2, WRITE_SLOTS)), dma((4,)),
        ],
        input_output_aliases={6: 0, 7: 1},
        compiler_params=pltpu.CompilerParams(vmem_limit_bytes=67043328),
        cost_estimate=pl.CostEstimate(flops=n_groups * n_batch * heads * seq * hd * 40, bytes_accessed=8 * key_t.size, transcendentals=0),
        name="cache_write",
    )(todo, pos, key_new, value_new, key_t, value_t, key_old, value_old)


def solution(mesh):
    n_pp = mesh.shape["pp"]
    n_tp = mesh.shape["tp"]
    cache_spec = P("pp", "dp", None, "tp", None, None)
    col_spec = P("pp", None, "tp")
    row_spec = P("pp", "tp", None)
    gain_spec = P("pp", None)
    in_specs = (P("dp", None, None), P("dp", None), cache_spec, cache_spec, gain_spec, col_spec, col_spec, col_spec, row_spec, gain_spec, col_spec, col_spec, row_spec)
    out_specs = (P("dp", None, None), cache_spec, cache_spec)

    def per_device(hidden, positions, key_cache, value_cache, attn_norm, w_query, w_key, w_value, w_out, mlp_norm, w_gate, w_up, w_down):
        _, n_groups, n_batch, heads, seq, hd = key_cache.shape
        d_model = hidden.shape[-1]
        ff = w_gate.shape[-1]
        dims = (n_groups, n_batch, d_model, heads, seq, hd, ff, n_pp, n_tp)
        angles = positions.astype(F32)[:, None, :] * rope_freqs(hd)[None, :, None]
        key_t = jnp.transpose(key_cache[0], (0, 2, 3, 4, 1))
        value_t = jnp.transpose(value_cache[0], (0, 2, 3, 4, 1))
        pos = positions[:, None, :]
        key_old, value_old, todo = keep_old(dims, positions, key_t, value_t)
        state, key_new, value_new = run_layer(
            dims, todo, jnp.cos(angles), jnp.sin(angles), pos, attn_norm, mlp_norm, hidden, key_t, value_t,
            w_query[0], w_key[0], w_value[0], w_out[0], w_gate[0], w_up[0], w_down[0])

        stage = lax.axis_index("pp")
        from_last = [lax.ppermute(state, "pp", [(n_pp - 1, dst)]) for dst in range(1, n_pp - 1)]
        key_t, value_t = write_new(dims, todo, pos, key_new, value_new, key_t, value_t, key_old, value_old)
        from_last[0], key_t = lax.optimization_barrier((from_last[0], key_t))
        from_last.append(lax.ppermute(from_last[0], "pp", [(1, 0)]))
        final = jnp.where(stage == n_pp - 1, state, sum(from_last[1:], from_last[0]))
        return final, jnp.transpose(key_t, (0, 4, 1, 2, 3))[None], jnp.transpose(value_t, (0, 4, 1, 2, 3))[None]

    return jax.shard_map(per_device, mesh=mesh, in_specs=in_specs, out_specs=out_specs, check_vma=False)
```

```python
import functools
import math
import jax
import jax.numpy as jnp
import numpy as np
from jax import lax
from jax.experimental import pallas as pl
from jax.experimental.pallas import tpu as pltpu
from jax.sharding import PartitionSpec as P

ROPE_THETA = 500000.0
SCALE_FACTOR = 8.0
LOW_FACTOR = 1.0
HIGH_FACTOR = 4.0
ORIG_CONTEXT = 8192.0
NORM_EPS = 1e-5
MESH = pl.DeviceIdType.MESH
F32 = jnp.float32
BF16 = jnp.bfloat16

COLS = 512
SLOTS = 8
NORM_ROWS = 64
KEEP_SLOTS = 16
WRITE_SLOTS = 24


def rope_freqs(head_dim):
    freq_index = np.arange(head_dim // 2, dtype=np.float64)
    base_freq = ROPE_THETA ** (-2.0 * freq_index / head_dim)
    wave_len = 2.0 * math.pi / base_freq
    smooth_t = (ORIG_CONTEXT / wave_len - LOW_FACTOR) / (HIGH_FACTOR - LOW_FACTOR)
    mixed_freq = (1.0 - smooth_t) * base_freq / SCALE_FACTOR + smooth_t * base_freq
    long_freq = np.where(wave_len > ORIG_CONTEXT / LOW_FACTOR, base_freq / SCALE_FACTOR, mixed_freq)
    return np.where(wave_len < ORIG_CONTEXT / HIGH_FACTOR, base_freq, long_freq).astype(np.float32)


def layer_kernel(dims, after, freq_ref, pos_ref, ga_ref, gm_ref, hid, kc, vc, wq, wk, wv, wo, wg, wu, wd,
                 hout, knew, vnew,
                 wmix, wg_v, wu_v, ring, hbuf, recvp, recvd, nbuf, qt, ubuf, sc, cos_ref, sin_ref,
                 hid_sem, wqkv_sem, wo_sem, wd_sem, gu_sem, ring_sem,
                 p_send, p_recv, d_send, d_recv, h_send, h_recv):
    n_groups, n_batch, d_model, heads, seq, hd, ff, n_pp, n_tp = dims
    hw = heads * hd
    n_chunk = d_model // COLS
    n_gu = ff // COLS
    n_half = d_model // hw
    n_deep = ff // d_model
    pp = lax.axis_index("pp")
    tp = lax.axis_index("tp")
    peer = {"tp": lax.rem(tp + 1, n_tp)}
    nxt = {"pp": lax.rem(pp + 1, n_pp)}
    prv = {"pp": lax.rem(pp + n_pp - 1, n_pp)}

    n_kv = n_groups * heads

    def kv_copies(item, slot):
        g = item // heads
        h = lax.rem(item, heads)
        return (pltpu.make_async_copy(kc.at[g, h], ring.at[slot, pl.ds(0, seq)], ring_sem.at[slot, 0]),
                pltpu.make_async_copy(vc.at[g, h], ring.at[slot, pl.ds(seq, seq)], ring_sem.at[slot, 1]))

    def wd_copy(i):
        return pltpu.make_async_copy(wd.at[pl.ds(i % n_deep * d_model, d_model), pl.ds(i // n_deep * hw, hw)], wmix.at[i], wd_sem.at[i])

    def gu_copies(j):
        cols = pl.ds(pl.multiple_of(j * COLS, COLS), COLS)
        return (pltpu.make_async_copy(wg.at[:, cols], wg_v.at[j], gu_sem.at[0, j]),
                pltpu.make_async_copy(wu.at[:, cols], wu_v.at[j], gu_sem.at[1, j]))

    def qkv_copies():
        return [pltpu.make_async_copy(src, wmix.at[i], wqkv_sem.at[i]) for i, src in enumerate((wq, wk, wv))]

    def wo_copies():
        return [pltpu.make_async_copy(wo.at[:, pl.ds(i * hw, hw)], wmix.at[3, pl.ds(i * hw, hw)], wo_sem.at[i]) for i in range(n_half)]

    def hid_copy(g):
        return pltpu.make_async_copy(hid.at[g], hbuf.at[g], hid_sem.at[g])

    def piece(ref, g, c):
        return ref.at[g, :, pl.ds(pl.multiple_of(c * COLS, COLS), COLS)]

    def p_copy(g, c):
        return pltpu.make_async_remote_copy(piece(hout, g, c), piece(recvp, g, c), p_send.at[g, c], p_recv.at[g, c], device_id=peer, device_id_type=MESH)

    def d_copy(g, c):
        return pltpu.make_async_remote_copy(piece(recvp, g, c), piece(recvd, g, c), d_send.at[g, c], d_recv.at[g, c], device_id=peer, device_id_type=MESH)

    def h_copy(g, c):
        return pltpu.make_async_remote_copy(piece(hout, g, c), piece(hbuf, g, c), h_send.at[g, c], h_recv.at[g, c], device_id=nxt, device_id_type=MESH)

    first = pp == 0
    last = pp == n_pp - 1

    @pl.when(first)
    def _():
        for g in range(n_groups):
            hid_copy(g).start()
    for copy in qkv_copies():
        copy.start()

    def start_kv_wo():
        for slot in range(SLOTS):
            for copy in kv_copies(slot, slot):
                copy.start()
        for copy in wo_copies():
            copy.start()

    @pl.when(pp > 0)
    def _():
        start_kv_wo()
        for j in range(n_gu):
            for copy in gu_copies(j):
                copy.start()

    for g in range(n_groups):
        angles = pos_ref[g].astype(F32) * freq_ref[...]
        cos_ref[g] = jnp.cos(angles)
        sin_ref[g] = jnp.sin(angles)

    barrier = pltpu.get_barrier_semaphore()
    pl.semaphore_signal(barrier, inc=1, device_id=peer, device_id_type=MESH)

    @pl.when(jnp.logical_not(last))
    def _():
        pl.semaphore_signal(barrier, inc=1, device_id=nxt, device_id_type=MESH)

    @pl.when(pp > 0)
    def _():
        pl.semaphore_signal(barrier, inc=1, device_id=prv, device_id_type=MESH)
    ends = jnp.logical_or(first, last)

    @pl.when(ends)
    def _():
        pl.semaphore_wait(barrier, 2)

    @pl.when(jnp.logical_not(ends))
    def _():
        pl.semaphore_wait(barrier, 3)

    def norm_rows(g, gain_ref, with_partial):
        def body(r, carry):
            rows = pl.ds(pl.multiple_of(r * NORM_ROWS, NORM_ROWS), NORM_ROWS)
            x = hbuf[g, rows, :].astype(F32)
            if with_partial:
                part = (hout[g, rows, :].astype(F32) + recvp[g, rows, :].astype(F32)).astype(BF16)
                x = (x + part.astype(F32)).astype(BF16)
                hbuf[g, rows, :] = x
                x = x.astype(F32)
            inv = lax.rsqrt(jnp.mean(x * x, axis=-1, keepdims=True) + NORM_EPS)
            nbuf[rows, :] = (x * inv * gain_ref[...].astype(F32)).astype(BF16)
            return carry
        lax.fori_loop(0, n_batch // NORM_ROWS, body, 0)

    def attention_phase(g, carry):
        @pl.when(first)
        def _():
            hid_copy(g).wait()

        @pl.when(pp > 0)
        def _():
            for c in range(n_chunk):
                h_copy(g, c).wait_recv()

        norm_rows(g, ga_ref, False)
        cosine = cos_ref[g]
        sine = sin_ref[g]
        half = hd // 2

        @pl.when(g == 0)
        def _():
            for i, copy in enumerate(qkv_copies()):
                copy.wait()
                if i == 0:
                    pl.when(first)(start_kv_wo)

        for which in range(3):
            for c in range(hw // COLS):
                cols = slice(c * COLS, (c + 1) * COLS)
                prod_t = jnp.dot(nbuf[...], wmix[which, :, cols], preferred_element_type=F32).T
                for i in range(COLS // hd):
                    head = c * (COLS // hd) + i
                    a = prod_t[i * hd:i * hd + half]
                    b = prod_t[i * hd + half:(i + 1) * hd]
                    if which < 2:
                        a, b = a * cosine - b * sine, b * cosine + a * sine
                    both = jnp.concatenate([a, b], axis=0).astype(BF16)
                    if which == 0:
                        qt[head * hd:(head + 1) * hd, :] = both
                    else:
                        dst = knew if which == 1 else vnew
                        dst[g, head] = both

        pos = pos_ref[g]
        row_id = lax.broadcasted_iota(jnp.int32, (seq, n_batch), 0)
        hit = row_id == pos
        seen = row_id <= pos

        def head_body(h, inner):
            item = g * heads + h
            slot = lax.rem(item, SLOTS)
            for copy in kv_copies(item, slot):
                copy.wait()
            rows = pl.ds(pl.multiple_of(h * hd, hd), hd)
            q = qt[rows, :].astype(F32)
            fresh = jnp.sum(q * knew[g, h].astype(F32), axis=0, keepdims=True)
            for s in range(seq):
                sc[s:s + 1, :] = jnp.sum(ring[slot, s].astype(F32) * q, axis=0, keepdims=True)
            scores = jnp.where(hit, fresh, sc[...]) * hd ** -0.5
            scores = jnp.where(seen, scores, -jnp.inf)
            top = jnp.max(scores, axis=0, keepdims=True)
            expd = jnp.exp(scores - top)
            probs = (expd / jnp.sum(expd, axis=0, keepdims=True)).astype(BF16).astype(F32)
            sc[...] = jnp.where(hit, 0.0, probs)
            acc = jnp.sum(jnp.where(hit, probs, 0.0), axis=0, keepdims=True) * vnew[g, h].astype(F32)
            for s in range(seq):
                acc = acc + sc[s:s + 1, :] * ring[slot, seq + s].astype(F32)
            qt[rows, :] = acc.astype(BF16)

            @pl.when(item + SLOTS < n_kv)
            def _():
                for copy in kv_copies(item + SLOTS, slot):
                    copy.start()

            @pl.when(jnp.logical_and(jnp.logical_and(first, item + SLOTS < n_kv), lax.rem(item, SLOTS) == SLOTS // 2))
            def _():
                for copy in gu_copies(item // SLOTS):
                    copy.start()

            @pl.when(item + SLOTS == n_kv)
            def _():
                @pl.when(first)
                def _():
                    for j in range((n_kv - SLOTS) // SLOTS, n_gu):
                        for copy in gu_copies(j):
                            copy.start()
                for i in range(3):
                    wd_copy(i).start()
            return inner
        lax.fori_loop(0, heads, head_body, 0)

        @pl.when(g == 0)
        def _():
            for copy in wo_copies():
                copy.wait()
        for c in range(hw // COLS):
            cols = slice(c * COLS, (c + 1) * COLS)
            nbuf[:, cols] = qt[cols, :].astype(F32).T.astype(BF16)

        for c in range(n_chunk):
            at, col = divmod(c * COLS, hw)
            part = jnp.dot(nbuf[:, 0:hw], wmix[3, at * hw:(at + 1) * hw, col:col + COLS], preferred_element_type=F32)
            hout[g, :, c * COLS:(c + 1) * COLS] = part.astype(BF16)
        for c in range(n_chunk):
            p_copy(g, c).start()

        @pl.when(g == n_groups - 1)
        def _():
            wd_copy(3).start()
        return carry

    def mlp_phase(g, carry):
        for c in range(n_chunk):
            p_copy(g, c).wait()
        norm_rows(g, gm_ref, True)

        some = n_gu // 2

        def finish_some(part):
            @pl.when(g > 0)
            def _():
                for c in range(n_chunk // 2):
                    finish_piece(g - 1, part * (n_chunk // 2) + c)

        def gu_body(part, inner):
            tiles = [part * some + i for i in range(some)]

            @pl.when(g == 0)
            def _():
                for j in tiles:
                    for copy in gu_copies(j):
                        copy.wait()
            pl.when(part > 0)(lambda: finish_some(part - 1))
            for j in tiles:
                gate = jnp.dot(nbuf[...], wg_v[j], preferred_element_type=F32)
                up = jnp.dot(nbuf[...], wu_v[j], preferred_element_type=F32)
                ubuf[:, pl.ds(pl.multiple_of(j * COLS, COLS), COLS)] = (jax.nn.silu(gate) * up).astype(BF16)
            return inner
        lax.fori_loop(0, 2, gu_body, 0)
        finish_some(1)

        for c in range(n_chunk):
            at, col = divmod(c * COLS, hw)
            if col == 0:
                @pl.when(g == 0)
                def _():
                    for i in range(n_deep):
                        wd_copy(at * n_deep + i).wait()
            acc = None
            for i in range(n_deep):
                prod = jnp.dot(ubuf[:, i * d_model:(i + 1) * d_model], wmix[at * n_deep + i, :, col:col + COLS], preferred_element_type=F32)
                acc = prod if acc is None else acc + prod
            recvp[g, :, c * COLS:(c + 1) * COLS] = acc.astype(BF16)
            d_copy(g, c).start()
        return carry

    def finish_piece(g, c):
        d_copy(g, c).wait()
        cols = pl.ds(pl.multiple_of(c * COLS, COLS), COLS)
        part = (recvd[g, :, cols].astype(F32) + recvp[g, :, cols].astype(F32)).astype(BF16)
        hout[g, :, cols] = (hbuf[g, :, cols].astype(F32) + part.astype(F32)).astype(BF16)

        @pl.when(jnp.logical_not(last))
        def _():
            h_copy(g, c).start()

    lax.fori_loop(0, n_groups, attention_phase, 0)
    lax.fori_loop(0, n_groups, mlp_phase, 0)
    for c in range(n_chunk):
        finish_piece(n_groups - 1, c)

    @pl.when(jnp.logical_not(last))
    def _():
        for g in range(n_groups):
            for c in range(n_chunk):
                h_copy(g, c).wait_send()


def run_layer(dims, *args):
    n_groups, n_batch, d_model, heads, seq, hd, ff, n_pp, n_tp = dims
    hw = heads * hd
    n_chunk = d_model // COLS
    n_gu = ff // COLS
    assert ff * d_model == 4 * d_model * hw
    vmem = pl.BlockSpec(memory_space=pltpu.VMEM)
    hbm = pl.BlockSpec(memory_space=pltpu.HBM)
    dma = pltpu.SemaphoreType.DMA
    return pl.pallas_call(
        functools.partial(layer_kernel, dims),
        out_shape=(jax.ShapeDtypeStruct((n_groups, n_batch, d_model), BF16),
                   jax.ShapeDtypeStruct((n_groups, heads, hd, n_batch), BF16),
                   jax.ShapeDtypeStruct((n_groups, heads, hd, n_batch), BF16)),
        in_specs=[hbm] + [vmem] * 4 + [hbm] * 10,
        out_specs=(vmem, vmem, vmem),
        scratch_shapes=[
            pltpu.VMEM((4, d_model, hw), BF16),
            pltpu.VMEM((n_gu, d_model, COLS), BF16),
            pltpu.VMEM((n_gu, d_model, COLS), BF16),
            pltpu.VMEM((SLOTS, 2 * seq, hd, n_batch), BF16),
            pltpu.VMEM((n_groups, n_batch, d_model), BF16),
            pltpu.VMEM((n_groups, n_batch, d_model), BF16),
            pltpu.VMEM((n_groups, n_batch, d_model), BF16),
            pltpu.VMEM((n_batch, d_model), BF16),
            pltpu.VMEM((hw, n_batch), BF16),
            pltpu.VMEM((n_batch, ff), BF16),
            pltpu.VMEM((seq, n_batch), F32),
            pltpu.VMEM((n_groups, hd // 2, n_batch), F32),
            pltpu.VMEM((n_groups, hd // 2, n_batch), F32),
            dma((n_groups,)), dma((3,)), dma((d_model // hw,)), dma((4,)), dma((2, n_gu)), dma((SLOTS, 2)),
            dma((n_groups, n_chunk)), dma((n_groups, n_chunk)), dma((n_groups, n_chunk)),
            dma((n_groups, n_chunk)), dma((n_groups, n_chunk)), dma((n_groups, n_chunk)),
        ],
        compiler_params=pltpu.CompilerParams(collective_id=0, has_side_effects=True, vmem_limit_bytes=67043328),
        name="layer",
    )(*args)


def keep_kernel(dims, pos_hbm, kc, vc, kout, vout, todo_hbm, kb, vb, pos, todo, flags, in_sem, out_sem, pos_sem, todo_sem):
    n_groups, n_batch, _, heads, seq, _, _, n_pp, _ = dims
    n_slab = n_groups * seq
    n_items = n_groups * heads
    ahead = KEEP_SLOTS // 2
    last = lax.axis_index("pp") == n_pp - 1

    def loads(i):
        slot = lax.rem(i, KEEP_SLOTS)
        g, h = i // heads, lax.rem(i, heads)
        return (pltpu.make_async_copy(kc.at[g, h], kb.at[slot], in_sem.at[0, slot]),
                pltpu.make_async_copy(vc.at[g, h], vb.at[slot], in_sem.at[1, slot]))

    def stores(i):
        slot = lax.rem(i, KEEP_SLOTS)
        g, h = i // heads, lax.rem(i, heads)
        return (pltpu.make_async_copy(kb.at[slot], kout.at[g, h], out_sem.at[0, slot]),
                pltpu.make_async_copy(vb.at[slot], vout.at[g, h], out_sem.at[1, slot]))

    @pl.when(last)
    def _():
        for i in range(ahead):
            for copy in loads(i):
                copy.start()

        pos_copy = pltpu.make_async_copy(pos_hbm, pos, pos_sem)
        pos_copy.start()
        pos_copy.wait()

        def clear(i, carry):
            flags[i] = 0
            todo[i + 1] = 0
            return carry
        lax.fori_loop(0, n_slab, clear, 0)
        for g in range(n_groups):
            def mark(b, carry):
                flags[g * seq + pos[g, b]] = 1
                return carry
            lax.fori_loop(0, n_batch, mark, 0)

        def pick(i, count):
            hit = flags[i]

            @pl.when(hit == 1)
            def _():
                todo[count + 1] = i
            return count + hit
        todo[0] = lax.fori_loop(0, n_slab, pick, jnp.int32(0))
        todo_copy = pltpu.make_async_copy(todo, todo_hbm, todo_sem)
        todo_copy.start()

        def body(i, carry):
            for copy in loads(i):
                copy.wait()
            for copy in stores(i):
                copy.start()

            @pl.when(i + ahead < n_items)
            def _():
                @pl.when(i >= ahead)
                def _():
                    for copy in stores(i - ahead):
                        copy.wait()
                for copy in loads(i + ahead):
                    copy.start()
            return carry
        lax.fori_loop(0, n_items, body, 0)
        for i in range(n_items - 2 * ahead, n_items):
            for copy in stores(i):
                copy.wait()
        todo_copy.wait()


def keep_old(dims, positions, key_t, value_t):
    n_groups, n_batch, _, heads, seq, hd, _, _, _ = dims
    hbm = pl.BlockSpec(memory_space=pltpu.HBM)
    dma = pltpu.SemaphoreType.DMA
    return pl.pallas_call(
        functools.partial(keep_kernel, dims),
        out_shape=(jax.ShapeDtypeStruct(key_t.shape, BF16), jax.ShapeDtypeStruct(value_t.shape, BF16),
                   jax.ShapeDtypeStruct((n_groups * seq + 1,), jnp.int32)),
        in_specs=[hbm] * 3,
        out_specs=(hbm, hbm, hbm),
        scratch_shapes=[
            pltpu.VMEM((KEEP_SLOTS, seq, hd, n_batch), BF16),
            pltpu.VMEM((KEEP_SLOTS, seq, hd, n_batch), BF16),
            pltpu.SMEM((n_groups, n_batch), jnp.int32),
            pltpu.SMEM((n_groups * seq + 1,), jnp.int32),
            pltpu.SMEM((n_groups * seq,), jnp.int32),
            dma((2, KEEP_SLOTS)), dma((2, KEEP_SLOTS)), dma, dma,
        ],
        compiler_params=pltpu.CompilerParams(vmem_limit_bytes=67043328),
        name="cache_keep",
    )(positions, key_t, value_t)


def write_kernel(dims, todo_hbm, pos_hbm, knew_hbm, vnew_hbm, kc, vc, kold, vold, kout, vout,
                 todo, pos_ref, knew, vnew, kb, vb, in_sem, out_sem, small_sem):
    n_groups, _, _, _, seq, _, _, n_pp, _ = dims
    ahead = WRITE_SLOTS // 2
    last = lax.axis_index("pp") == n_pp - 1
    small = [pltpu.make_async_copy(src, dst, small_sem.at[i]) for i, (src, dst) in enumerate(
        ((todo_hbm, todo), (pos_hbm, pos_ref), (knew_hbm, knew), (vnew_hbm, vnew)))]
    for copy in small:
        copy.start()
    small[0].wait()
    count = jnp.where(last, todo[0], n_groups * seq)

    def place(i):
        entry = jnp.where(last, todo[i + 1], i)
        return entry // seq, lax.rem(entry, seq), lax.rem(i, WRITE_SLOTS)

    def loads(i):
        g, s, slot = place(i)
        return (pltpu.make_async_copy(kc.at[g, :, s], kb.at[slot], in_sem.at[0, slot]),
                pltpu.make_async_copy(vc.at[g, :, s], vb.at[slot], in_sem.at[1, slot]))

    def stores(i):
        g, s, slot = place(i)
        return (pltpu.make_async_copy(kb.at[slot], kout.at[g, :, s], out_sem.at[0, slot]),
                pltpu.make_async_copy(vb.at[slot], vout.at[g, :, s], out_sem.at[1, slot]))

    for i in range(ahead):
        @pl.when(i < count)
        def _():
            for copy in loads(i):
                copy.start()

    for copy in small[1:]:
        copy.wait()

    def body(i, carry):
        g, s, slot = place(i)
        for copy in loads(i):
            copy.wait()
        hit = (pos_ref[g] == s)[None]
        for new, buf in ((knew, kb), (vnew, vb)):
            buf[slot] = jnp.where(hit, new[g].astype(F32), buf[slot].astype(F32)).astype(BF16)
        for copy in stores(i):
            copy.start()

        @pl.when(i + ahead < count)
        def _():
            @pl.when(i >= ahead)
            def _():
                for copy in stores(i - ahead):
                    copy.wait()
            for copy in loads(i + ahead):
                copy.start()
        return carry
    lax.fori_loop(0, count, body, 0)

    def drain(i, carry):
        for copy in stores(i):
            copy.wait()
        return carry
    lax.fori_loop(jnp.maximum(count - 2 * ahead, 0), count, drain, 0)


def write_new(dims, todo, pos, key_new, value_new, key_t, value_t, key_old, value_old):
    n_groups, n_batch, _, heads, seq, hd, _, _, _ = dims
    hbm = pl.BlockSpec(memory_space=pltpu.HBM)
    dma = pltpu.SemaphoreType.DMA
    return pl.pallas_call(
        functools.partial(write_kernel, dims),
        out_shape=(jax.ShapeDtypeStruct(key_t.shape, BF16), jax.ShapeDtypeStruct(value_t.shape, BF16)),
        in_specs=[hbm] * 8,
        out_specs=(hbm, hbm),
        scratch_shapes=[
            pltpu.SMEM((n_groups * seq + 1,), jnp.int32),
            pltpu.VMEM((n_groups, 1, n_batch), jnp.int32),
            pltpu.VMEM((n_groups, heads, hd, n_batch), BF16),
            pltpu.VMEM((n_groups, heads, hd, n_batch), BF16),
            pltpu.VMEM((WRITE_SLOTS, heads, hd, n_batch), BF16),
            pltpu.VMEM((WRITE_SLOTS, heads, hd, n_batch), BF16),
            dma((2, WRITE_SLOTS)), dma((2, WRITE_SLOTS)), dma((4,)),
        ],
        input_output_aliases={6: 0, 7: 1},
        compiler_params=pltpu.CompilerParams(vmem_limit_bytes=67043328),
        cost_estimate=pl.CostEstimate(flops=n_groups * n_batch * heads * seq * hd * 40, bytes_accessed=8 * key_t.size, transcendentals=0),
        name="cache_write",
    )(todo, pos, key_new, value_new, key_t, value_t, key_old, value_old)


def solution(mesh):
    n_pp = mesh.shape["pp"]
    n_tp = mesh.shape["tp"]
    cache_spec = P("pp", "dp", None, "tp", None, None)
    col_spec = P("pp", None, "tp")
    row_spec = P("pp", "tp", None)
    gain_spec = P("pp", None)
    in_specs = (P("dp", None, None), P("dp", None), cache_spec, cache_spec, gain_spec, col_spec, col_spec, col_spec, row_spec, gain_spec, col_spec, col_spec, row_spec)
    out_specs = (P("dp", None, None), cache_spec, cache_spec)

    def per_device(hidden, positions, key_cache, value_cache, attn_norm, w_query, w_key, w_value, w_out, mlp_norm, w_gate, w_up, w_down):
        _, n_groups, n_batch, heads, seq, hd = key_cache.shape
        d_model = hidden.shape[-1]
        ff = w_gate.shape[-1]
        dims = (n_groups, n_batch, d_model, heads, seq, hd, ff, n_pp, n_tp)
        freqs = jnp.asarray(np.broadcast_to(rope_freqs(hd)[:, None], (hd // 2, n_batch)))
        key_t = jnp.transpose(key_cache[0], (0, 2, 3, 4, 1))
        value_t = jnp.transpose(value_cache[0], (0, 2, 3, 4, 1))
        pos = positions[:, None, :]
        key_old, value_old, todo = keep_old(dims, positions, key_t, value_t)
        state, key_new, value_new = run_layer(
            dims, todo, freqs, pos, attn_norm, mlp_norm, hidden, key_t, value_t,
            w_query[0], w_key[0], w_value[0], w_out[0], w_gate[0], w_up[0], w_down[0])

        stage = lax.axis_index("pp")
        from_last = [lax.ppermute(state, "pp", [(n_pp - 1, dst)]) for dst in range(1, n_pp - 1)]
        key_t, value_t = write_new(dims, todo, pos, key_new, value_new, key_t, value_t, key_old, value_old)
        from_last[0], key_t = lax.optimization_barrier((from_last[0], key_t))
        from_last.append(lax.ppermute(from_last[0], "pp", [(1, 0)]))
        final = jnp.where(stage == n_pp - 1, state, sum(from_last[1:], from_last[0]))
        return final, jnp.transpose(key_t, (0, 4, 1, 2, 3))[None], jnp.transpose(value_t, (0, 4, 1, 2, 3))[None]

    return jax.shard_map(per_device, mesh=mesh, in_specs=in_specs, out_specs=out_specs, check_vma=False)
```

```python
import functools
import math
import jax
import jax.numpy as jnp
import numpy as np
from jax import lax
from jax.experimental import pallas as pl
from jax.experimental.pallas import tpu as pltpu
from jax.sharding import PartitionSpec as P

ROPE_THETA = 500000.0
SCALE_FACTOR = 8.0
LOW_FACTOR = 1.0
HIGH_FACTOR = 4.0
ORIG_CONTEXT = 8192.0
NORM_EPS = 1e-5
MESH = pl.DeviceIdType.MESH
F32 = jnp.float32
BF16 = jnp.bfloat16

COLS = 512
SLOTS = 8
NORM_ROWS = 64
KEEP_SLOTS = 16
WRITE_SLOTS = 24


def rope_freqs(head_dim):
    freq_index = np.arange(head_dim // 2, dtype=np.float64)
    base_freq = ROPE_THETA ** (-2.0 * freq_index / head_dim)
    wave_len = 2.0 * math.pi / base_freq
    smooth_t = (ORIG_CONTEXT / wave_len - LOW_FACTOR) / (HIGH_FACTOR - LOW_FACTOR)
    mixed_freq = (1.0 - smooth_t) * base_freq / SCALE_FACTOR + smooth_t * base_freq
    long_freq = np.where(wave_len > ORIG_CONTEXT / LOW_FACTOR, base_freq / SCALE_FACTOR, mixed_freq)
    return np.where(wave_len < ORIG_CONTEXT / HIGH_FACTOR, base_freq, long_freq).astype(np.float32)


def layer_kernel(dims, after, pos_ref, ga_ref, gm_ref, hid, kc, vc, wq, wk, wv, wo, wg, wu, wd,
                 hout, knew, vnew,
                 wmix, wg_v, wu_v, ring, hbuf, recvp, recvd, nbuf, qt, ubuf, sc, cos_ref, sin_ref,
                 hid_sem, wqkv_sem, wo_sem, wd_sem, gu_sem, ring_sem,
                 p_send, p_recv, d_send, d_recv, h_send, h_recv):
    n_groups, n_batch, d_model, heads, seq, hd, ff, n_pp, n_tp = dims
    hw = heads * hd
    n_chunk = d_model // COLS
    n_gu = ff // COLS
    n_half = d_model // hw
    n_deep = ff // d_model
    pp = lax.axis_index("pp")
    tp = lax.axis_index("tp")
    peer = {"tp": lax.rem(tp + 1, n_tp)}
    nxt = {"pp": lax.rem(pp + 1, n_pp)}
    prv = {"pp": lax.rem(pp + n_pp - 1, n_pp)}

    n_kv = n_groups * heads

    def kv_copies(item, slot):
        g = item // heads
        h = lax.rem(item, heads)
        return (pltpu.make_async_copy(kc.at[g, h], ring.at[slot, pl.ds(0, seq)], ring_sem.at[slot, 0]),
                pltpu.make_async_copy(vc.at[g, h], ring.at[slot, pl.ds(seq, seq)], ring_sem.at[slot, 1]))

    def wd_copy(i):
        return pltpu.make_async_copy(wd.at[pl.ds(i % n_deep * d_model, d_model), pl.ds(i // n_deep * hw, hw)], wmix.at[i], wd_sem.at[i])

    def gu_copies(j):
        cols = pl.ds(pl.multiple_of(j * COLS, COLS), COLS)
        return (pltpu.make_async_copy(wg.at[:, cols], wg_v.at[j], gu_sem.at[0, j]),
                pltpu.make_async_copy(wu.at[:, cols], wu_v.at[j], gu_sem.at[1, j]))

    def qkv_copies():
        return [pltpu.make_async_copy(src, wmix.at[i], wqkv_sem.at[i]) for i, src in enumerate((wq, wk, wv))]

    def wo_copies():
        return [pltpu.make_async_copy(wo.at[:, pl.ds(i * hw, hw)], wmix.at[3, pl.ds(i * hw, hw)], wo_sem.at[i]) for i in range(n_half)]

    def hid_copy(g):
        return pltpu.make_async_copy(hid.at[g], hbuf.at[g], hid_sem.at[g])

    def piece(ref, g, c):
        return ref.at[g, :, pl.ds(pl.multiple_of(c * COLS, COLS), COLS)]

    def p_copy(g, c):
        return pltpu.make_async_remote_copy(piece(hout, g, c), piece(recvp, g, c), p_send.at[g, c], p_recv.at[g, c], device_id=peer, device_id_type=MESH)

    def d_copy(g, c):
        return pltpu.make_async_remote_copy(piece(recvp, g, c), piece(recvd, g, c), d_send.at[g, c], d_recv.at[g, c], device_id=peer, device_id_type=MESH)

    def h_copy(g, c):
        return pltpu.make_async_remote_copy(piece(hout, g, c), piece(hbuf, g, c), h_send.at[g, c], h_recv.at[g, c], device_id=nxt, device_id_type=MESH)

    first = pp == 0
    last = pp == n_pp - 1

    @pl.when(first)
    def _():
        for g in range(n_groups):
            hid_copy(g).start()
    for copy in qkv_copies():
        copy.start()

    for slot in range(SLOTS):
        for copy in kv_copies(slot, slot):
            copy.start()
    for copy in wo_copies():
        copy.start()
    for j in range(n_gu // 2):
        for copy in gu_copies(j):
            copy.start()

    def start_more():
        for j in range(n_gu // 2, n_gu):
            for copy in gu_copies(j):
                copy.start()
    pl.when(pp > 0)(start_more)

    freq_id = lax.broadcasted_iota(jnp.int32, (hd // 2, n_batch), 0)
    freqs = jnp.zeros((hd // 2, n_batch), F32)
    for i, freq in enumerate(rope_freqs(hd)):
        freqs = jnp.where(freq_id == i, float(freq), freqs)
    for g in range(n_groups):
        angles = pos_ref[g].astype(F32) * freqs
        cos_ref[g] = jnp.cos(angles)
        sin_ref[g] = jnp.sin(angles)

    barrier = pltpu.get_barrier_semaphore()
    pl.semaphore_signal(barrier, inc=1, device_id=peer, device_id_type=MESH)

    @pl.when(jnp.logical_not(last))
    def _():
        pl.semaphore_signal(barrier, inc=1, device_id=nxt, device_id_type=MESH)

    @pl.when(pp > 0)
    def _():
        pl.semaphore_signal(barrier, inc=1, device_id=prv, device_id_type=MESH)
    ends = jnp.logical_or(first, last)

    @pl.when(ends)
    def _():
        pl.semaphore_wait(barrier, 2)

    @pl.when(jnp.logical_not(ends))
    def _():
        pl.semaphore_wait(barrier, 3)

    def norm_rows(g, gain_ref, with_partial):
        def body(r, carry):
            rows = pl.ds(pl.multiple_of(r * NORM_ROWS, NORM_ROWS), NORM_ROWS)
            x = hbuf[g, rows, :].astype(F32)
            if with_partial:
                part = (hout[g, rows, :].astype(F32) + recvp[g, rows, :].astype(F32)).astype(BF16)
                x = (x + part.astype(F32)).astype(BF16)
                hbuf[g, rows, :] = x
                x = x.astype(F32)
            inv = lax.rsqrt(jnp.mean(x * x, axis=-1, keepdims=True) + NORM_EPS)
            nbuf[rows, :] = (x * inv * gain_ref[...].astype(F32)).astype(BF16)
            return carry
        lax.fori_loop(0, n_batch // NORM_ROWS, body, 0)

    def attention_phase(g, carry):
        @pl.when(first)
        def _():
            hid_copy(g).wait()

        @pl.when(pp > 0)
        def _():
            for c in range(n_chunk):
                h_copy(g, c).wait_recv()

        norm_rows(g, ga_ref, False)
        cosine = cos_ref[g]
        sine = sin_ref[g]
        half = hd // 2

        @pl.when(g == 0)
        def _():
            for copy in qkv_copies():
                copy.wait()

        for which in range(3):
            for c in range(hw // COLS):
                cols = slice(c * COLS, (c + 1) * COLS)
                prod_t = jnp.dot(nbuf[...], wmix[which, :, cols], preferred_element_type=F32).T
                for i in range(COLS // hd):
                    head = c * (COLS // hd) + i
                    a = prod_t[i * hd:i * hd + half]
                    b = prod_t[i * hd + half:(i + 1) * hd]
                    if which < 2:
                        a, b = a * cosine - b * sine, b * cosine + a * sine
                    both = jnp.concatenate([a, b], axis=0).astype(BF16)
                    if which == 0:
                        qt[head * hd:(head + 1) * hd, :] = both
                    else:
                        dst = knew if which == 1 else vnew
                        dst[g, head] = both

        pos = pos_ref[g]
        row_id = lax.broadcasted_iota(jnp.int32, (seq, n_batch), 0)
        hit = row_id == pos
        seen = row_id <= pos

        def head_body(h, inner):
            item = g * heads + h
            slot = lax.rem(item, SLOTS)
            for copy in kv_copies(item, slot):
                copy.wait()
            rows = pl.ds(pl.multiple_of(h * hd, hd), hd)
            q = qt[rows, :].astype(F32)
            fresh = jnp.sum(q * knew[g, h].astype(F32), axis=0, keepdims=True)
            for s in range(seq):
                sc[s:s + 1, :] = jnp.sum(ring[slot, s].astype(F32) * q, axis=0, keepdims=True)
            scores = jnp.where(hit, fresh, sc[...]) * hd ** -0.5
            scores = jnp.where(seen, scores, -jnp.inf)
            top = jnp.max(scores, axis=0, keepdims=True)
            expd = jnp.exp(scores - top)
            probs = (expd / jnp.sum(expd, axis=0, keepdims=True)).astype(BF16).astype(F32)
            sc[...] = jnp.where(hit, 0.0, probs)
            acc = jnp.sum(jnp.where(hit, probs, 0.0), axis=0, keepdims=True) * vnew[g, h].astype(F32)
            for s in range(seq):
                acc = acc + sc[s:s + 1, :] * ring[slot, seq + s].astype(F32)
            qt[rows, :] = acc.astype(BF16)

            @pl.when(item + SLOTS < n_kv)
            def _():
                for copy in kv_copies(item + SLOTS, slot):
                    copy.start()

            @pl.when(item + SLOTS == n_kv)
            def _():
                for i in range(3):
                    wd_copy(i).start()
            return inner
        lax.fori_loop(0, heads, head_body, 0)
        pl.when(jnp.logical_and(first, g == 0))(start_more)

        @pl.when(g == 0)
        def _():
            for copy in wo_copies():
                copy.wait()
        for c in range(hw // COLS):
            cols = slice(c * COLS, (c + 1) * COLS)
            nbuf[:, cols] = qt[cols, :].astype(F32).T.astype(BF16)

        for c in range(n_chunk):
            at, col = divmod(c * COLS, hw)
            part = jnp.dot(nbuf[:, 0:hw], wmix[3, at * hw:(at + 1) * hw, col:col + COLS], preferred_element_type=F32)
            hout[g, :, c * COLS:(c + 1) * COLS] = part.astype(BF16)
        for c in range(n_chunk):
            p_copy(g, c).start()

        @pl.when(g == n_groups - 1)
        def _():
            wd_copy(3).start()
        return carry

    def mlp_phase(g, carry):
        for c in range(n_chunk):
            p_copy(g, c).wait()
        norm_rows(g, gm_ref, True)

        some = n_gu // 2

        def finish_some(part):
            @pl.when(g > 0)
            def _():
                for c in range(n_chunk // 2):
                    finish_piece(g - 1, part * (n_chunk // 2) + c)

        def gu_body(part, inner):
            tiles = [part * some + i for i in range(some)]

            @pl.when(g == 0)
            def _():
                for j in tiles:
                    for copy in gu_copies(j):
                        copy.wait()
            pl.when(part > 0)(lambda: finish_some(part - 1))
            for j in tiles:
                gate = jnp.dot(nbuf[...], wg_v[j], preferred_element_type=F32)
                up = jnp.dot(nbuf[...], wu_v[j], preferred_element_type=F32)
                ubuf[:, pl.ds(pl.multiple_of(j * COLS, COLS), COLS)] = (jax.nn.silu(gate) * up).astype(BF16)
            return inner
        lax.fori_loop(0, 2, gu_body, 0)
        finish_some(1)

        for c in range(n_chunk):
            at, col = divmod(c * COLS, hw)
            if col == 0:
                @pl.when(g == 0)
                def _():
                    for i in range(n_deep):
                        wd_copy(at * n_deep + i).wait()
            acc = None
            for i in range(n_deep):
                prod = jnp.dot(ubuf[:, i * d_model:(i + 1) * d_model], wmix[at * n_deep + i, :, col:col + COLS], preferred_element_type=F32)
                acc = prod if acc is None else acc + prod
            recvp[g, :, c * COLS:(c + 1) * COLS] = acc.astype(BF16)
            d_copy(g, c).start()
        return carry

    def finish_piece(g, c):
        d_copy(g, c).wait()
        cols = pl.ds(pl.multiple_of(c * COLS, COLS), COLS)
        part = (recvd[g, :, cols].astype(F32) + recvp[g, :, cols].astype(F32)).astype(BF16)
        hout[g, :, cols] = (hbuf[g, :, cols].astype(F32) + part.astype(F32)).astype(BF16)

        @pl.when(jnp.logical_not(last))
        def _():
            h_copy(g, c).start()

    lax.fori_loop(0, n_groups, attention_phase, 0)
    lax.fori_loop(0, n_groups, mlp_phase, 0)
    for c in range(n_chunk):
        finish_piece(n_groups - 1, c)

    @pl.when(jnp.logical_not(last))
    def _():
        for g in range(n_groups):
            for c in range(n_chunk):
                h_copy(g, c).wait_send()


def run_layer(dims, *args):
    n_groups, n_batch, d_model, heads, seq, hd, ff, n_pp, n_tp = dims
    hw = heads * hd
    n_chunk = d_model // COLS
    n_gu = ff // COLS
    assert ff * d_model == 4 * d_model * hw
    vmem = pl.BlockSpec(memory_space=pltpu.VMEM)
    hbm = pl.BlockSpec(memory_space=pltpu.HBM)
    dma = pltpu.SemaphoreType.DMA
    return pl.pallas_call(
        functools.partial(layer_kernel, dims),
        out_shape=(jax.ShapeDtypeStruct((n_groups, n_batch, d_model), BF16),
                   jax.ShapeDtypeStruct((n_groups, heads, hd, n_batch), BF16),
                   jax.ShapeDtypeStruct((n_groups, heads, hd, n_batch), BF16)),
        in_specs=[hbm] + [vmem] * 3 + [hbm] * 10,
        out_specs=(vmem, vmem, vmem),
        scratch_shapes=[
            pltpu.VMEM((4, d_model, hw), BF16),
            pltpu.VMEM((n_gu, d_model, COLS), BF16),
            pltpu.VMEM((n_gu, d_model, COLS), BF16),
            pltpu.VMEM((SLOTS, 2 * seq, hd, n_batch), BF16),
            pltpu.VMEM((n_groups, n_batch, d_model), BF16),
            pltpu.VMEM((n_groups, n_batch, d_model), BF16),
            pltpu.VMEM((n_groups, n_batch, d_model), BF16),
            pltpu.VMEM((n_batch, d_model), BF16),
            pltpu.VMEM((hw, n_batch), BF16),
            pltpu.VMEM((n_batch, ff), BF16),
            pltpu.VMEM((seq, n_batch), F32),
            pltpu.VMEM((n_groups, hd // 2, n_batch), F32),
            pltpu.VMEM((n_groups, hd // 2, n_batch), F32),
            dma((n_groups,)), dma((3,)), dma((d_model // hw,)), dma((4,)), dma((2, n_gu)), dma((SLOTS, 2)),
            dma((n_groups, n_chunk)), dma((n_groups, n_chunk)), dma((n_groups, n_chunk)),
            dma((n_groups, n_chunk)), dma((n_groups, n_chunk)), dma((n_groups, n_chunk)),
        ],
        compiler_params=pltpu.CompilerParams(collective_id=0, has_side_effects=True, vmem_limit_bytes=67043328),
        name="layer",
    )(*args)


def keep_kernel(dims, pos_hbm, kc, vc, kout, vout, todo_hbm, kb, vb, pos, todo, flags, in_sem, out_sem, pos_sem, todo_sem):
    n_groups, n_batch, _, heads, seq, _, _, n_pp, _ = dims
    n_slab = n_groups * seq
    n_items = n_groups * heads
    ahead = KEEP_SLOTS // 2
    last = lax.axis_index("pp") == n_pp - 1

    def loads(i):
        slot = lax.rem(i, KEEP_SLOTS)
        g, h = i // heads, lax.rem(i, heads)
        return (pltpu.make_async_copy(kc.at[g, h], kb.at[slot], in_sem.at[0, slot]),
                pltpu.make_async_copy(vc.at[g, h], vb.at[slot], in_sem.at[1, slot]))

    def stores(i):
        slot = lax.rem(i, KEEP_SLOTS)
        g, h = i // heads, lax.rem(i, heads)
        return (pltpu.make_async_copy(kb.at[slot], kout.at[g, h], out_sem.at[0, slot]),
                pltpu.make_async_copy(vb.at[slot], vout.at[g, h], out_sem.at[1, slot]))

    @pl.when(last)
    def _():
        for i in range(ahead):
            for copy in loads(i):
                copy.start()

        pos_copy = pltpu.make_async_copy(pos_hbm, pos, pos_sem)
        pos_copy.start()
        pos_copy.wait()

        def clear(i, carry):
            flags[i] = 0
            todo[i + 1] = 0
            return carry
        lax.fori_loop(0, n_slab, clear, 0)
        for g in range(n_groups):
            def mark(b, carry):
                flags[g * seq + pos[g, b]] = 1
                return carry
            lax.fori_loop(0, n_batch, mark, 0)

        def pick(i, count):
            hit = flags[i]

            @pl.when(hit == 1)
            def _():
                todo[count + 1] = i
            return count + hit
        todo[0] = lax.fori_loop(0, n_slab, pick, jnp.int32(0))
        todo_copy = pltpu.make_async_copy(todo, todo_hbm, todo_sem)
        todo_copy.start()

        def body(i, carry):
            for copy in loads(i):
                copy.wait()
            for copy in stores(i):
                copy.start()

            @pl.when(i + ahead < n_items)
            def _():
                @pl.when(i >= ahead)
                def _():
                    for copy in stores(i - ahead):
                        copy.wait()
                for copy in loads(i + ahead):
                    copy.start()
            return carry
        lax.fori_loop(0, n_items, body, 0)
        for i in range(n_items - 2 * ahead, n_items):
            for copy in stores(i):
                copy.wait()
        todo_copy.wait()


def keep_old(dims, positions, key_t, value_t):
    n_groups, n_batch, _, heads, seq, hd, _, _, _ = dims
    hbm = pl.BlockSpec(memory_space=pltpu.HBM)
    dma = pltpu.SemaphoreType.DMA
    return pl.pallas_call(
        functools.partial(keep_kernel, dims),
        out_shape=(jax.ShapeDtypeStruct(key_t.shape, BF16), jax.ShapeDtypeStruct(value_t.shape, BF16),
                   jax.ShapeDtypeStruct((n_groups * seq + 1,), jnp.int32)),
        in_specs=[hbm] * 3,
        out_specs=(hbm, hbm, hbm),
        scratch_shapes=[
            pltpu.VMEM((KEEP_SLOTS, seq, hd, n_batch), BF16),
            pltpu.VMEM((KEEP_SLOTS, seq, hd, n_batch), BF16),
            pltpu.SMEM((n_groups, n_batch), jnp.int32),
            pltpu.SMEM((n_groups * seq + 1,), jnp.int32),
            pltpu.SMEM((n_groups * seq,), jnp.int32),
            dma((2, KEEP_SLOTS)), dma((2, KEEP_SLOTS)), dma, dma,
        ],
        compiler_params=pltpu.CompilerParams(vmem_limit_bytes=67043328),
        name="cache_keep",
    )(positions, key_t, value_t)


def write_kernel(dims, todo_hbm, pos_hbm, knew_hbm, vnew_hbm, kc, vc, kold, vold, kout, vout,
                 todo, pos_ref, knew, vnew, kb, vb, in_sem, out_sem, small_sem):
    n_groups, _, _, _, seq, _, _, n_pp, _ = dims
    ahead = WRITE_SLOTS // 2
    last = lax.axis_index("pp") == n_pp - 1
    small = [pltpu.make_async_copy(src, dst, small_sem.at[i]) for i, (src, dst) in enumerate(
        ((todo_hbm, todo), (pos_hbm, pos_ref), (knew_hbm, knew), (vnew_hbm, vnew)))]
    for copy in small:
        copy.start()
    small[0].wait()
    count = jnp.where(last, todo[0], n_groups * seq)

    def place(i):
        entry = jnp.where(last, todo[i + 1], i)
        return entry // seq, lax.rem(entry, seq), lax.rem(i, WRITE_SLOTS)

    def loads(i):
        g, s, slot = place(i)
        return (pltpu.make_async_copy(kc.at[g, :, s], kb.at[slot], in_sem.at[0, slot]),
                pltpu.make_async_copy(vc.at[g, :, s], vb.at[slot], in_sem.at[1, slot]))

    def stores(i):
        g, s, slot = place(i)
        return (pltpu.make_async_copy(kb.at[slot], kout.at[g, :, s], out_sem.at[0, slot]),
                pltpu.make_async_copy(vb.at[slot], vout.at[g, :, s], out_sem.at[1, slot]))

    for i in range(ahead):
        @pl.when(i < count)
        def _():
            for copy in loads(i):
                copy.start()

    for copy in small[1:]:
        copy.wait()

    def body(i, carry):
        g, s, slot = place(i)
        for copy in loads(i):
            copy.wait()
        hit = (pos_ref[g] == s)[None]
        for new, buf in ((knew, kb), (vnew, vb)):
            buf[slot] = jnp.where(hit, new[g].astype(F32), buf[slot].astype(F32)).astype(BF16)
        for copy in stores(i):
            copy.start()

        @pl.when(i + ahead < count)
        def _():
            @pl.when(i >= ahead)
            def _():
                for copy in stores(i - ahead):
                    copy.wait()
            for copy in loads(i + ahead):
                copy.start()
        return carry
    lax.fori_loop(0, count, body, 0)

    def drain(i, carry):
        for copy in stores(i):
            copy.wait()
        return carry
    lax.fori_loop(jnp.maximum(count - 2 * ahead, 0), count, drain, 0)


def write_new(dims, todo, pos, key_new, value_new, key_t, value_t, key_old, value_old):
    n_groups, n_batch, _, heads, seq, hd, _, _, _ = dims
    hbm = pl.BlockSpec(memory_space=pltpu.HBM)
    dma = pltpu.SemaphoreType.DMA
    return pl.pallas_call(
        functools.partial(write_kernel, dims),
        out_shape=(jax.ShapeDtypeStruct(key_t.shape, BF16), jax.ShapeDtypeStruct(value_t.shape, BF16)),
        in_specs=[hbm] * 8,
        out_specs=(hbm, hbm),
        scratch_shapes=[
            pltpu.SMEM((n_groups * seq + 1,), jnp.int32),
            pltpu.VMEM((n_groups, 1, n_batch), jnp.int32),
            pltpu.VMEM((n_groups, heads, hd, n_batch), BF16),
            pltpu.VMEM((n_groups, heads, hd, n_batch), BF16),
            pltpu.VMEM((WRITE_SLOTS, heads, hd, n_batch), BF16),
            pltpu.VMEM((WRITE_SLOTS, heads, hd, n_batch), BF16),
            dma((2, WRITE_SLOTS)), dma((2, WRITE_SLOTS)), dma((4,)),
        ],
        input_output_aliases={6: 0, 7: 1},
        compiler_params=pltpu.CompilerParams(vmem_limit_bytes=67043328),
        cost_estimate=pl.CostEstimate(flops=n_groups * n_batch * heads * seq * hd * 40, bytes_accessed=8 * key_t.size, transcendentals=0),
        name="cache_write",
    )(todo, pos, key_new, value_new, key_t, value_t, key_old, value_old)


def solution(mesh):
    n_pp = mesh.shape["pp"]
    n_tp = mesh.shape["tp"]
    cache_spec = P("pp", "dp", None, "tp", None, None)
    col_spec = P("pp", None, "tp")
    row_spec = P("pp", "tp", None)
    gain_spec = P("pp", None)
    in_specs = (P("dp", None, None), P("dp", None), cache_spec, cache_spec, gain_spec, col_spec, col_spec, col_spec, row_spec, gain_spec, col_spec, col_spec, row_spec)
    out_specs = (P("dp", None, None), cache_spec, cache_spec)

    def per_device(hidden, positions, key_cache, value_cache, attn_norm, w_query, w_key, w_value, w_out, mlp_norm, w_gate, w_up, w_down):
        _, n_groups, n_batch, heads, seq, hd = key_cache.shape
        d_model = hidden.shape[-1]
        ff = w_gate.shape[-1]
        dims = (n_groups, n_batch, d_model, heads, seq, hd, ff, n_pp, n_tp)
        key_t = jnp.transpose(key_cache[0], (0, 2, 3, 4, 1))
        value_t = jnp.transpose(value_cache[0], (0, 2, 3, 4, 1))
        pos = positions[:, None, :]
        key_old, value_old, todo = keep_old(dims, positions, key_t, value_t)
        state, key_new, value_new = run_layer(
            dims, todo, pos, attn_norm, mlp_norm, hidden, key_t, value_t,
            w_query[0], w_key[0], w_value[0], w_out[0], w_gate[0], w_up[0], w_down[0])

        stage = lax.axis_index("pp")
        key_t, value_t = write_new(dims, todo, pos, key_new, value_new, key_t, value_t, key_old, value_old)
        from_last = [lax.ppermute(state, "pp", [(n_pp - 1, 1)])]
        from_last[0], state, key_t = lax.optimization_barrier((from_last[0], state, key_t))
        from_last.append(lax.ppermute(from_last[0], "pp", [(1, 0)]))
        from_last.extend(lax.ppermute(state, "pp", [(n_pp - 1, dst)]) for dst in range(2, n_pp - 1))
        final = jnp.where(stage == n_pp - 1, state, sum(from_last[1:], from_last[0]))
        return final, jnp.transpose(key_t, (0, 4, 1, 2, 3))[None], jnp.transpose(value_t, (0, 4, 1, 2, 3))[None]

    return jax.shard_map(per_device, mesh=mesh, in_specs=in_specs, out_specs=out_specs, check_vma=False)
```

```python
import functools
import math
import jax
import jax.numpy as jnp
import numpy as np
from jax import lax
from jax.experimental import pallas as pl
from jax.experimental.pallas import tpu as pltpu
from jax.sharding import PartitionSpec as P

ROPE_THETA = 500000.0
SCALE_FACTOR = 8.0
LOW_FACTOR = 1.0
HIGH_FACTOR = 4.0
ORIG_CONTEXT = 8192.0
NORM_EPS = 1e-5
MESH = pl.DeviceIdType.MESH
F32 = jnp.float32
BF16 = jnp.bfloat16

COLS = 512
SLOTS = 8
NORM_ROWS = 64
KEEP_SLOTS = 16
WRITE_SLOTS = 48


def rope_freqs(head_dim):
    freq_index = np.arange(head_dim // 2, dtype=np.float64)
    base_freq = ROPE_THETA ** (-2.0 * freq_index / head_dim)
    wave_len = 2.0 * math.pi / base_freq
    smooth_t = (ORIG_CONTEXT / wave_len - LOW_FACTOR) / (HIGH_FACTOR - LOW_FACTOR)
    mixed_freq = (1.0 - smooth_t) * base_freq / SCALE_FACTOR + smooth_t * base_freq
    long_freq = np.where(wave_len > ORIG_CONTEXT / LOW_FACTOR, base_freq / SCALE_FACTOR, mixed_freq)
    return np.where(wave_len < ORIG_CONTEXT / HIGH_FACTOR, base_freq, long_freq).astype(np.float32)


def layer_kernel(dims, after, pos_ref, ga_ref, gm_ref, hid, kc, vc, wq, wk, wv, wo, wg, wu, wd,
                 hout, knew, vnew,
                 wmix, wg_v, wu_v, ring, hbuf, recvp, recvd, nbuf, qt, ubuf, sc, cos_ref, sin_ref,
                 hid_sem, wqkv_sem, wo_sem, wd_sem, gu_sem, ring_sem,
                 p_send, p_recv, d_send, d_recv, h_send, h_recv):
    n_groups, n_batch, d_model, heads, seq, hd, ff, n_pp, n_tp = dims
    hw = heads * hd
    n_chunk = d_model // COLS
    n_gu = ff // COLS
    n_half = d_model // hw
    n_deep = ff // d_model
    pp = lax.axis_index("pp")
    tp = lax.axis_index("tp")
    peer = {"tp": lax.rem(tp + 1, n_tp)}
    nxt = {"pp": lax.rem(pp + 1, n_pp)}
    prv = {"pp": lax.rem(pp + n_pp - 1, n_pp)}

    n_kv = n_groups * heads

    def kv_copies(item, slot):
        g = item // heads
        h = lax.rem(item, heads)
        return (pltpu.make_async_copy(kc.at[g, h], ring.at[slot, pl.ds(0, seq)], ring_sem.at[slot, 0]),
                pltpu.make_async_copy(vc.at[g, h], ring.at[slot, pl.ds(seq, seq)], ring_sem.at[slot, 1]))

    def wd_copy(i):
        return pltpu.make_async_copy(wd.at[pl.ds(i % n_deep * d_model, d_model), pl.ds(i // n_deep * hw, hw)], wmix.at[i], wd_sem.at[i])

    def gu_copies(j):
        cols = pl.ds(pl.multiple_of(j * COLS, COLS), COLS)
        return (pltpu.make_async_copy(wg.at[:, cols], wg_v.at[j], gu_sem.at[0, j]),
                pltpu.make_async_copy(wu.at[:, cols], wu_v.at[j], gu_sem.at[1, j]))

    def qkv_copies():
        return [pltpu.make_async_copy(src, wmix.at[i], wqkv_sem.at[i]) for i, src in enumerate((wq, wk, wv))]

    def wo_copies():
        return [pltpu.make_async_copy(wo.at[:, pl.ds(i * hw, hw)], wmix.at[3, pl.ds(i * hw, hw)], wo_sem.at[i]) for i in range(n_half)]

    def hid_copy(g):
        return pltpu.make_async_copy(hid.at[g], hbuf.at[g], hid_sem.at[g])

    def piece(ref, g, c):
        return ref.at[g, :, pl.ds(pl.multiple_of(c * COLS, COLS), COLS)]

    def p_copy(g, c):
        return pltpu.make_async_remote_copy(piece(hout, g, c), piece(recvp, g, c), p_send.at[g, c], p_recv.at[g, c], device_id=peer, device_id_type=MESH)

    def d_copy(g, c):
        return pltpu.make_async_remote_copy(piece(recvp, g, c), piece(recvd, g, c), d_send.at[g, c], d_recv.at[g, c], device_id=peer, device_id_type=MESH)

    def h_copy(g, c):
        return pltpu.make_async_remote_copy(piece(hout, g, c), piece(hbuf, g, c), h_send.at[g, c], h_recv.at[g, c], device_id=nxt, device_id_type=MESH)

    first = pp == 0
    last = pp == n_pp - 1

    @pl.when(first)
    def _():
        for g in range(n_groups):
            hid_copy(g).start()
    for copy in qkv_copies():
        copy.start()

    def start_kv_wo():
        for slot in range(SLOTS):
            for copy in kv_copies(slot, slot):
                copy.start()
        for copy in wo_copies():
            copy.start()

    @pl.when(pp > 0)
    def _():
        start_kv_wo()
        for j in range(n_gu):
            for copy in gu_copies(j):
                copy.start()

    freq_id = lax.broadcasted_iota(jnp.int32, (hd // 2, n_batch), 0)
    freqs = jnp.zeros((hd // 2, n_batch), F32)
    for i, freq in enumerate(rope_freqs(hd)):
        freqs = jnp.where(freq_id == i, float(freq), freqs)
    for g in range(n_groups):
        angles = pos_ref[g].astype(F32) * freqs
        cos_ref[g] = jnp.cos(angles)
        sin_ref[g] = jnp.sin(angles)

    barrier = pltpu.get_barrier_semaphore()
    pl.semaphore_signal(barrier, inc=1, device_id=peer, device_id_type=MESH)

    @pl.when(jnp.logical_not(last))
    def _():
        pl.semaphore_signal(barrier, inc=1, device_id=nxt, device_id_type=MESH)

    @pl.when(pp > 0)
    def _():
        pl.semaphore_signal(barrier, inc=1, device_id=prv, device_id_type=MESH)
    ends = jnp.logical_or(first, last)

    @pl.when(ends)
    def _():
        pl.semaphore_wait(barrier, 2)

    @pl.when(jnp.logical_not(ends))
    def _():
        pl.semaphore_wait(barrier, 3)

    def norm_rows(g, gain_ref, with_partial):
        def body(r, carry):
            rows = pl.ds(pl.multiple_of(r * NORM_ROWS, NORM_ROWS), NORM_ROWS)
            x = hbuf[g, rows, :].astype(F32)
            if with_partial:
                part = (hout[g, rows, :].astype(F32) + recvp[g, rows, :].astype(F32)).astype(BF16)
                x = (x + part.astype(F32)).astype(BF16)
                hbuf[g, rows, :] = x
                x = x.astype(F32)
            inv = lax.rsqrt(jnp.mean(x * x, axis=-1, keepdims=True) + NORM_EPS)
            nbuf[rows, :] = (x * inv * gain_ref[...].astype(F32)).astype(BF16)
            return carry
        lax.fori_loop(0, n_batch // NORM_ROWS, body, 0)

    def attention_phase(g, carry):
        @pl.when(first)
        def _():
            hid_copy(g).wait()

        @pl.when(pp > 0)
        def _():
            for c in range(n_chunk):
                h_copy(g, c).wait_recv()

        norm_rows(g, ga_ref, False)
        cosine = cos_ref[g]
        sine = sin_ref[g]
        half = hd // 2

        @pl.when(g == 0)
        def _():
            for i, copy in enumerate(qkv_copies()):
                copy.wait()
                if i == 0:
                    pl.when(first)(start_kv_wo)

        for which in range(3):
            for c in range(hw // COLS):
                cols = slice(c * COLS, (c + 1) * COLS)
                prod_t = jnp.dot(nbuf[...], wmix[which, :, cols], preferred_element_type=F32).T
                for i in range(COLS // hd):
                    head = c * (COLS // hd) + i
                    a = prod_t[i * hd:i * hd + half]
                    b = prod_t[i * hd + half:(i + 1) * hd]
                    if which < 2:
                        a, b = a * cosine - b * sine, b * cosine + a * sine
                    both = jnp.concatenate([a, b], axis=0).astype(BF16)
                    if which == 0:
                        qt[head * hd:(head + 1) * hd, :] = both
                    else:
                        dst = knew if which == 1 else vnew
                        dst[g, head] = both

        pos = pos_ref[g]
        row_id = lax.broadcasted_iota(jnp.int32, (seq, n_batch), 0)
        hit = row_id == pos
        seen = row_id <= pos

        def head_body(h, inner):
            item = g * heads + h
            slot = lax.rem(item, SLOTS)
            for copy in kv_copies(item, slot):
                copy.wait()
            rows = pl.ds(pl.multiple_of(h * hd, hd), hd)
            q = qt[rows, :].astype(F32)
            fresh = jnp.sum(q * knew[g, h].astype(F32), axis=0, keepdims=True)
            for s in range(seq):
                total = None
                for d in range(4):
                    piece_d = ring[slot, s, d * 16:(d + 1) * 16].astype(F32) * q[d * 16:(d + 1) * 16]
                    total = piece_d if total is None else total + piece_d
                sc[s:s + 1, :] = jnp.sum(total, axis=0, keepdims=True)
            scores = jnp.where(hit, fresh, sc[...]) * hd ** -0.5
            scores = jnp.where(seen, scores, -jnp.inf)
            top = jnp.max(scores, axis=0, keepdims=True)
            expd = jnp.exp(scores - top)
            probs = (expd / jnp.sum(expd, axis=0, keepdims=True)).astype(BF16).astype(F32)
            sc[...] = jnp.where(hit, 0.0, probs)
            acc = jnp.sum(jnp.where(hit, probs, 0.0), axis=0, keepdims=True) * vnew[g, h].astype(F32)
            quarter = hd // 4
            for d in range(4):
                some = acc[d * quarter:(d + 1) * quarter]
                for s in range(seq):
                    some = some + sc[s:s + 1, :] * ring[slot, seq + s, d * quarter:(d + 1) * quarter].astype(F32)
                qt[pl.ds(pl.multiple_of(h * hd + d * quarter, quarter), quarter), :] = some.astype(BF16)

            @pl.when(item + SLOTS < n_kv)
            def _():
                for copy in kv_copies(item + SLOTS, slot):
                    copy.start()

            @pl.when(jnp.logical_and(jnp.logical_and(first, item + SLOTS < n_kv), lax.rem(item, SLOTS) == SLOTS // 2))
            def _():
                for copy in gu_copies(item // SLOTS):
                    copy.start()

            @pl.when(item + SLOTS == n_kv)
            def _():
                @pl.when(first)
                def _():
                    for j in range((n_kv - SLOTS) // SLOTS, n_gu):
                        for copy in gu_copies(j):
                            copy.start()
                for i in range(3):
                    wd_copy(i).start()
            return inner
        lax.fori_loop(0, heads, head_body, 0)

        @pl.when(g == 0)
        def _():
            for copy in wo_copies():
                copy.wait()
        for c in range(hw // COLS):
            cols = slice(c * COLS, (c + 1) * COLS)
            nbuf[:, cols] = qt[cols, :].astype(F32).T.astype(BF16)

        for c in range(n_chunk):
            at, col = divmod(c * COLS, hw)
            part = jnp.dot(nbuf[:, 0:hw], wmix[3, at * hw:(at + 1) * hw, col:col + COLS], preferred_element_type=F32)
            hout[g, :, c * COLS:(c + 1) * COLS] = part.astype(BF16)
        for c in range(n_chunk):
            p_copy(g, c).start()

        @pl.when(g == n_groups - 1)
        def _():
            wd_copy(3).start()
        return carry

    def mlp_phase(g, carry):
        for c in range(n_chunk):
            p_copy(g, c).wait()
        norm_rows(g, gm_ref, True)

        some = n_gu // 2

        def finish_some(part):
            @pl.when(g > 0)
            def _():
                for c in range(n_chunk // 2):
                    finish_piece(g - 1, part * (n_chunk // 2) + c)

        def gu_body(part, inner):
            tiles = [part * some + i for i in range(some)]

            @pl.when(g == 0)
            def _():
                for j in tiles:
                    for copy in gu_copies(j):
                        copy.wait()
            pl.when(part > 0)(lambda: finish_some(part - 1))
            for j in tiles:
                gate = jnp.dot(nbuf[...], wg_v[j], preferred_element_type=F32)
                up = jnp.dot(nbuf[...], wu_v[j], preferred_element_type=F32)
                ubuf[:, pl.ds(pl.multiple_of(j * COLS, COLS), COLS)] = (jax.nn.silu(gate) * up).astype(BF16)
            return inner
        lax.fori_loop(0, 2, gu_body, 0)
        finish_some(1)

        for c in range(n_chunk):
            at, col = divmod(c * COLS, hw)
            if col == 0:
                @pl.when(g == 0)
                def _():
                    for i in range(n_deep):
                        wd_copy(at * n_deep + i).wait()
            acc = None
            for i in range(n_deep):
                prod = jnp.dot(ubuf[:, i * d_model:(i + 1) * d_model], wmix[at * n_deep + i, :, col:col + COLS], preferred_element_type=F32)
                acc = prod if acc is None else acc + prod
            recvp[g, :, c * COLS:(c + 1) * COLS] = acc.astype(BF16)
            d_copy(g, c).start()
        return carry

    def finish_piece(g, c):
        d_copy(g, c).wait()
        cols = pl.ds(pl.multiple_of(c * COLS, COLS), COLS)
        part = (recvd[g, :, cols].astype(F32) + recvp[g, :, cols].astype(F32)).astype(BF16)
        hout[g, :, cols] = (hbuf[g, :, cols].astype(F32) + part.astype(F32)).astype(BF16)

        @pl.when(jnp.logical_not(last))
        def _():
            h_copy(g, c).start()

    lax.fori_loop(0, n_groups, attention_phase, 0)
    lax.fori_loop(0, n_groups, mlp_phase, 0)
    for c in range(n_chunk):
        finish_piece(n_groups - 1, c)

    @pl.when(jnp.logical_not(last))
    def _():
        for g in range(n_groups):
            for c in range(n_chunk):
                h_copy(g, c).wait_send()


def run_layer(dims, *args):
    n_groups, n_batch, d_model, heads, seq, hd, ff, n_pp, n_tp = dims
    hw = heads * hd
    n_chunk = d_model // COLS
    n_gu = ff // COLS
    assert ff * d_model == 4 * d_model * hw
    vmem = pl.BlockSpec(memory_space=pltpu.VMEM)
    hbm = pl.BlockSpec(memory_space=pltpu.HBM)
    dma = pltpu.SemaphoreType.DMA
    return pl.pallas_call(
        functools.partial(layer_kernel, dims),
        out_shape=(jax.ShapeDtypeStruct((n_groups, n_batch, d_model), BF16),
                   jax.ShapeDtypeStruct((n_groups, heads, hd, n_batch), BF16),
                   jax.ShapeDtypeStruct((n_groups, heads, hd, n_batch), BF16)),
        in_specs=[hbm] + [vmem] * 3 + [hbm] * 10,
        out_specs=(vmem, vmem, vmem),
        scratch_shapes=[
            pltpu.VMEM((4, d_model, hw), BF16),
            pltpu.VMEM((n_gu, d_model, COLS), BF16),
            pltpu.VMEM((n_gu, d_model, COLS), BF16),
            pltpu.VMEM((SLOTS, 2 * seq, hd, n_batch), BF16),
            pltpu.VMEM((n_groups, n_batch, d_model), BF16),
            pltpu.VMEM((n_groups, n_batch, d_model), BF16),
            pltpu.VMEM((n_groups, n_batch, d_model), BF16),
            pltpu.VMEM((n_batch, d_model), BF16),
            pltpu.VMEM((hw, n_batch), BF16),
            pltpu.VMEM((n_batch, ff), BF16),
            pltpu.VMEM((seq, n_batch), F32),
            pltpu.VMEM((n_groups, hd // 2, n_batch), F32),
            pltpu.VMEM((n_groups, hd // 2, n_batch), F32),
            dma((n_groups,)), dma((3,)), dma((d_model // hw,)), dma((4,)), dma((2, n_gu)), dma((SLOTS, 2)),
            dma((n_groups, n_chunk)), dma((n_groups, n_chunk)), dma((n_groups, n_chunk)),
            dma((n_groups, n_chunk)), dma((n_groups, n_chunk)), dma((n_groups, n_chunk)),
        ],
        compiler_params=pltpu.CompilerParams(collective_id=0, has_side_effects=True, vmem_limit_bytes=67043328),
        name="layer",
    )(*args)


def keep_kernel(dims, pos_hbm, kc, vc, kout, vout, todo_hbm, kb, vb, pos, todo, flags, in_sem, out_sem, pos_sem, todo_sem):
    n_groups, n_batch, _, heads, seq, _, _, n_pp, _ = dims
    n_slab = n_groups * seq
    n_items = n_groups * heads
    ahead = KEEP_SLOTS // 2
    last = lax.axis_index("pp") == n_pp - 1

    def loads(i):
        slot = lax.rem(i, KEEP_SLOTS)
        g, h = i // heads, lax.rem(i, heads)
        return (pltpu.make_async_copy(kc.at[g, h], kb.at[slot], in_sem.at[0, slot]),
                pltpu.make_async_copy(vc.at[g, h], vb.at[slot], in_sem.at[1, slot]))

    def stores(i):
        slot = lax.rem(i, KEEP_SLOTS)
        g, h = i // heads, lax.rem(i, heads)
        return (pltpu.make_async_copy(kb.at[slot], kout.at[g, h], out_sem.at[0, slot]),
                pltpu.make_async_copy(vb.at[slot], vout.at[g, h], out_sem.at[1, slot]))

    @pl.when(last)
    def _():
        for i in range(ahead):
            for copy in loads(i):
                copy.start()

        pos_copy = pltpu.make_async_copy(pos_hbm, pos, pos_sem)
        pos_copy.start()
        pos_copy.wait()

        def clear(i, carry):
            flags[i] = 0
            todo[i + 1] = 0
            return carry
        lax.fori_loop(0, n_slab, clear, 0)
        for g in range(n_groups):
            def mark(b, carry):
                flags[g * seq + pos[g, b]] = 1
                return carry
            lax.fori_loop(0, n_batch, mark, 0)

        def pick(i, count):
            hit = flags[i]

            @pl.when(hit == 1)
            def _():
                todo[count + 1] = i
            return count + hit
        todo[0] = lax.fori_loop(0, n_slab, pick, jnp.int32(0))
        todo_copy = pltpu.make_async_copy(todo, todo_hbm, todo_sem)
        todo_copy.start()

        def body(i, carry):
            for copy in loads(i):
                copy.wait()
            for copy in stores(i):
                copy.start()

            @pl.when(i + ahead < n_items)
            def _():
                @pl.when(i >= ahead)
                def _():
                    for copy in stores(i - ahead):
                        copy.wait()
                for copy in loads(i + ahead):
                    copy.start()
            return carry
        lax.fori_loop(0, n_items, body, 0)
        for i in range(n_items - 2 * ahead, n_items):
            for copy in stores(i):
                copy.wait()
        todo_copy.wait()


def keep_old(dims, positions, key_t, value_t):
    n_groups, n_batch, _, heads, seq, hd, _, _, _ = dims
    hbm = pl.BlockSpec(memory_space=pltpu.HBM)
    dma = pltpu.SemaphoreType.DMA
    return pl.pallas_call(
        functools.partial(keep_kernel, dims),
        out_shape=(jax.ShapeDtypeStruct(key_t.shape, BF16), jax.ShapeDtypeStruct(value_t.shape, BF16),
                   jax.ShapeDtypeStruct((n_groups * seq + 1,), jnp.int32)),
        in_specs=[hbm] * 3,
        out_specs=(hbm, hbm, hbm),
        scratch_shapes=[
            pltpu.VMEM((KEEP_SLOTS, seq, hd, n_batch), BF16),
            pltpu.VMEM((KEEP_SLOTS, seq, hd, n_batch), BF16),
            pltpu.SMEM((n_groups, n_batch), jnp.int32),
            pltpu.SMEM((n_groups * seq + 1,), jnp.int32),
            pltpu.SMEM((n_groups * seq,), jnp.int32),
            dma((2, KEEP_SLOTS)), dma((2, KEEP_SLOTS)), dma, dma,
        ],
        compiler_params=pltpu.CompilerParams(vmem_limit_bytes=67043328),
        name="cache_keep",
    )(positions, key_t, value_t)


def write_kernel(dims, todo_hbm, pos_hbm, knew_hbm, vnew_hbm, kc, vc, kold, vold, kout, vout,
                 todo, pos_ref, knew, vnew, kb, vb, in_sem, out_sem, small_sem):
    n_groups, _, _, _, seq, _, _, n_pp, _ = dims
    ahead = WRITE_SLOTS // 2
    last = lax.axis_index("pp") == n_pp - 1
    small = [pltpu.make_async_copy(src, dst, small_sem.at[i]) for i, (src, dst) in enumerate(
        ((todo_hbm, todo), (pos_hbm, pos_ref), (knew_hbm, knew), (vnew_hbm, vnew)))]
    for copy in small:
        copy.start()
    small[0].wait()
    count = jnp.where(last, todo[0], n_groups * seq)

    def place(i):
        entry = jnp.where(last, todo[i + 1], i)
        return entry // seq, lax.rem(entry, seq), lax.rem(i, WRITE_SLOTS)

    def loads(i):
        g, s, slot = place(i)
        return (pltpu.make_async_copy(kc.at[g, :, s], kb.at[slot], in_sem.at[0, slot]),
                pltpu.make_async_copy(vc.at[g, :, s], vb.at[slot], in_sem.at[1, slot]))

    def stores(i):
        g, s, slot = place(i)
        return (pltpu.make_async_copy(kb.at[slot], kout.at[g, :, s], out_sem.at[0, slot]),
                pltpu.make_async_copy(vb.at[slot], vout.at[g, :, s], out_sem.at[1, slot]))

    for i in range(ahead):
        @pl.when(i < count)
        def _():
            for copy in loads(i):
                copy.start()

    for copy in small[1:]:
        copy.wait()

    def body(i, carry):
        g, s, slot = place(i)
        for copy in loads(i):
            copy.wait()
        hit = (pos_ref[g] == s)[None]
        for new, buf in ((knew, kb), (vnew, vb)):
            buf[slot] = jnp.where(hit, new[g].astype(F32), buf[slot].astype(F32)).astype(BF16)
        for copy in stores(i):
            copy.start()

        @pl.when(i + ahead < count)
        def _():
            @pl.when(i >= ahead)
            def _():
                for copy in stores(i - ahead):
                    copy.wait()
            for copy in loads(i + ahead):
                copy.start()
        return carry
    lax.fori_loop(0, count, body, 0)

    def drain(i, carry):
        for copy in stores(i):
            copy.wait()
        return carry
    lax.fori_loop(jnp.maximum(count - 2 * ahead, 0), count, drain, 0)


def write_new(dims, todo, pos, key_new, value_new, key_t, value_t, key_old, value_old):
    n_groups, n_batch, _, heads, seq, hd, _, _, _ = dims
    hbm = pl.BlockSpec(memory_space=pltpu.HBM)
    dma = pltpu.SemaphoreType.DMA
    return pl.pallas_call(
        functools.partial(write_kernel, dims),
        out_shape=(jax.ShapeDtypeStruct(key_t.shape, BF16), jax.ShapeDtypeStruct(value_t.shape, BF16)),
        in_specs=[hbm] * 8,
        out_specs=(hbm, hbm),
        scratch_shapes=[
            pltpu.SMEM((n_groups * seq + 1,), jnp.int32),
            pltpu.VMEM((n_groups, 1, n_batch), jnp.int32),
            pltpu.VMEM((n_groups, heads, hd, n_batch), BF16),
            pltpu.VMEM((n_groups, heads, hd, n_batch), BF16),
            pltpu.VMEM((WRITE_SLOTS, heads, hd, n_batch), BF16),
            pltpu.VMEM((WRITE_SLOTS, heads, hd, n_batch), BF16),
            dma((2, WRITE_SLOTS)), dma((2, WRITE_SLOTS)), dma((4,)),
        ],
        input_output_aliases={6: 0, 7: 1},
        compiler_params=pltpu.CompilerParams(vmem_limit_bytes=67043328),
        cost_estimate=pl.CostEstimate(flops=n_groups * n_batch * heads * seq * hd * 40, bytes_accessed=8 * key_t.size, transcendentals=0),
        name="cache_write",
    )(todo, pos, key_new, value_new, key_t, value_t, key_old, value_old)


def solution(mesh):
    n_pp = mesh.shape["pp"]
    n_tp = mesh.shape["tp"]
    cache_spec = P("pp", "dp", None, "tp", None, None)
    col_spec = P("pp", None, "tp")
    row_spec = P("pp", "tp", None)
    gain_spec = P("pp", None)
    in_specs = (P("dp", None, None), P("dp", None), cache_spec, cache_spec, gain_spec, col_spec, col_spec, col_spec, row_spec, gain_spec, col_spec, col_spec, row_spec)
    out_specs = (P("dp", None, None), cache_spec, cache_spec)

    def per_device(hidden, positions, key_cache, value_cache, attn_norm, w_query, w_key, w_value, w_out, mlp_norm, w_gate, w_up, w_down):
        _, n_groups, n_batch, heads, seq, hd = key_cache.shape
        d_model = hidden.shape[-1]
        ff = w_gate.shape[-1]
        dims = (n_groups, n_batch, d_model, heads, seq, hd, ff, n_pp, n_tp)
        key_t = jnp.transpose(key_cache[0], (0, 2, 3, 4, 1))
        value_t = jnp.transpose(value_cache[0], (0, 2, 3, 4, 1))
        pos = positions[:, None, :]
        key_old, value_old, todo = keep_old(dims, positions, key_t, value_t)
        state, key_new, value_new = run_layer(
            dims, todo, pos, attn_norm, mlp_norm, hidden, key_t, value_t,
            w_query[0], w_key[0], w_value[0], w_out[0], w_gate[0], w_up[0], w_down[0])

        stage = lax.axis_index("pp")
        from_last = [lax.ppermute(state, "pp", [(n_pp - 1, dst)]) for dst in range(1, n_pp - 1)]
        key_t, value_t = write_new(dims, todo, pos, key_new, value_new, key_t, value_t, key_old, value_old)
        from_last[0], key_t = lax.optimization_barrier((from_last[0], key_t))
        from_last.append(lax.ppermute(from_last[0], "pp", [(1, 0)]))
        final = jnp.where(stage == n_pp - 1, state, sum(from_last[1:], from_last[0]))
        return final, jnp.transpose(key_t, (0, 4, 1, 2, 3))[None], jnp.transpose(value_t, (0, 4, 1, 2, 3))[None]

    return jax.shard_map(per_device, mesh=mesh, in_specs=in_specs, out_specs=out_specs, check_vma=False)
```

```python
import functools
import math
import jax
import jax.numpy as jnp
import numpy as np
from jax import lax
from jax.experimental import pallas as pl
from jax.experimental.pallas import tpu as pltpu
from jax.sharding import PartitionSpec as P

ROPE_THETA = 500000.0
SCALE_FACTOR = 8.0
LOW_FACTOR = 1.0
HIGH_FACTOR = 4.0
ORIG_CONTEXT = 8192.0
NORM_EPS = 1e-5
MESH = pl.DeviceIdType.MESH
F32 = jnp.float32
BF16 = jnp.bfloat16

COLS = 512
SLOTS = 8
NORM_ROWS = 64
KEEP_SLOTS = 16
WRITE_SLOTS = 24


def rope_freqs(head_dim):
    freq_index = np.arange(head_dim // 2, dtype=np.float64)
    base_freq = ROPE_THETA ** (-2.0 * freq_index / head_dim)
    wave_len = 2.0 * math.pi / base_freq
    smooth_t = (ORIG_CONTEXT / wave_len - LOW_FACTOR) / (HIGH_FACTOR - LOW_FACTOR)
    mixed_freq = (1.0 - smooth_t) * base_freq / SCALE_FACTOR + smooth_t * base_freq
    long_freq = np.where(wave_len > ORIG_CONTEXT / LOW_FACTOR, base_freq / SCALE_FACTOR, mixed_freq)
    return np.where(wave_len < ORIG_CONTEXT / HIGH_FACTOR, base_freq, long_freq).astype(np.float32)


def layer_kernel(dims, after, pos_ref, ga_ref, gm_ref, hid, kc, vc, wq, wk, wv, wo, wg, wu, wd,
                 hout, knew, vnew,
                 wmix, wg_v, wu_v, ring, hbuf, recvp, recvd, nbuf, qt, ubuf, sc, cos_ref, sin_ref,
                 hid_sem, wqkv_sem, wo_sem, wd_sem, gu_sem, ring_sem,
                 p_send, p_recv, d_send, d_recv, h_send, h_recv):
    n_groups, n_batch, d_model, heads, seq, hd, ff, n_pp, n_tp = dims
    hw = heads * hd
    n_chunk = d_model // COLS
    n_gu = ff // COLS
    n_half = d_model // hw
    n_deep = ff // d_model
    pp = lax.axis_index("pp")
    tp = lax.axis_index("tp")
    peer = {"tp": lax.rem(tp + 1, n_tp)}
    nxt = {"pp": lax.rem(pp + 1, n_pp)}
    prv = {"pp": lax.rem(pp + n_pp - 1, n_pp)}

    n_kv = n_groups * heads

    def kv_copies(item, slot):
        g = item // heads
        h = lax.rem(item, heads)
        return (pltpu.make_async_copy(kc.at[g, h], ring.at[slot, pl.ds(0, seq)], ring_sem.at[slot, 0]),
                pltpu.make_async_copy(vc.at[g, h], ring.at[slot, pl.ds(seq, seq)], ring_sem.at[slot, 1]))

    def wd_copy(i):
        return pltpu.make_async_copy(wd.at[pl.ds(i % n_deep * d_model, d_model), pl.ds(i // n_deep * hw, hw)], wmix.at[i], wd_sem.at[i])

    def gu_copies(j):
        cols = pl.ds(pl.multiple_of(j * COLS, COLS), COLS)
        return (pltpu.make_async_copy(wg.at[:, cols], wg_v.at[j], gu_sem.at[0, j]),
                pltpu.make_async_copy(wu.at[:, cols], wu_v.at[j], gu_sem.at[1, j]))

    def qkv_copies():
        return [pltpu.make_async_copy(src, wmix.at[i], wqkv_sem.at[i]) for i, src in enumerate((wq, wk, wv))]

    def wo_copies():
        return [pltpu.make_async_copy(wo.at[:, pl.ds(i * hw, hw)], wmix.at[3, pl.ds(i * hw, hw)], wo_sem.at[i]) for i in range(n_half)]

    def hid_copy(g):
        return pltpu.make_async_copy(hid.at[g], hbuf.at[g], hid_sem.at[g])

    def piece(ref, g, c):
        return ref.at[g, :, pl.ds(pl.multiple_of(c * COLS, COLS), COLS)]

    def p_copy(g, c):
        return pltpu.make_async_remote_copy(piece(hout, g, c), piece(recvp, g, c), p_send.at[g, c], p_recv.at[g, c], device_id=peer, device_id_type=MESH)

    def d_copy(g, c):
        return pltpu.make_async_remote_copy(piece(recvp, g, c), piece(recvd, g, c), d_send.at[g, c], d_recv.at[g, c], device_id=peer, device_id_type=MESH)

    def h_copy(g, c):
        return pltpu.make_async_remote_copy(piece(hout, g, c), piece(hbuf, g, c), h_send.at[g, c], h_recv.at[g, c], device_id=nxt, device_id_type=MESH)

    first = pp == 0
    last = pp == n_pp - 1

    @pl.when(first)
    def _():
        for g in range(n_groups):
            hid_copy(g).start()
    for copy in qkv_copies():
        copy.start()

    def start_kv_wo():
        for slot in range(SLOTS):
            for copy in kv_copies(slot, slot):
                copy.start()
        for copy in wo_copies():
            copy.start()

    @pl.when(pp > 0)
    def _():
        start_kv_wo()
        for j in range(n_gu):
            for copy in gu_copies(j):
                copy.start()

    freq_id = lax.broadcasted_iota(jnp.int32, (hd // 2, n_batch), 0)
    freqs = jnp.zeros((hd // 2, n_batch), F32)
    for i, freq in enumerate(rope_freqs(hd)):
        freqs = jnp.where(freq_id == i, float(freq), freqs)
    for g in range(n_groups):
        angles = pos_ref[g].astype(F32) * freqs
        cos_ref[g] = jnp.cos(angles)
        sin_ref[g] = jnp.sin(angles)

    barrier = pltpu.get_barrier_semaphore()
    pl.semaphore_signal(barrier, inc=1, device_id=peer, device_id_type=MESH)

    @pl.when(jnp.logical_not(last))
    def _():
        pl.semaphore_signal(barrier, inc=1, device_id=nxt, device_id_type=MESH)

    @pl.when(pp > 0)
    def _():
        pl.semaphore_signal(barrier, inc=1, device_id=prv, device_id_type=MESH)
    ends = jnp.logical_or(first, last)

    @pl.when(ends)
    def _():
        pl.semaphore_wait(barrier, 2)

    @pl.when(jnp.logical_not(ends))
    def _():
        pl.semaphore_wait(barrier, 3)

    def norm_rows(g, gain_ref, with_partial):
        def body(r, carry):
            rows = pl.ds(pl.multiple_of(r * NORM_ROWS, NORM_ROWS), NORM_ROWS)
            x = hbuf[g, rows, :].astype(F32)
            if with_partial:
                part = (hout[g, rows, :].astype(F32) + recvp[g, rows, :].astype(F32)).astype(BF16)
                x = (x + part.astype(F32)).astype(BF16)
                hbuf[g, rows, :] = x
                x = x.astype(F32)
            inv = lax.rsqrt(jnp.mean(x * x, axis=-1, keepdims=True) + NORM_EPS)
            nbuf[rows, :] = (x * inv * gain_ref[...].astype(F32)).astype(BF16)
            return carry
        lax.fori_loop(0, n_batch // NORM_ROWS, body, 0)

    def attention_phase(g, carry):
        @pl.when(first)
        def _():
            hid_copy(g).wait()

        @pl.when(pp > 0)
        def _():
            for c in range(n_chunk):
                h_copy(g, c).wait_recv()

        norm_rows(g, ga_ref, False)
        cosine = cos_ref[g]
        sine = sin_ref[g]
        half = hd // 2

        @pl.when(g == 0)
        def _():
            for i, copy in enumerate(qkv_copies()):
                copy.wait()
                if i == 0:
                    pl.when(first)(start_kv_wo)

        for which in range(3):
            for c in range(hw // COLS):
                cols = slice(c * COLS, (c + 1) * COLS)
                prod_t = jnp.dot(nbuf[...], wmix[which, :, cols], preferred_element_type=F32).T
                for i in range(COLS // hd):
                    head = c * (COLS // hd) + i
                    a = prod_t[i * hd:i * hd + half]
                    b = prod_t[i * hd + half:(i + 1) * hd]
                    if which < 2:
                        a, b = a * cosine - b * sine, b * cosine + a * sine
                    both = jnp.concatenate([a, b], axis=0).astype(BF16)
                    if which == 0:
                        qt[head * hd:(head + 1) * hd, :] = both
                    else:
                        dst = knew if which == 1 else vnew
                        dst[g, head] = both

        pos = pos_ref[g]
        row_id = lax.broadcasted_iota(jnp.int32, (seq, n_batch), 0)
        hit = row_id == pos
        seen = row_id <= pos

        def head_body(h, inner):
            item = g * heads + h
            slot = lax.rem(item, SLOTS)
            for copy in kv_copies(item, slot):
                copy.wait()
            rows = pl.ds(pl.multiple_of(h * hd, hd), hd)
            q = qt[rows, :].astype(F32)
            fresh = jnp.sum(q * knew[g, h].astype(F32), axis=0, keepdims=True)
            for s in range(seq):
                total = None
                for d in range(4):
                    piece_d = ring[slot, s, d * 16:(d + 1) * 16].astype(F32) * q[d * 16:(d + 1) * 16]
                    total = piece_d if total is None else total + piece_d
                sc[s:s + 1, :] = jnp.sum(total, axis=0, keepdims=True)
            scores = jnp.where(hit, fresh, sc[...]) * hd ** -0.5
            scores = jnp.where(seen, scores, -jnp.inf)
            top = jnp.max(scores, axis=0, keepdims=True)
            expd = jnp.exp(scores - top)
            probs = (expd / jnp.sum(expd, axis=0, keepdims=True)).astype(BF16).astype(F32)
            sc[...] = jnp.where(hit, 0.0, probs)
            acc = jnp.sum(jnp.where(hit, probs, 0.0), axis=0, keepdims=True) * vnew[g, h].astype(F32)
            for s in range(seq):
                acc = acc + sc[s:s + 1, :] * ring[slot, seq + s].astype(F32)
            qt[rows, :] = acc.astype(BF16)

            @pl.when(item + SLOTS < n_kv)
            def _():
                for copy in kv_copies(item + SLOTS, slot):
                    copy.start()

            @pl.when(jnp.logical_and(jnp.logical_and(first, item + SLOTS < n_kv), lax.rem(item, SLOTS) == SLOTS // 2))
            def _():
                for copy in gu_copies(item // SLOTS):
                    copy.start()

            @pl.when(item + SLOTS == n_kv)
            def _():
                @pl.when(first)
                def _():
                    for j in range((n_kv - SLOTS) // SLOTS, n_gu):
                        for copy in gu_copies(j):
                            copy.start()
                for i in range(3):
                    wd_copy(i).start()
            return inner
        lax.fori_loop(0, heads, head_body, 0)

        @pl.when(g == 0)
        def _():
            for copy in wo_copies():
                copy.wait()
        for c in range(hw // COLS):
            cols = slice(c * COLS, (c + 1) * COLS)
            nbuf[:, cols] = qt[cols, :].astype(F32).T.astype(BF16)

        for c in range(n_chunk):
            at, col = divmod(c * COLS, hw)
            part = jnp.dot(nbuf[:, 0:hw], wmix[3, at * hw:(at + 1) * hw, col:col + COLS], preferred_element_type=F32)
            hout[g, :, c * COLS:(c + 1) * COLS] = part.astype(BF16)
        for c in range(n_chunk):
            p_copy(g, c).start()

        @pl.when(g == n_groups - 1)
        def _():
            wd_copy(3).start()
        return carry

    def mlp_phase(g, carry):
        for c in range(n_chunk):
            p_copy(g, c).wait()
        norm_rows(g, gm_ref, True)

        some = n_gu // 2

        def finish_some(part):
            @pl.when(g > 0)
            def _():
                for c in range(n_chunk // 2):
                    finish_piece(g - 1, part * (n_chunk // 2) + c)

        def gu_body(part, inner):
            tiles = [part * some + i for i in range(some)]

            @pl.when(g == 0)
            def _():
                for j in tiles:
                    for copy in gu_copies(j):
                        copy.wait()
            pl.when(part > 0)(lambda: finish_some(part - 1))
            for j in tiles:
                gate = jnp.dot(nbuf[...], wg_v[j], preferred_element_type=F32)
                up = jnp.dot(nbuf[...], wu_v[j], preferred_element_type=F32)
                ubuf[:, pl.ds(pl.multiple_of(j * COLS, COLS), COLS)] = (jax.nn.silu(gate) * up).astype(BF16)
            return inner
        lax.fori_loop(0, 2, gu_body, 0)
        finish_some(1)

        for c in range(n_chunk):
            at, col = divmod(c * COLS, hw)
            if col == 0:
                @pl.when(g == 0)
                def _():
                    for i in range(n_deep):
                        wd_copy(at * n_deep + i).wait()
            acc = None
            for i in range(n_deep):
                prod = jnp.dot(ubuf[:, i * d_model:(i + 1) * d_model], wmix[at * n_deep + i, :, col:col + COLS], preferred_element_type=F32)
                acc = prod if acc is None else acc + prod
            recvp[g, :, c * COLS:(c + 1) * COLS] = acc.astype(BF16)
            d_copy(g, c).start()
        return carry

    def finish_piece(g, c):
        d_copy(g, c).wait()
        cols = pl.ds(pl.multiple_of(c * COLS, COLS), COLS)
        part = (recvd[g, :, cols].astype(F32) + recvp[g, :, cols].astype(F32)).astype(BF16)
        hout[g, :, cols] = (hbuf[g, :, cols].astype(F32) + part.astype(F32)).astype(BF16)

        @pl.when(jnp.logical_not(last))
        def _():
            h_copy(g, c).start()

    lax.fori_loop(0, n_groups, attention_phase, 0)
    lax.fori_loop(0, n_groups, mlp_phase, 0)
    for c in range(n_chunk):
        finish_piece(n_groups - 1, c)

    @pl.when(jnp.logical_not(last))
    def _():
        for g in range(n_groups):
            for c in range(n_chunk):
                h_copy(g, c).wait_send()


def run_layer(dims, *args):
    n_groups, n_batch, d_model, heads, seq, hd, ff, n_pp, n_tp = dims
    hw = heads * hd
    n_chunk = d_model // COLS
    n_gu = ff // COLS
    assert ff * d_model == 4 * d_model * hw
    vmem = pl.BlockSpec(memory_space=pltpu.VMEM)
    hbm = pl.BlockSpec(memory_space=pltpu.HBM)
    dma = pltpu.SemaphoreType.DMA
    return pl.pallas_call(
        functools.partial(layer_kernel, dims),
        out_shape=(jax.ShapeDtypeStruct((n_groups, n_batch, d_model), BF16),
                   jax.ShapeDtypeStruct((n_groups, heads, hd, n_batch), BF16),
                   jax.ShapeDtypeStruct((n_groups, heads, hd, n_batch), BF16)),
        in_specs=[hbm] + [vmem] * 3 + [hbm] * 10,
        out_specs=(vmem, vmem, vmem),
        scratch_shapes=[
            pltpu.VMEM((4, d_model, hw), BF16),
            pltpu.VMEM((n_gu, d_model, COLS), BF16),
            pltpu.VMEM((n_gu, d_model, COLS), BF16),
            pltpu.VMEM((SLOTS, 2 * seq, hd, n_batch), BF16),
            pltpu.VMEM((n_groups, n_batch, d_model), BF16),
            pltpu.VMEM((n_groups, n_batch, d_model), BF16),
            pltpu.VMEM((n_groups, n_batch, d_model), BF16),
            pltpu.VMEM((n_batch, d_model), BF16),
            pltpu.VMEM((hw, n_batch), BF16),
            pltpu.VMEM((n_batch, ff), BF16),
            pltpu.VMEM((seq, n_batch), F32),
            pltpu.VMEM((n_groups, hd // 2, n_batch), F32),
            pltpu.VMEM((n_groups, hd // 2, n_batch), F32),
            dma((n_groups,)), dma((3,)), dma((d_model // hw,)), dma((4,)), dma((2, n_gu)), dma((SLOTS, 2)),
            dma((n_groups, n_chunk)), dma((n_groups, n_chunk)), dma((n_groups, n_chunk)),
            dma((n_groups, n_chunk)), dma((n_groups, n_chunk)), dma((n_groups, n_chunk)),
        ],
        compiler_params=pltpu.CompilerParams(collective_id=0, has_side_effects=True, vmem_limit_bytes=67043328),
        name="layer",
    )(*args)


def keep_kernel(dims, pos_hbm, kc, vc, kout, vout, todo_hbm, kb, vb, pos, todo, flags, in_sem, out_sem, pos_sem, todo_sem):
    n_groups, n_batch, _, heads, seq, _, _, n_pp, _ = dims
    n_slab = n_groups * seq
    n_items = n_groups * heads
    ahead = KEEP_SLOTS // 2
    last = lax.axis_index("pp") == n_pp - 1

    def loads(i):
        slot = lax.rem(i, KEEP_SLOTS)
        g, h = i // heads, lax.rem(i, heads)
        return (pltpu.make_async_copy(kc.at[g, h], kb.at[slot], in_sem.at[0, slot]),
                pltpu.make_async_copy(vc.at[g, h], vb.at[slot], in_sem.at[1, slot]))

    def stores(i):
        slot = lax.rem(i, KEEP_SLOTS)
        g, h = i // heads, lax.rem(i, heads)
        return (pltpu.make_async_copy(kb.at[slot], kout.at[g, h], out_sem.at[0, slot]),
                pltpu.make_async_copy(vb.at[slot], vout.at[g, h], out_sem.at[1, slot]))

    @pl.when(last)
    def _():
        for i in range(ahead):
            for copy in loads(i):
                copy.start()

        pos_copy = pltpu.make_async_copy(pos_hbm, pos, pos_sem)
        pos_copy.start()
        pos_copy.wait()

        def clear(i, carry):
            flags[i] = 0
            todo[i + 1] = 0
            return carry
        lax.fori_loop(0, n_slab, clear, 0)
        for g in range(n_groups):
            def mark(b, carry):
                flags[g * seq + pos[g, b]] = 1
                return carry
            lax.fori_loop(0, n_batch, mark, 0)

        def pick(i, count):
            hit = flags[i]

            @pl.when(hit == 1)
            def _():
                todo[count + 1] = i
            return count + hit
        todo[0] = lax.fori_loop(0, n_slab, pick, jnp.int32(0))
        todo_copy = pltpu.make_async_copy(todo, todo_hbm, todo_sem)
        todo_copy.start()

        def body(i, carry):
            for copy in loads(i):
                copy.wait()
            for copy in stores(i):
                copy.start()

            @pl.when(i + ahead < n_items)
            def _():
                @pl.when(i >= ahead)
                def _():
                    for copy in stores(i - ahead):
                        copy.wait()
                for copy in loads(i + ahead):
                    copy.start()
            return carry
        lax.fori_loop(0, n_items, body, 0)
        for i in range(n_items - 2 * ahead, n_items):
            for copy in stores(i):
                copy.wait()
        todo_copy.wait()


def keep_old(dims, positions, key_t, value_t):
    n_groups, n_batch, _, heads, seq, hd, _, _, _ = dims
    hbm = pl.BlockSpec(memory_space=pltpu.HBM)
    dma = pltpu.SemaphoreType.DMA
    return pl.pallas_call(
        functools.partial(keep_kernel, dims),
        out_shape=(jax.ShapeDtypeStruct(key_t.shape, BF16), jax.ShapeDtypeStruct(value_t.shape, BF16),
                   jax.ShapeDtypeStruct((n_groups * seq + 1,), jnp.int32)),
        in_specs=[hbm] * 3,
        out_specs=(hbm, hbm, hbm),
        scratch_shapes=[
            pltpu.VMEM((KEEP_SLOTS, seq, hd, n_batch), BF16),
            pltpu.VMEM((KEEP_SLOTS, seq, hd, n_batch), BF16),
            pltpu.SMEM((n_groups, n_batch), jnp.int32),
            pltpu.SMEM((n_groups * seq + 1,), jnp.int32),
            pltpu.SMEM((n_groups * seq,), jnp.int32),
            dma((2, KEEP_SLOTS)), dma((2, KEEP_SLOTS)), dma, dma,
        ],
        compiler_params=pltpu.CompilerParams(vmem_limit_bytes=67043328),
        name="cache_keep",
    )(positions, key_t, value_t)


def write_kernel(dims, todo_hbm, pos_hbm, knew_hbm, vnew_hbm, kc, vc, kold, vold, kout, vout,
                 todo, pos_ref, knew, vnew, kb, vb, in_sem, out_sem, small_sem):
    n_groups, _, _, _, seq, _, _, n_pp, _ = dims
    ahead = WRITE_SLOTS // 2
    last = lax.axis_index("pp") == n_pp - 1
    small = [pltpu.make_async_copy(src, dst, small_sem.at[i]) for i, (src, dst) in enumerate(
        ((todo_hbm, todo), (pos_hbm, pos_ref), (knew_hbm, knew), (vnew_hbm, vnew)))]
    for copy in small:
        copy.start()
    small[0].wait()
    count = jnp.where(last, todo[0], n_groups * seq)

    def place(i):
        entry = jnp.where(last, todo[i + 1], i)
        return entry // seq, lax.rem(entry, seq), lax.rem(i, WRITE_SLOTS)

    def loads(i):
        g, s, slot = place(i)
        return (pltpu.make_async_copy(kc.at[g, :, s], kb.at[slot], in_sem.at[0, slot]),
                pltpu.make_async_copy(vc.at[g, :, s], vb.at[slot], in_sem.at[1, slot]))

    def stores(i):
        g, s, slot = place(i)
        return (pltpu.make_async_copy(kb.at[slot], kout.at[g, :, s], out_sem.at[0, slot]),
                pltpu.make_async_copy(vb.at[slot], vout.at[g, :, s], out_sem.at[1, slot]))

    for i in range(ahead):
        @pl.when(i < count)
        def _():
            for copy in loads(i):
                copy.start()

    for copy in small[1:]:
        copy.wait()

    def body(i, carry):
        g, s, slot = place(i)
        for copy in loads(i):
            copy.wait()
        hit = (pos_ref[g] == s)[None]
        for new, buf in ((knew, kb), (vnew, vb)):
            buf[slot] = jnp.where(hit, new[g].astype(F32), buf[slot].astype(F32)).astype(BF16)
        for copy in stores(i):
            copy.start()

        @pl.when(i + ahead < count)
        def _():
            @pl.when(i >= ahead)
            def _():
                for copy in stores(i - ahead):
                    copy.wait()
            for copy in loads(i + ahead):
                copy.start()
        return carry
    lax.fori_loop(0, count, body, 0)

    def drain(i, carry):
        for copy in stores(i):
            copy.wait()
        return carry
    lax.fori_loop(jnp.maximum(count - 2 * ahead, 0), count, drain, 0)


def write_new(dims, todo, pos, key_new, value_new, key_t, value_t, key_old, value_old):
    n_groups, n_batch, _, heads, seq, hd, _, _, _ = dims
    hbm = pl.BlockSpec(memory_space=pltpu.HBM)
    dma = pltpu.SemaphoreType.DMA
    return pl.pallas_call(
        functools.partial(write_kernel, dims),
        out_shape=(jax.ShapeDtypeStruct(key_t.shape, BF16), jax.ShapeDtypeStruct(value_t.shape, BF16)),
        in_specs=[hbm] * 8,
        out_specs=(hbm, hbm),
        scratch_shapes=[
            pltpu.SMEM((n_groups * seq + 1,), jnp.int32),
            pltpu.VMEM((n_groups, 1, n_batch), jnp.int32),
            pltpu.VMEM((n_groups, heads, hd, n_batch), BF16),
            pltpu.VMEM((n_groups, heads, hd, n_batch), BF16),
            pltpu.VMEM((WRITE_SLOTS, heads, hd, n_batch), BF16),
            pltpu.VMEM((WRITE_SLOTS, heads, hd, n_batch), BF16),
            dma((2, WRITE_SLOTS)), dma((2, WRITE_SLOTS)), dma((4,)),
        ],
        input_output_aliases={6: 0, 7: 1},
        compiler_params=pltpu.CompilerParams(vmem_limit_bytes=67043328),
        cost_estimate=pl.CostEstimate(flops=n_groups * n_batch * heads * seq * hd * 40, bytes_accessed=8 * key_t.size, transcendentals=0),
        name="cache_write",
    )(todo, pos, key_new, value_new, key_t, value_t, key_old, value_old)


def solution(mesh):
    n_pp = mesh.shape["pp"]
    n_tp = mesh.shape["tp"]
    cache_spec = P("pp", "dp", None, "tp", None, None)
    col_spec = P("pp", None, "tp")
    row_spec = P("pp", "tp", None)
    gain_spec = P("pp", None)
    in_specs = (P("dp", None, None), P("dp", None), cache_spec, cache_spec, gain_spec, col_spec, col_spec, col_spec, row_spec, gain_spec, col_spec, col_spec, row_spec)
    out_specs = (P("dp", None, None), cache_spec, cache_spec)

    def per_device(hidden, positions, key_cache, value_cache, attn_norm, w_query, w_key, w_value, w_out, mlp_norm, w_gate, w_up, w_down):
        _, n_groups, n_batch, heads, seq, hd = key_cache.shape
        d_model = hidden.shape[-1]
        ff = w_gate.shape[-1]
        dims = (n_groups, n_batch, d_model, heads, seq, hd, ff, n_pp, n_tp)
        key_t = jnp.transpose(key_cache[0], (0, 2, 3, 4, 1))
        value_t = jnp.transpose(value_cache[0], (0, 2, 3, 4, 1))
        pos = positions[:, None, :]
        key_old, value_old, todo = keep_old(dims, positions, key_t, value_t)
        state, key_new, value_new = run_layer(
            dims, todo, pos, attn_norm, mlp_norm, hidden, key_t, value_t,
            w_query[0], w_key[0], w_value[0], w_out[0], w_gate[0], w_up[0], w_down[0])

        stage = lax.axis_index("pp")
        from_last = [lax.ppermute(state, "pp", [(n_pp - 1, dst)]) for dst in range(1, n_pp - 1)]
        key_t, value_t = write_new(dims, todo, pos, key_new, value_new, key_t, value_t, key_old, value_old)
        from_last[0], key_t = lax.optimization_barrier((from_last[0], key_t))
        from_last.append(lax.ppermute(from_last[0], "pp", [(1, 0)]))
        final = jnp.where(stage == n_pp - 1, state, sum(from_last[1:], from_last[0]))
        return final, jnp.transpose(key_t, (0, 4, 1, 2, 3))[None], jnp.transpose(value_t, (0, 4, 1, 2, 3))[None]

    return jax.shard_map(per_device, mesh=mesh, in_specs=in_specs, out_specs=out_specs, check_vma=False)
```

```python
import functools
import math
import jax
import jax.numpy as jnp
import numpy as np
from jax import lax
from jax.experimental import pallas as pl
from jax.experimental.pallas import tpu as pltpu
from jax.sharding import PartitionSpec as P

ROPE_THETA = 500000.0
SCALE_FACTOR = 8.0
LOW_FACTOR = 1.0
HIGH_FACTOR = 4.0
ORIG_CONTEXT = 8192.0
NORM_EPS = 1e-5
MESH = pl.DeviceIdType.MESH
F32 = jnp.float32
BF16 = jnp.bfloat16

COLS = 512
SLOTS = 8
NORM_ROWS = 64
KEEP_SLOTS = 16
WRITE_SLOTS = 24


def rope_freqs(head_dim):
    freq_index = np.arange(head_dim // 2, dtype=np.float64)
    base_freq = ROPE_THETA ** (-2.0 * freq_index / head_dim)
    wave_len = 2.0 * math.pi / base_freq
    smooth_t = (ORIG_CONTEXT / wave_len - LOW_FACTOR) / (HIGH_FACTOR - LOW_FACTOR)
    mixed_freq = (1.0 - smooth_t) * base_freq / SCALE_FACTOR + smooth_t * base_freq
    long_freq = np.where(wave_len > ORIG_CONTEXT / LOW_FACTOR, base_freq / SCALE_FACTOR, mixed_freq)
    return np.where(wave_len < ORIG_CONTEXT / HIGH_FACTOR, base_freq, long_freq).astype(np.float32)


def layer_kernel(dims, after, pos_ref, ga_ref, gm_ref, hid, kc, vc, wq, wk, wv, wo, wg, wu, wd,
                 hout, knew, vnew,
                 wmix, wg_v, wu_v, ring, hbuf, recvp, recvd, nbuf, qt, ubuf, sc, cos_ref, sin_ref,
                 hid_sem, wqkv_sem, wo_sem, wd_sem, gu_sem, ring_sem,
                 p_send, p_recv, d_send, d_recv, h_send, h_recv):
    n_groups, n_batch, d_model, heads, seq, hd, ff, n_pp, n_tp = dims
    hw = heads * hd
    n_chunk = d_model // COLS
    n_gu = ff // COLS
    n_half = d_model // hw
    n_deep = ff // d_model
    pp = lax.axis_index("pp")
    tp = lax.axis_index("tp")
    peer = {"tp": lax.rem(tp + 1, n_tp)}
    nxt = {"pp": lax.rem(pp + 1, n_pp)}
    prv = {"pp": lax.rem(pp + n_pp - 1, n_pp)}

    n_kv = n_groups * heads

    def kv_copies(item, slot):
        g = item // heads
        h = lax.rem(item, heads)
        return (pltpu.make_async_copy(kc.at[g, h], ring.at[slot, pl.ds(0, seq)], ring_sem.at[slot, 0]),
                pltpu.make_async_copy(vc.at[g, h], ring.at[slot, pl.ds(seq, seq)], ring_sem.at[slot, 1]))

    def wd_copy(i):
        return pltpu.make_async_copy(wd.at[pl.ds(i % n_deep * d_model, d_model), pl.ds(i // n_deep * hw, hw)], wmix.at[i], wd_sem.at[i])

    def gu_copies(j):
        cols = pl.ds(pl.multiple_of(j * COLS, COLS), COLS)
        return (pltpu.make_async_copy(wg.at[:, cols], wg_v.at[j], gu_sem.at[0, j]),
                pltpu.make_async_copy(wu.at[:, cols], wu_v.at[j], gu_sem.at[1, j]))

    def qkv_copies():
        return [pltpu.make_async_copy(src, wmix.at[i], wqkv_sem.at[i]) for i, src in enumerate((wq, wk, wv))]

    def wo_copies():
        return [pltpu.make_async_copy(wo.at[:, pl.ds(i * hw, hw)], wmix.at[3, pl.ds(i * hw, hw)], wo_sem.at[i]) for i in range(n_half)]

    def hid_copy(g):
        return pltpu.make_async_copy(hid.at[g], hbuf.at[g], hid_sem.at[g])

    def piece(ref, g, c):
        return ref.at[g, :, pl.ds(pl.multiple_of(c * COLS, COLS), COLS)]

    def p_copy(g, c):
        return pltpu.make_async_remote_copy(piece(hout, g, c), piece(recvp, g, c), p_send.at[g, c], p_recv.at[g, c], device_id=peer, device_id_type=MESH)

    def d_copy(g, c):
        return pltpu.make_async_remote_copy(piece(recvp, g, c), piece(recvd, g, c), d_send.at[g, c], d_recv.at[g, c], device_id=peer, device_id_type=MESH)

    def h_copy(g, c):
        return pltpu.make_async_remote_copy(piece(hout, g, c), piece(hbuf, g, c), h_send.at[g, c], h_recv.at[g, c], device_id=nxt, device_id_type=MESH)

    first = pp == 0
    last = pp == n_pp - 1

    @pl.when(first)
    def _():
        for g in range(n_groups):
            hid_copy(g).start()
    for copy in qkv_copies():
        copy.start()

    def start_kv_wo():
        for slot in range(SLOTS):
            for copy in kv_copies(slot, slot):
                copy.start()
        for copy in wo_copies():
            copy.start()

    @pl.when(pp > 0)
    def _():
        start_kv_wo()
        for j in range(n_gu):
            for copy in gu_copies(j):
                copy.start()

    freq_id = lax.broadcasted_iota(jnp.int32, (hd // 2, n_batch), 0)
    freqs = jnp.zeros((hd // 2, n_batch), F32)
    for i, freq in enumerate(rope_freqs(hd)):
        freqs = jnp.where(freq_id == i, float(freq), freqs)
    for g in range(n_groups):
        angles = pos_ref[g].astype(F32) * freqs
        cos_ref[g] = jnp.cos(angles)
        sin_ref[g] = jnp.sin(angles)

    barrier = pltpu.get_barrier_semaphore()
    pl.semaphore_signal(barrier, inc=1, device_id=peer, device_id_type=MESH)

    @pl.when(jnp.logical_not(last))
    def _():
        pl.semaphore_signal(barrier, inc=1, device_id=nxt, device_id_type=MESH)

    @pl.when(pp > 0)
    def _():
        pl.semaphore_signal(barrier, inc=1, device_id=prv, device_id_type=MESH)
    ends = jnp.logical_or(first, last)

    @pl.when(ends)
    def _():
        pl.semaphore_wait(barrier, 2)

    @pl.when(jnp.logical_not(ends))
    def _():
        pl.semaphore_wait(barrier, 3)

    def norm_rows(g, gain_ref, with_partial):
        def body(r, carry):
            rows = pl.ds(pl.multiple_of(r * NORM_ROWS, NORM_ROWS), NORM_ROWS)
            x = hbuf[g, rows, :].astype(F32)
            if with_partial:
                part = (hout[g, rows, :].astype(F32) + recvp[g, rows, :].astype(F32)).astype(BF16)
                x = (x + part.astype(F32)).astype(BF16)
                hbuf[g, rows, :] = x
                x = x.astype(F32)
            inv = lax.rsqrt(jnp.mean(x * x, axis=-1, keepdims=True) + NORM_EPS)
            nbuf[rows, :] = (x * inv * gain_ref[...].astype(F32)).astype(BF16)
            return carry
        lax.fori_loop(0, n_batch // NORM_ROWS, body, 0)

    def attention_phase(g, carry):
        @pl.when(first)
        def _():
            hid_copy(g).wait()

        @pl.when(pp > 0)
        def _():
            for c in range(n_chunk):
                h_copy(g, c).wait_recv()

        norm_rows(g, ga_ref, False)
        cosine = cos_ref[g]
        sine = sin_ref[g]
        half = hd // 2

        @pl.when(g == 0)
        def _():
            for i, copy in enumerate(qkv_copies()):
                copy.wait()
                if i == 0:
                    pl.when(first)(start_kv_wo)

        for which in range(3):
            for c in range(hw // COLS):
                cols = slice(c * COLS, (c + 1) * COLS)
                prod_t = jnp.dot(nbuf[...], wmix[which, :, cols], preferred_element_type=F32).T
                for i in range(COLS // hd):
                    head = c * (COLS // hd) + i
                    a = prod_t[i * hd:i * hd + half]
                    b = prod_t[i * hd + half:(i + 1) * hd]
                    if which < 2:
                        a, b = a * cosine - b * sine, b * cosine + a * sine
                    both = jnp.concatenate([a, b], axis=0).astype(BF16)
                    if which == 0:
                        qt[head * hd:(head + 1) * hd, :] = both
                    else:
                        dst = knew if which == 1 else vnew
                        dst[g, head] = both

        pos = pos_ref[g]
        row_id = lax.broadcasted_iota(jnp.int32, (seq, n_batch), 0)
        hit = row_id == pos
        seen = row_id <= pos

        def head_body(h, inner):
            item = g * heads + h
            slot = lax.rem(item, SLOTS)
            for copy in kv_copies(item, slot):
                copy.wait()
            rows = pl.ds(pl.multiple_of(h * hd, hd), hd)
            q = qt[rows, :].astype(F32)
            fresh = jnp.sum(q * knew[g, h].astype(F32), axis=0, keepdims=True)
            for s in range(seq):
                total = None
                for d in range(4):
                    piece_d = ring[slot, s, d * 16:(d + 1) * 16].astype(F32) * q[d * 16:(d + 1) * 16]
                    total = piece_d if total is None else total + piece_d
                sc[s:s + 1, :] = jnp.sum(total, axis=0, keepdims=True)
            scores = jnp.where(hit, fresh, sc[...]) * hd ** -0.5
            scores = jnp.where(seen, scores, -jnp.inf)
            top = jnp.max(scores, axis=0, keepdims=True)
            expd = jnp.exp(scores - top)
            probs = (expd / jnp.sum(expd, axis=0, keepdims=True)).astype(BF16).astype(F32)
            sc[...] = jnp.where(hit, 0.0, probs)
            acc = jnp.sum(jnp.where(hit, probs, 0.0), axis=0, keepdims=True) * vnew[g, h].astype(F32)
            for s in range(seq):
                acc = acc + sc[s:s + 1, :] * ring[slot, seq + s].astype(F32)
            qt[rows, :] = acc.astype(BF16)

            @pl.when(item + SLOTS < n_kv)
            def _():
                for copy in kv_copies(item + SLOTS, slot):
                    copy.start()

            @pl.when(jnp.logical_and(jnp.logical_and(first, item + SLOTS < n_kv), lax.rem(item, SLOTS) == SLOTS // 2))
            def _():
                for copy in gu_copies(item // SLOTS):
                    copy.start()

            @pl.when(item + SLOTS == n_kv)
            def _():
                @pl.when(first)
                def _():
                    for j in range((n_kv - SLOTS) // SLOTS, n_gu):
                        for copy in gu_copies(j):
                            copy.start()
                for i in range(3):
                    wd_copy(i).start()
            return inner
        lax.fori_loop(0, heads, head_body, 0)

        @pl.when(g == 0)
        def _():
            for copy in wo_copies():
                copy.wait()
        for c in range(hw // COLS):
            cols = slice(c * COLS, (c + 1) * COLS)
            nbuf[:, cols] = qt[cols, :].astype(F32).T.astype(BF16)

        for c in range(n_chunk):
            at, col = divmod(c * COLS, hw)
            part = jnp.dot(nbuf[:, 0:hw], wmix[3, at * hw:(at + 1) * hw, col:col + COLS], preferred_element_type=F32)
            hout[g, :, c * COLS:(c + 1) * COLS] = part.astype(BF16)
            p_copy(g, c).start()

        @pl.when(g == n_groups - 1)
        def _():
            wd_copy(3).start()
        return carry

    def mlp_phase(g, carry):
        for c in range(n_chunk):
            p_copy(g, c).wait()
        norm_rows(g, gm_ref, True)

        some = n_gu // 2

        def finish_some(part):
            @pl.when(g > 0)
            def _():
                for c in range(n_chunk // 2):
                    finish_piece(g - 1, part * (n_chunk // 2) + c)

        def gu_body(part, inner):
            tiles = [part * some + i for i in range(some)]

            @pl.when(g == 0)
            def _():
                for j in tiles:
                    for copy in gu_copies(j):
                        copy.wait()
            pl.when(part > 0)(lambda: finish_some(part - 1))
            for j in tiles:
                gate = jnp.dot(nbuf[...], wg_v[j], preferred_element_type=F32)
                up = jnp.dot(nbuf[...], wu_v[j], preferred_element_type=F32)
                ubuf[:, pl.ds(pl.multiple_of(j * COLS, COLS), COLS)] = (jax.nn.silu(gate) * up).astype(BF16)
            return inner
        lax.fori_loop(0, 2, gu_body, 0)
        finish_some(1)

        for c in range(n_chunk):
            at, col = divmod(c * COLS, hw)
            if col == 0:
                @pl.when(g == 0)
                def _():
                    for i in range(n_deep):
                        wd_copy(at * n_deep + i).wait()
            acc = None
            for i in range(n_deep):
                prod = jnp.dot(ubuf[:, i * d_model:(i + 1) * d_model], wmix[at * n_deep + i, :, col:col + COLS], preferred_element_type=F32)
                acc = prod if acc is None else acc + prod
            recvp[g, :, c * COLS:(c + 1) * COLS] = acc.astype(BF16)
            d_copy(g, c).start()
        return carry

    def finish_piece(g, c):
        d_copy(g, c).wait()
        cols = pl.ds(pl.multiple_of(c * COLS, COLS), COLS)
        part = (recvd[g, :, cols].astype(F32) + recvp[g, :, cols].astype(F32)).astype(BF16)
        hout[g, :, cols] = (hbuf[g, :, cols].astype(F32) + part.astype(F32)).astype(BF16)

        @pl.when(jnp.logical_not(last))
        def _():
            h_copy(g, c).start()

    lax.fori_loop(0, n_groups, attention_phase, 0)
    lax.fori_loop(0, n_groups, mlp_phase, 0)
    for c in range(n_chunk):
        finish_piece(n_groups - 1, c)

    @pl.when(jnp.logical_not(last))
    def _():
        for g in range(n_groups):
            for c in range(n_chunk):
                h_copy(g, c).wait_send()


def run_layer(dims, *args):
    n_groups, n_batch, d_model, heads, seq, hd, ff, n_pp, n_tp = dims
    hw = heads * hd
    n_chunk = d_model // COLS
    n_gu = ff // COLS
    assert ff * d_model == 4 * d_model * hw
    vmem = pl.BlockSpec(memory_space=pltpu.VMEM)
    hbm = pl.BlockSpec(memory_space=pltpu.HBM)
    dma = pltpu.SemaphoreType.DMA
    return pl.pallas_call(
        functools.partial(layer_kernel, dims),
        out_shape=(jax.ShapeDtypeStruct((n_groups, n_batch, d_model), BF16),
                   jax.ShapeDtypeStruct((n_groups, heads, hd, n_batch), BF16),
                   jax.ShapeDtypeStruct((n_groups, heads, hd, n_batch), BF16)),
        in_specs=[hbm] + [vmem] * 3 + [hbm] * 10,
        out_specs=(vmem, vmem, vmem),
        scratch_shapes=[
            pltpu.VMEM((4, d_model, hw), BF16),
            pltpu.VMEM((n_gu, d_model, COLS), BF16),
            pltpu.VMEM((n_gu, d_model, COLS), BF16),
            pltpu.VMEM((SLOTS, 2 * seq, hd, n_batch), BF16),
            pltpu.VMEM((n_groups, n_batch, d_model), BF16),
            pltpu.VMEM((n_groups, n_batch, d_model), BF16),
            pltpu.VMEM((n_groups, n_batch, d_model), BF16),
            pltpu.VMEM((n_batch, d_model), BF16),
            pltpu.VMEM((hw, n_batch), BF16),
            pltpu.VMEM((n_batch, ff), BF16),
            pltpu.VMEM((seq, n_batch), F32),
            pltpu.VMEM((n_groups, hd // 2, n_batch), F32),
            pltpu.VMEM((n_groups, hd // 2, n_batch), F32),
            dma((n_groups,)), dma((3,)), dma((d_model // hw,)), dma((4,)), dma((2, n_gu)), dma((SLOTS, 2)),
            dma((n_groups, n_chunk)), dma((n_groups, n_chunk)), dma((n_groups, n_chunk)),
            dma((n_groups, n_chunk)), dma((n_groups, n_chunk)), dma((n_groups, n_chunk)),
        ],
        compiler_params=pltpu.CompilerParams(collective_id=0, has_side_effects=True, vmem_limit_bytes=67043328),
        name="layer",
    )(*args)


def keep_kernel(dims, pos_hbm, kc, vc, kout, vout, todo_hbm, kb, vb, pos, todo, flags, in_sem, out_sem, pos_sem, todo_sem):
    n_groups, n_batch, _, heads, seq, _, _, n_pp, _ = dims
    n_slab = n_groups * seq
    n_items = n_groups * heads
    ahead = KEEP_SLOTS // 2
    last = lax.axis_index("pp") == n_pp - 1

    def loads(i):
        slot = lax.rem(i, KEEP_SLOTS)
        g, h = i // heads, lax.rem(i, heads)
        return (pltpu.make_async_copy(kc.at[g, h], kb.at[slot], in_sem.at[0, slot]),
                pltpu.make_async_copy(vc.at[g, h], vb.at[slot], in_sem.at[1, slot]))

    def stores(i):
        slot = lax.rem(i, KEEP_SLOTS)
        g, h = i // heads, lax.rem(i, heads)
        return (pltpu.make_async_copy(kb.at[slot], kout.at[g, h], out_sem.at[0, slot]),
                pltpu.make_async_copy(vb.at[slot], vout.at[g, h], out_sem.at[1, slot]))

    @pl.when(last)
    def _():
        for i in range(ahead):
            for copy in loads(i):
                copy.start()

        pos_copy = pltpu.make_async_copy(pos_hbm, pos, pos_sem)
        pos_copy.start()
        pos_copy.wait()

        def clear(i, carry):
            flags[i] = 0
            todo[i + 1] = 0
            return carry
        lax.fori_loop(0, n_slab, clear, 0)
        for g in range(n_groups):
            def mark(b, carry):
                flags[g * seq + pos[g, b]] = 1
                return carry
            lax.fori_loop(0, n_batch, mark, 0)

        def pick(i, count):
            hit = flags[i]

            @pl.when(hit == 1)
            def _():
                todo[count + 1] = i
            return count + hit
        todo[0] = lax.fori_loop(0, n_slab, pick, jnp.int32(0))
        todo_copy = pltpu.make_async_copy(todo, todo_hbm, todo_sem)
        todo_copy.start()

        def body(i, carry):
            for copy in loads(i):
                copy.wait()
            for copy in stores(i):
                copy.start()

            @pl.when(i + ahead < n_items)
            def _():
                @pl.when(i >= ahead)
                def _():
                    for copy in stores(i - ahead):
                        copy.wait()
                for copy in loads(i + ahead):
                    copy.start()
            return carry
        lax.fori_loop(0, n_items, body, 0)
        for i in range(n_items - 2 * ahead, n_items):
            for copy in stores(i):
                copy.wait()
        todo_copy.wait()


def keep_old(dims, positions, key_t, value_t):
    n_groups, n_batch, _, heads, seq, hd, _, _, _ = dims
    hbm = pl.BlockSpec(memory_space=pltpu.HBM)
    dma = pltpu.SemaphoreType.DMA
    return pl.pallas_call(
        functools.partial(keep_kernel, dims),
        out_shape=(jax.ShapeDtypeStruct(key_t.shape, BF16), jax.ShapeDtypeStruct(value_t.shape, BF16),
                   jax.ShapeDtypeStruct((n_groups * seq + 1,), jnp.int32)),
        in_specs=[hbm] * 3,
        out_specs=(hbm, hbm, hbm),
        scratch_shapes=[
            pltpu.VMEM((KEEP_SLOTS, seq, hd, n_batch), BF16),
            pltpu.VMEM((KEEP_SLOTS, seq, hd, n_batch), BF16),
            pltpu.SMEM((n_groups, n_batch), jnp.int32),
            pltpu.SMEM((n_groups * seq + 1,), jnp.int32),
            pltpu.SMEM((n_groups * seq,), jnp.int32),
            dma((2, KEEP_SLOTS)), dma((2, KEEP_SLOTS)), dma, dma,
        ],
        compiler_params=pltpu.CompilerParams(vmem_limit_bytes=67043328),
        name="cache_keep",
    )(positions, key_t, value_t)


def write_kernel(dims, todo_hbm, pos_hbm, knew_hbm, vnew_hbm, kc, vc, kold, vold, kout, vout,
                 todo, pos_ref, knew, vnew, kb, vb, in_sem, out_sem, small_sem):
    n_groups, _, _, _, seq, _, _, n_pp, _ = dims
    ahead = WRITE_SLOTS // 2
    last = lax.axis_index("pp") == n_pp - 1
    small = [pltpu.make_async_copy(src, dst, small_sem.at[i]) for i, (src, dst) in enumerate(
        ((todo_hbm, todo), (pos_hbm, pos_ref), (knew_hbm, knew), (vnew_hbm, vnew)))]
    for copy in small:
        copy.start()
    small[0].wait()
    count = jnp.where(last, todo[0], n_groups * seq)

    def place(i):
        entry = jnp.where(last, todo[i + 1], i)
        return entry // seq, lax.rem(entry, seq), lax.rem(i, WRITE_SLOTS)

    def loads(i):
        g, s, slot = place(i)
        return (pltpu.make_async_copy(kc.at[g, :, s], kb.at[slot], in_sem.at[0, slot]),
                pltpu.make_async_copy(vc.at[g, :, s], vb.at[slot], in_sem.at[1, slot]))

    def stores(i):
        g, s, slot = place(i)
        return (pltpu.make_async_copy(kb.at[slot], kout.at[g, :, s], out_sem.at[0, slot]),
                pltpu.make_async_copy(vb.at[slot], vout.at[g, :, s], out_sem.at[1, slot]))

    for i in range(ahead):
        @pl.when(i < count)
        def _():
            for copy in loads(i):
                copy.start()

    for copy in small[1:]:
        copy.wait()

    def body(i, carry):
        g, s, slot = place(i)
        for copy in loads(i):
            copy.wait()
        hit = (pos_ref[g] == s)[None]
        for new, buf in ((knew, kb), (vnew, vb)):
            buf[slot] = jnp.where(hit, new[g].astype(F32), buf[slot].astype(F32)).astype(BF16)
        for copy in stores(i):
            copy.start()

        @pl.when(i + ahead < count)
        def _():
            @pl.when(i >= ahead)
            def _():
                for copy in stores(i - ahead):
                    copy.wait()
            for copy in loads(i + ahead):
                copy.start()
        return carry
    lax.fori_loop(0, count, body, 0)

    def drain(i, carry):
        for copy in stores(i):
            copy.wait()
        return carry
    lax.fori_loop(jnp.maximum(count - 2 * ahead, 0), count, drain, 0)


def write_new(dims, todo, pos, key_new, value_new, key_t, value_t, key_old, value_old):
    n_groups, n_batch, _, heads, seq, hd, _, _, _ = dims
    hbm = pl.BlockSpec(memory_space=pltpu.HBM)
    dma = pltpu.SemaphoreType.DMA
    return pl.pallas_call(
        functools.partial(write_kernel, dims),
        out_shape=(jax.ShapeDtypeStruct(key_t.shape, BF16), jax.ShapeDtypeStruct(value_t.shape, BF16)),
        in_specs=[hbm] * 8,
        out_specs=(hbm, hbm),
        scratch_shapes=[
            pltpu.SMEM((n_groups * seq + 1,), jnp.int32),
            pltpu.VMEM((n_groups, 1, n_batch), jnp.int32),
            pltpu.VMEM((n_groups, heads, hd, n_batch), BF16),
            pltpu.VMEM((n_groups, heads, hd, n_batch), BF16),
            pltpu.VMEM((WRITE_SLOTS, heads, hd, n_batch), BF16),
            pltpu.VMEM((WRITE_SLOTS, heads, hd, n_batch), BF16),
            dma((2, WRITE_SLOTS)), dma((2, WRITE_SLOTS)), dma((4,)),
        ],
        input_output_aliases={6: 0, 7: 1},
        compiler_params=pltpu.CompilerParams(vmem_limit_bytes=67043328),
        cost_estimate=pl.CostEstimate(flops=n_groups * n_batch * heads * seq * hd * 40, bytes_accessed=8 * key_t.size, transcendentals=0),
        name="cache_write",
    )(todo, pos, key_new, value_new, key_t, value_t, key_old, value_old)


def solution(mesh):
    n_pp = mesh.shape["pp"]
    n_tp = mesh.shape["tp"]
    cache_spec = P("pp", "dp", None, "tp", None, None)
    col_spec = P("pp", None, "tp")
    row_spec = P("pp", "tp", None)
    gain_spec = P("pp", None)
    in_specs = (P("dp", None, None), P("dp", None), cache_spec, cache_spec, gain_spec, col_spec, col_spec, col_spec, row_spec, gain_spec, col_spec, col_spec, row_spec)
    out_specs = (P("dp", None, None), cache_spec, cache_spec)

    def per_device(hidden, positions, key_cache, value_cache, attn_norm, w_query, w_key, w_value, w_out, mlp_norm, w_gate, w_up, w_down):
        _, n_groups, n_batch, heads, seq, hd = key_cache.shape
        d_model = hidden.shape[-1]
        ff = w_gate.shape[-1]
        dims = (n_groups, n_batch, d_model, heads, seq, hd, ff, n_pp, n_tp)
        key_t = jnp.transpose(key_cache[0], (0, 2, 3, 4, 1))
        value_t = jnp.transpose(value_cache[0], (0, 2, 3, 4, 1))
        pos = positions[:, None, :]
        key_old, value_old, todo = keep_old(dims, positions, key_t, value_t)
        state, key_new, value_new = run_layer(
            dims, todo, pos, attn_norm, mlp_norm, hidden, key_t, value_t,
            w_query[0], w_key[0], w_value[0], w_out[0], w_gate[0], w_up[0], w_down[0])

        stage = lax.axis_index("pp")
        from_last = [lax.ppermute(state, "pp", [(n_pp - 1, dst)]) for dst in range(1, n_pp - 1)]
        key_t, value_t = write_new(dims, todo, pos, key_new, value_new, key_t, value_t, key_old, value_old)
        from_last[0], key_t = lax.optimization_barrier((from_last[0], key_t))
        from_last.append(lax.ppermute(from_last[0], "pp", [(1, 0)]))
        final = jnp.where(stage == n_pp - 1, state, sum(from_last[1:], from_last[0]))
        return final, jnp.transpose(key_t, (0, 4, 1, 2, 3))[None], jnp.transpose(value_t, (0, 4, 1, 2, 3))[None]

    return jax.shard_map(per_device, mesh=mesh, in_specs=in_specs, out_specs=out_specs, check_vma=False)
```
